128 devices in a mesh: blk: 32 (over x, y_hi, z), shard: 4 (over y_lo, core).
Axes of the slice: x: 4, y: 4 (y_hi: 2, y_lo: 2; y = y_hi * 2 + y_lo), z: 4, core: 2. Of those that a mesh axis runs over, the one named last changes fastest.
Arguments:
- tokens: bfloat16 [32768, 2048], P(('blk', 'shard')), may hold values from -6 to 6
- targets: bfloat16 [32768, 2048], P(('blk', 'shard')), may hold values from -6 to 6
- up_weight: bfloat16 [2048, 7168], P(None, 'shard'), may hold values from -0.125 to 0.125
- down_weight: bfloat16 [32, 7168, 2048], P('blk', 'shard'), may hold values from -6 to 6
- mix_numer: int32 [2, 32, 3], replicated, may hold values from 1 to 2, as said below
Outputs:
- drift: bfloat16 [32, 7168, 2048], P('blk', 'shard')
The draws below stay inside these ranges and needn't reach their ends.
Inputs may be any that keep to these rules, and one draw needn't show every extreme that they name: Each row of mix_numer is (2, 1, 1), (1, 2, 1) or (1, 1, 2).
All inputs are finite; a program needn't handle non-finite values.
Results may differ from the reference program's by a relative error of at most 0.017.
Values may be sent and summed in bfloat16 or wider, within the bound.
A program may use at most 128 MiB of HBM per device.

```python
import jax
import jax.numpy as jnp
from jax import lax

D = 2048
FF = 7168
TOK = 1024
ROUNDS = 2
NW = 32


def draw_mix_numer(key, part):
    picked = jax.random.randint(key, (ROUNDS, NW), 0, 3)
    return (1 + (picked[:, :, None] == jnp.arange(3, dtype=jnp.int32)[None, None, :]).astype(jnp.int32)).astype(jnp.int32)


def levels(key, shape, shards, low, high):
    factor_of = 1.0
    for axis_at, shards_of in shards:
        steps = jax.random.uniform(jax.random.fold_in(jax.random.fold_in(key, 6), axis_at), (shards_of,), jnp.float32, low / len(shards), high / len(shards))
        factor_of = factor_of * jnp.repeat(jnp.exp(steps), shape[axis_at] // shards_of).reshape((-1,) + (1,) * (len(shape) - 1 - axis_at))
    return factor_of


def noise(rng, shape, spread, limit, cuts=(), kind=jnp.bfloat16):
    result = jax.random.normal(rng, shape, jnp.float32) * spread
    if len(cuts) > 0:
        result = levels(rng, shape, cuts, -0.22, 0.18) * result
    return jnp.clip(result, min=-limit, max=limit).astype(kind)


def setup_inputs(seed: int = 0) -> dict:
    key_list = jax.random.split(jax.random.key(seed), 6)
    tokens = noise(key_list[0], (NW * TOK, D), 1.0, 6.0, ((0, 128),))
    targets = noise(key_list[1], (NW * TOK, D), 1.0, 6.0, ((0, 128),))
    up_weight = noise(key_list[2], (D, FF), D ** -0.5, 0.125, ((1, 4),))
    down_weight = noise(key_list[3], (NW, FF, D), 1.0, 6.0, ((0, 32), (1, 4)))
    mix_numer = draw_mix_numer(jax.random.fold_in(key_list[5], 71), 0)
    return {"tokens": tokens, "targets": targets, "up_weight": up_weight, "down_weight": down_weight, "mix_numer": mix_numer}


learn_rate = 2.0

def local_step(inputs, wanted, up_weight, weight):
    hidden = jax.nn.silu(jnp.dot(inputs, up_weight, preferred_element_type=jnp.float32)).astype(jnp.bfloat16)
    output = jnp.dot(hidden, weight, preferred_element_type=jnp.float32) / jnp.sqrt(jnp.float32(FF))
    resid = (output - wanted.astype(jnp.float32)).astype(jnp.bfloat16)
    grad = jnp.dot(hidden.T, resid, preferred_element_type=jnp.float32)
    return (weight.astype(jnp.float32) - learn_rate * grad / jnp.sqrt(jnp.float32(FF))).astype(jnp.bfloat16)

def mix_round(params, numer):

    def one(index):
        left_index = (index - 1) % NW
        right_index = (index + 1) % NW
        weights = numer[index].astype(jnp.float32)
        total = weights[0] * params[index].astype(jnp.float32) + weights[1] * params[left_index].astype(jnp.float32) + weights[2] * params[right_index].astype(jnp.float32)
        return (total / 4.0).astype(jnp.bfloat16)
    return lax.map(one, jnp.arange(NW, dtype=jnp.int32))

def reference(tokens, targets, up_weight, down_weight, mix_numer):
    inputs = tokens.reshape(NW, TOK, D)
    wanted = targets.reshape(NW, TOK, D)
    stepped = lax.map(lambda item: local_step(item[0], item[1], up_weight, item[2]), (inputs, wanted, down_weight))
    mixed = stepped
    for round_index in range(ROUNDS):
        mixed = mix_round(mixed, mix_numer[round_index])

    def accumulate(index, total):
        return total + mixed[index].astype(jnp.float32)
    total = lax.fori_loop(0, NW, accumulate, jnp.zeros((FF, D), jnp.float32))
    average = total / jnp.float32(NW)
    return lax.map(lambda item: (item.astype(jnp.float32) - average).astype(jnp.bfloat16), mixed)
```

```python
import functools
import jax
import jax.numpy as jnp
from jax import lax
from jax.experimental import pallas as pl
from jax.experimental.pallas import tpu as pltpu
from jax.sharding import PartitionSpec as P

MESH = pl.DeviceIdType.MESH
LEARN_RATE = 2.0
NW = 32
CH = 16
DEPTH = 2
F32 = jnp.float32
BF16 = jnp.bfloat16


def place():
    b, s = lax.axis_index("blk"), lax.axis_index("shard")
    return b, s, b // 8, (b // 4) % 2, b % 4


def gossip(numer, s, out, l1, r1, l2, r2, avg, rsx, piece, yrx, zrx,
           gs, gr, xs, xr, ys, yr, zs, zr, os):
    b, sh, x, yh, z = place()
    rows, width = s.shape[1], s.shape[2]
    chunks = s.shape[0]
    groups = 4
    per = chunks // groups
    quarter, half = rows // 4, rows // 8
    left, right = ((b + 31) % 32, sh), ((b + 1) % 32, sh)

    def at(xx, yy, zz):
        return (xx * 8 + yy * 4 + zz, sh)

    inner = jnp.logical_or(z == 1, z == 2)
    outer = jnp.logical_or(z == 0, z == 3)
    ydev = at(x, 1 - yh, z)
    zdev = at(x, yh, 3 - z)
    back = jnp.logical_and(yh == 1, z == 3)
    step = jnp.where(back, 3, 1)
    xnext = at((x + step) % 4, yh, z)

    barrier = pltpu.get_barrier_semaphore()
    for dev in (left, right, at((x + 1) % 4, yh, z), at((x + 2) % 4, yh, z), at((x + 3) % 4, yh, z),
                ydev, at(x, yh, (z + 1) % 4), at(x, yh, (z + 3) % 4)):
        pl.semaphore_signal(barrier, inc=1, device_id=dev, device_id_type=MESH)
    pl.semaphore_wait(barrier, 8)

    def n(r, k, j):
        return numer[r * 96 + k * 3 + j].astype(F32)

    kl, kr, kll, krr = (b + 31) % 32, (b + 1) % 32, (b + 30) % 32, (b + 2) % 32

    def v(k0, k, k1):
        return n(1, k, 0) + n(1, k1, 1) + n(1, k0, 2)

    vb, vl, vr = v(kl, b, kr), v(kll, kl, b), v(b, kr, krr)
    vll, vrr = v((b + 29) % 32, kll, kl), v(kr, krr, (b + 3) % 32)
    wb = (n(0, b, 0) * vb + n(0, kr, 1) * vr + n(0, kl, 2) * vl) * (1.0 / 16)
    wl = (n(0, kl, 0) * vl + n(0, b, 1) * vb + n(0, kll, 2) * vll) * (1.0 / 16)
    wr = (n(0, kr, 0) * vr + n(0, krr, 1) * vrr + n(0, b, 2) * vb) * (1.0 / 16)
    wl = jnp.where(z == 1, wl, 0.0)
    wr = jnp.where(z == 2, wr, 0.0)
    m = [[n(r, b, j) * 0.25 for j in range(3)] for r in range(2)]

    def send(src, dst, ss, rs, dev):
        return pltpu.make_async_remote_copy(src, dst, ss, rs, device_id=dev, device_id_type=MESH)

    def items(i):
        c = i % chunks
        src, dl, dr = (s, l1, r1) if i < chunks else (l1, l2, r2)
        return (send(src.at[c], dl.at[c], gs.at[0, i], gr.at[0, i], right),
                send(src.at[c], dr.at[c], gs.at[1, i], gr.at[1, i], left))

    BR = 128

    def over(total, body):
        def one(i, _):
            body(pl.ds(pl.multiple_of(i * BR, BR), BR))
            return 0
        lax.fori_loop(0, total // BR, one, 0)

    def first(c):
        def body(d):
            a = s[c, d, :].astype(F32)
            p = l1[c, d, :].astype(F32)
            q = r1[c, d, :].astype(F32)
            l1[c, d, :] = (m[0][0] * a + m[0][1] * p + m[0][2] * q).astype(BF16)
            r1[c, d, :] = (wb * a + wl * p + wr * q).astype(BF16)
        over(rows, body)

    def second(c):
        def body(d):
            a = l1[c, d, :].astype(F32)
            p = l2[c, d, :].astype(F32)
            q = r2[c, d, :].astype(F32)
            l2[c, d, :] = (m[1][0] * a + m[1][1] * p + m[1][2] * q).astype(BF16)
        over(rows, body)

    def last(c):
        def body(d):
            l2[c, d, :] = (l2[c, d, :].astype(F32) - avg[c, d, :].astype(F32)).astype(BF16)
        over(rows, body)
        pltpu.make_async_copy(l2.at[c], out.at[:, pl.ds(c * width, width)], os.at[c]).start()

    def own(g, xx, lo, size):
        return (pl.ds(g * per, per), pl.ds(pl.multiple_of(xx * quarter + lo, 32), size), slice(None))

    def a_rs(g, j):
        xx = (x + j) % 4
        return send(r1.at[own(g, xx, 0, quarter)], rsx.at[j - 1, pl.ds(g * per, per)],
                    xs.at[0, g, j - 1], xr.at[0, g, j - 1], at(xx, yh, z))

    def a_y(g):
        return send(piece.at[pl.ds(g * per, per), pl.ds(pl.multiple_of((1 - yh) * half, 32), half)],
                    yrx.at[pl.ds(g * per, per)], ys.at[0, g], yr.at[0, g], ydev)

    def a_z(g):
        return send(piece.at[pl.ds(g * per, per), pl.ds(pl.multiple_of(yh * half, 32), half)],
                    zrx.at[pl.ds(g * per, per)], zs.at[0, g], zr.at[0, g], zdev)

    def a_yg(g):
        ref = avg.at[own(g, x, yh * half, half)]
        return send(ref, ref, ys.at[1, g], yr.at[1, g], ydev)

    def a_zb(g):
        ref = avg.at[own(g, x, 0, quarter)]
        return send(ref, ref, zs.at[1, g], zr.at[1, g], at(x, yh, jnp.where(z == 1, 0, 3)))

    def a_x(g, k):
        ref = avg.at[own(g, (x - k * step + 16) % 4, 0, quarter)]
        return send(ref, ref, xs.at[1, g, k], xr.at[1, g, k], xnext)

    def when(cond, f):
        pl.when(cond)(f)

    def e_rs(g):
        def go():
            for j in (1, 2, 3):
                a_rs(g, j).start()
        when(inner, go)

    def e_y(g):
        def go():
            for j in (1, 2, 3):
                a_rs(g, j).wait_recv()
            for cc in range(per):
                c = g * per + cc
                def one(i, _):
                    d = pl.ds(pl.multiple_of(i * 64, 64), 64)
                    o = pl.ds(pl.multiple_of(x * quarter + i * 64, 64), 64)
                    t = r1[c, o, :].astype(F32)
                    for j in range(3):
                        t += rsx[j, c, d, :].astype(F32)
                    piece[c, d, :] = t.astype(BF16)
                    return 0
                lax.fori_loop(0, quarter // 64, one, 0)
            a_y(g).start()
        when(inner, go)

    def add_half(g, other, scale, dst):
        for cc in range(per):
            c = g * per + cc
            def one(i, _):
                d = pl.ds(pl.multiple_of(i * 32, 32), 32)
                o = pl.ds(pl.multiple_of(yh * half + i * 32, 32), 32)
                t = piece[c, o, :].astype(F32) + other[c, d, :].astype(F32)
                if scale is None:
                    piece[c, o, :] = t.astype(BF16)
                else:
                    p = pl.ds(pl.multiple_of(x * quarter + yh * half + i * 32, 32), 32)
                    avg[c, p, :] = (t * scale).astype(BF16)
                return 0
            lax.fori_loop(0, half // 32, one, 0)

    def e_z(g):
        def go():
            a_y(g).wait_recv()
            add_half(g, yrx, None, piece)
            a_z(g).start()
        when(inner, go)

    def e_yg(g):
        def go():
            a_z(g).wait_recv()
            add_half(g, zrx, 1.0 / NW, avg)
            a_yg(g).start()
        when(inner, go)

    def e_zb(g):
        def go():
            a_yg(g).wait_recv()
            a_zb(g).start()
        when(inner, go)

    def e_x0(g):
        when(outer, lambda: a_zb(g).wait_recv())
        a_x(g, 0).start()

    def e_x(g, k):
        a_x(g, k).wait_recv()
        if k < 2:
            a_x(g, k + 1).start()

    events = {}
    for g in range(groups):
        base = per * g + per - 1
        plan = [(0, e_rs), (2, e_y), (3, e_z), (6, e_yg), (7, e_zb), (10, e_x0)]
        plan += [(11 + k, functools.partial(e_x, k=k)) for k in range(3)]
        for at_slot, f in plan:
            events.setdefault(base + at_slot, []).append(functools.partial(f, g))

    for i in range(DEPTH):
        for cp in items(i):
            cp.start()
    ready = []
    for slot in range(2 * chunks):
        for cp in items(slot):
            cp.wait_recv()
        if slot < chunks:
            first(slot)
        else:
            second(slot - chunks)
        if slot + DEPTH < 2 * chunks:
            for cp in items(slot + DEPTH):
                cp.start()
        for f in events.get(slot, ()):
            f()
        if slot >= chunks:
            ready.append(slot - chunks)
            done = [c for c in ready if per * (c // per) + per - 1 + 13 <= slot]
            for c in done:
                last(c)
                ready.remove(c)
    assert not ready
    for i in range(2 * chunks):
        for cp in items(i):
            cp.wait_send()
    for g in range(groups):
        def drain():
            for j in (1, 2, 3):
                a_rs(g, j).wait_send()
            for f in (a_y, a_z, a_yg, a_zb):
                f(g).wait_send()
        when(inner, drain)
        for k in range(3):
            a_x(g, k).wait_send()
    for c in range(chunks):
        pltpu.make_async_copy(l2.at[c], out.at[:, pl.ds(c * width, width)], os.at[c]).wait()


def gossip_call(numer, s):
    chunks, rows, width = s.shape
    big = pltpu.VMEM(s.shape, BF16)
    q, h = rows // 4, rows // 8
    D = pltpu.SemaphoreType.DMA
    return pl.pallas_call(
        gossip,
        out_shape=jax.ShapeDtypeStruct((rows, chunks * width), BF16),
        in_specs=[pl.BlockSpec(memory_space=pltpu.SMEM), pl.BlockSpec(memory_space=pltpu.VMEM)],
        out_specs=pl.BlockSpec(memory_space=pl.ANY),
        scratch_shapes=[big] * 5 + [
            pltpu.VMEM((3, chunks, q, width), BF16),
            pltpu.VMEM((chunks, q, width), BF16),
            pltpu.VMEM((chunks, h, width), BF16),
            pltpu.VMEM((chunks, h, width), BF16),
            D((2, 2 * chunks)), D((2, 2 * chunks)), D((2, 4, 3)), D((2, 4, 3)),
            D((2, 4)), D((2, 4)), D((2, 4)), D((2, 4)), D((chunks,)),
        ],
        compiler_params=pltpu.CompilerParams(collective_id=0, has_side_effects=True, vmem_limit_bytes=62 * 2**20),
        name="gossip",
    )(numer, s)


def body(tokens, targets, up_weight, down_weight, mix_numer):
    weight = down_weight[0]
    ff = weight.shape[0] * lax.axis_size("shard")
    out_scale = 1.0 / jnp.sqrt(F32(ff))
    hidden = jax.nn.silu(
        jnp.dot(lax.all_gather(tokens, "shard", axis=0, tiled=True), up_weight, preferred_element_type=F32)
    ).astype(BF16)
    output = lax.psum_scatter(
        (jnp.dot(hidden, weight, preferred_element_type=F32) * out_scale).astype(BF16),
        "shard", scatter_dimension=0, tiled=True,
    ).astype(F32)
    resid = (output - targets.astype(F32)).astype(BF16)
    grad = lax.dot_general(
        hidden, lax.all_gather(resid, "shard", axis=0, tiled=True),
        (((0,), (0,)), ((), ())), preferred_element_type=F32,
    )
    stepped = (weight.astype(F32) - LEARN_RATE * grad * out_scale).astype(BF16)
    rows, cols = stepped.shape
    chunked = stepped.reshape(rows, CH, cols // CH).transpose(1, 0, 2)
    return gossip_call(mix_numer.reshape(-1), chunked)[None]


def solution(mesh):
    in_specs = (P(("blk", "shard"), None), P(("blk", "shard"), None), P(None, "shard"), P("blk", "shard", None), P())
    return jax.shard_map(body, mesh=mesh, in_specs=in_specs, out_specs=P("blk", "shard", None), check_vma=False)
```

```python
import jax
import jax.numpy as jnp
from jax import lax
from jax.experimental import pallas as pl
from jax.experimental.pallas import tpu as pltpu
from jax.sharding import PartitionSpec as P

MESH = pl.DeviceIdType.MESH
LEARN_RATE = 2.0
NW = 32
DEPTH = 2
EARLY = 10
F32 = jnp.float32
BF16 = jnp.bfloat16


def dot(a, b):
    return jnp.dot(a, b, preferred_element_type=F32)


def kernel(numer, tokens, targets, up, weight, out,
           s, l1, r1, l2, r2, avg, rsx, piece, yrx, zrx, tok, hid, qrx, rrx, pown,
           ls, ts, tr, ps, pr, qs, qr, rs, rr,
           gs, gr, xs, xr, as_, ar, ys, yr, zs, zr, os):
    b, sh = lax.axis_index("blk"), lax.axis_index("shard")
    x, yh, z = b // 8, (b // 4) % 2, b % 4
    yl, e = sh // 2, sh % 2
    slabs, rows, width = s.shape
    chunks, cr = 2 * slabs, rows // 2
    ff, dim = 4 * rows, slabs * width
    groups, per = 4, slabs // 4
    quarter, half = rows // 4, rows // 8
    trow = tokens.shape[0]
    tp = trow // 2

    def at(xx, yy, zz):
        return (xx * 8 + yy * 4 + zz, sh)

    left, right = ((b + 31) % 32, sh), ((b + 1) % 32, sh)
    core, mate = (b, 2 * yl + 1 - e), (b, 2 * (1 - yl) + e)
    ydev = at(x, 1 - yh, z)
    zdev = at(x, yh, 3 - z)
    xp, xm = at((x + 1) % 4, yh, z), at((x + 3) % 4, yh, z)
    inner = jnp.logical_or(z == 1, z == 2)
    outer = jnp.logical_or(z == 0, z == 3)

    def send(src, dst, ss, rsem, dev):
        return pltpu.make_async_remote_copy(src, dst, ss, rsem, device_id=dev, device_id_type=MESH)

    def up_a(j):
        return pltpu.make_async_copy(up.at[pl.ds(0, rows), pl.ds(j * width, width)], l2.at[j], ls.at[0, j])

    def up_b(j):
        return pltpu.make_async_copy(up.at[pl.ds(rows, dim - rows), pl.ds(j * width, width)],
                                     l2.at[slabs - 1, pl.ds(j * width, width)], ls.at[1, j])

    def w_in(c):
        return pltpu.make_async_copy(weight.at[0, :, pl.ds(c * width, width)], s.at[c], ls.at[2, c])

    def t_in(c):
        return pltpu.make_async_copy(targets.at[:, pl.ds(c * width, width)], piece.at[c, pl.ds(0, trow)], ls.at[3, c])

    def which(p, core_at):
        return p + core_at - 2 * p * core_at

    def spot(p, chip, core_from, core_at):
        at_row = (which(p, core_at) * 2 + chip) * trow + core_from * tp
        return pl.ds(pl.multiple_of(at_row, tp), tp)

    def own_in(p):
        return pltpu.make_async_copy(tokens.at[pl.ds(p * tp, tp)], tok.at[spot(p, yl, e, e)], ls.at[4, p])

    def t_core(p):
        return send(tokens.at[pl.ds(p * tp, tp)], tok.at[spot(p, yl, e, 1 - e)], ts.at[0, p], tr.at[0, p], core)

    def t_mate(p):
        return send(tokens.at[pl.ds(p * tp, tp)], tok.at[spot(p, yl, e, e)], ts.at[1, p], tr.at[1, p], mate)

    def t_fwd(p):
        return send(tok.at[spot(p, 1 - yl, e, e)], tok.at[spot(p, 1 - yl, e, 1 - e)], ts.at[2, p], tr.at[2, p], core)

    for p in range(2):
        own_in(p).start()
    for j in range(rows // width):
        up_a(j).start()
        up_b(j).start()

    barrier = pltpu.get_barrier_semaphore()
    for dev in (core, mate, left, right, xp, at((x + 2) % 4, yh, z), xm,
                ydev, at(x, yh, (z + 1) % 4), at(x, yh, (z + 3) % 4)):
        pl.semaphore_signal(barrier, inc=1, device_id=dev, device_id_type=MESH)
    pl.semaphore_wait(barrier, 10)

    for p in range(2):
        t_mate(p).start()
    for p in range(2):
        t_core(p).start()
    for c in range(slabs):
        w_in(c).start()
        t_in(c).start()

    def n(r, k, j):
        return numer[r * 96 + k * 3 + j].astype(F32)

    kl, kr, kll, krr = (b + 31) % 32, (b + 1) % 32, (b + 30) % 32, (b + 2) % 32

    def v(k0, k, k1):
        return n(1, k, 0) + n(1, k1, 1) + n(1, k0, 2)

    vb, vl, vr = v(kl, b, kr), v(kll, kl, b), v(b, kr, krr)
    vll, vrr = v((b + 29) % 32, kll, kl), v(kr, krr, (b + 3) % 32)
    wb = (n(0, b, 0) * vb + n(0, kr, 1) * vr + n(0, kl, 2) * vl) * (1.0 / 16)
    wl = (n(0, kl, 0) * vl + n(0, b, 1) * vb + n(0, kll, 2) * vll) * (1.0 / 16)
    wr = (n(0, kr, 0) * vr + n(0, krr, 1) * vrr + n(0, b, 2) * vb) * (1.0 / 16)
    wl = jnp.where(z == 1, wl, 0.0)
    wr = jnp.where(z == 2, wr, 0.0)
    m = [[n(r, b, j) * 0.25 for j in range(3)] for r in range(2)]

    def hidden(p, chip):
        t = which(p, e) * 2 + chip
        d = pl.ds(pl.multiple_of(t * trow, trow), trow)

        def one(j, _):
            lanes = pl.ds(pl.multiple_of(j * width, width), width)
            a = dot(tok[d, :rows], l2[j]) + dot(tok[d, rows:], l2[slabs - 1, lanes, :])
            h = a / (1.0 + jnp.exp(-a))
            hid[d, lanes] = h.astype(BF16)
            r2[t, lanes, :] = h.T.astype(BF16)
            return 0

        lax.fori_loop(0, rows // width, one, 0)

    for p in range(2):
        own_in(p).wait()
    for j in range(rows // width):
        up_a(j).wait()
        up_b(j).wait()
    for p in range(2):
        t_core(p).wait_recv()
        hidden(p, yl)
    for c in range(slabs):
        w_in(c).wait()
        t_in(c).wait()
    for p in range(2):
        t_mate(p).wait_recv()
        t_fwd(p).start()
        t_fwd(p).wait_recv()
        hidden(p, 1 - yl)
    for p in range(2):
        t_fwd(p).wait_send()

    scale = ff ** -0.5

    def prx(c):
        return r2.at[4 + c // 3, pl.ds(pl.multiple_of((c % 3) * 2 * trow, trow), 2 * trow)]

    def psend(c):
        return tok.at[pl.ds(0, 2 * trow), pl.ds(pl.multiple_of(c * width, width), width)]

    def qsend(c):
        return tok.at[pl.ds(2 * trow, 2 * trow), pl.ds(pl.multiple_of(c * width, width), width)]

    def c_p(c):
        return send(psend(c), prx(c), ps.at[c], pr.at[c], core)

    def c_q(c):
        return send(qsend(c), qrx.at[c], qs.at[c], qr.at[c], mate)

    def c_r(c):
        return send(qrx.at[c], rrx.at[c], rs.at[c], rr.at[c], core)

    def item(i):
        c, o = (i % chunks) // 2, i % 2
        d = pl.ds(o * cr, cr)
        return c, d

    def items(i):
        c, d = item(i)
        src, dl, dr = (s, l1, r1) if i < chunks else (l1, l2, r2)
        return (send(src.at[c, d], dl.at[c, d], gs.at[0, i], gr.at[0, i], right),
                send(src.at[c, d], dr.at[c, d], gs.at[1, i], gr.at[1, i], left))

    def s_items(c):
        for o in range(2):
            d = pl.ds(o * cr, cr)
            i = 2 * c + o
            send(s.at[c, d], l1.at[c, d], gs.at[0, i], gr.at[0, i], right).start()
            send(s.at[c, d], r1.at[c, d], gs.at[1, i], gr.at[1, i], left).start()

    row_core = lax.broadcasted_iota(jnp.int32, (trow, width), 0) // tp

    def stage_a(c):
        lanes = pl.ds(pl.multiple_of(c * width, width), width)

        def one(i, _):
            w, chip = i // 2, i % 2
            a = dot(hid[pl.ds(pl.multiple_of(i * trow, trow), trow), :], s[c]) * scale
            p = w + e - 2 * w * e
            y = piece[c, pl.ds(pl.multiple_of(p * tp, tp), tp), :].astype(F32)
            y = jnp.concatenate([y, y], axis=0)
            keep = jnp.logical_and(row_core == e, chip == yl)
            a = a - jnp.where(keep, y, 0.0)

            @pl.when(w == 0)
            def _():
                pown[pl.ds(pl.multiple_of(chip * trow, trow), trow), :] = a

            @pl.when(w == 1)
            def _():
                tok[pl.ds(pl.multiple_of(chip * trow, trow), trow), lanes] = a.astype(BF16)

            return 0

        lax.fori_loop(0, 4, one, 0)
        c_p(c).start()

    def stage_b(c):
        c_p(c).wait_recv()
        lanes = pl.ds(pl.multiple_of(c * width, width), width)

        def one(i, _):
            o = pl.ds(pl.multiple_of(i * 64, 64), 64)
            other = r2[4 + c // 3, pl.ds(pl.multiple_of((c % 3) * 2 * trow + i * 64, 64), 64), :]
            tok[pl.ds(pl.multiple_of(2 * trow + i * 64, 64), 64), lanes] = (pown[o, :] + other.astype(F32)).astype(BF16)
            return 0

        lax.fori_loop(0, 2 * trow // 64, one, 0)
        c_q(c).start()

    def stage_c(c):
        c_q(c).wait_recv()
        lanes = pl.ds(pl.multiple_of(c * width, width), width)

        def one(i, _):
            o = pl.ds(pl.multiple_of(i * 64, 64), 64)
            mine = tok[pl.ds(pl.multiple_of(2 * trow + i * 64, 64), 64), lanes]
            qrx[c, o, :] = (qrx[c, o, :].astype(F32) + mine.astype(F32)).astype(BF16)
            return 0

        lax.fori_loop(0, 2 * trow // 64, one, 0)
        c_r(c).start()

    def stage_d(c):
        c_r(c).wait_recv()

        def one(i, _):
            d = pl.ds(pl.multiple_of(i * width, width), width)
            g = dot(r2[0, d, :], qrx[c, :trow, :])
            g += dot(r2[1, d, :], qrx[c, trow:, :])
            g += dot(r2[2, d, :], rrx[c, :trow, :])
            g += dot(r2[3, d, :], rrx[c, trow:, :])
            s[c, d, :] = (s[c, d, :].astype(F32) - (LEARN_RATE * scale) * g).astype(BF16)
            return 0

        lax.fori_loop(0, rows // width, one, 0)
        pl.when(c < EARLY // 2)(lambda: s_items(c))

    def k1(i, _):
        pl.when(jnp.logical_and(i >= 1, i <= slabs))(lambda: stage_b(i - 1))
        pl.when(i >= 2)(lambda: stage_c(i - 2))
        pl.when(i < slabs)(lambda: stage_a(i))
        pl.when(i >= 2)(lambda: stage_d(i - 2))
        return 0

    lax.fori_loop(0, slabs + 2, k1, 0)

    BR = 64

    def over(i, body):
        c, _ = item(i)
        lo = (i % 2) * cr

        def one(k, _):
            body(c, pl.ds(pl.multiple_of(lo + k * BR, BR), BR))
            return 0

        lax.fori_loop(0, cr // BR, one, 0)

    def first(i):
        def body(c, d):
            a = s[c, d, :].astype(F32)
            p = l1[c, d, :].astype(F32)
            q = r1[c, d, :].astype(F32)
            l1[c, d, :] = (m[0][0] * a + m[0][1] * p + m[0][2] * q).astype(BF16)
            r1[c, d, :] = (wb * a + wl * p + wr * q).astype(BF16)
        over(i, body)

    def second(i):
        def body(c, d):
            a = l1[c, d, :].astype(F32)
            p = l2[c, d, :].astype(F32)
            q = r2[c, d, :].astype(F32)
            l2[c, d, :] = (m[1][0] * a + m[1][1] * p + m[1][2] * q).astype(BF16)
        over(i, body)

    def o_copy(i):
        c, d = item(i)
        return pltpu.make_async_copy(l2.at[c, d], out.at[0, d, pl.ds(c * width, width)], os.at[i])

    def last(i):
        def body(c, d):
            l2[c, d, :] = (l2[c, d, :].astype(F32) - avg[c, d, :].astype(F32)).astype(BF16)
        over(i, body)
        o_copy(i).start()

    def own(g, xx, lo, size):
        return (pl.ds(g * per, per), pl.ds(pl.multiple_of(xx * quarter + lo, 32), size), slice(None))

    def a_rs(g, j):
        xx = (x + j) % 4
        return send(r1.at[own(g, xx, 0, quarter)], rsx.at[j - 1, pl.ds(g * per, per)],
                    xs.at[g, j - 1], xr.at[g, j - 1], at(xx, yh, z))

    def a_y(g):
        return send(piece.at[pl.ds(g * per, per), pl.ds(pl.multiple_of((1 - yh) * half, 32), half)],
                    yrx.at[pl.ds(g * per, per)], ys.at[0, g], yr.at[0, g], ydev)

    def a_z(g):
        return send(piece.at[pl.ds(g * per, per), pl.ds(pl.multiple_of(yh * half, 32), half)],
                    zrx.at[pl.ds(g * per, per)], zs.at[0, g], zr.at[0, g], zdev)

    def a_yg(g):
        ref = avg.at[own(g, x, yh * half, half)]
        return send(ref, ref, ys.at[1, g], yr.at[1, g], ydev)

    around = [g < groups - 1 for g in range(groups)]

    def a_zb(g):
        to = at(x, yh, jnp.where(z == 1, 0, jnp.where(z == 2, 3, 3 - z)))
        if around[g]:
            ref = avg.at[own(g, x, jnp.where(z <= 1, 0, half), half)]
        else:
            ref = avg.at[own(g, x, 0, quarter)]
        return send(ref, ref, zs.at[1, g], zr.at[1, g], to)

    def a_zf(g):
        ref = avg.at[own(g, x, jnp.where(z <= 1, 0, half), half)]
        return send(ref, ref, zs.at[2, g], zr.at[2, g], zdev)

    def a_x(g, k):
        if k == 0:
            ref, to = avg.at[own(g, x, 0, quarter)], xp
        elif k == 1:
            ref, to = avg.at[own(g, x, 0, quarter)], xm
        elif k == 2:
            ref, to = avg.at[own(g, (x + 3) % 4, 0, half)], xp
        else:
            ref, to = avg.at[own(g, (x + 1) % 4, half, half)], xm
        return send(ref, ref, as_.at[g, k], ar.at[g, k], to)

    when = lambda cond, f: pl.when(cond)(f)

    def e_rs(g):
        def go():
            for j in (1, 2, 3):
                a_rs(g, j).start()
        when(inner, go)

    def e_y(g):
        def go():
            for j in (1, 2, 3):
                a_rs(g, j).wait_recv()
            for cc in range(per):
                c = g * per + cc

                def one(i, _):
                    d = pl.ds(pl.multiple_of(i * 64, 64), 64)
                    o = pl.ds(pl.multiple_of(x * quarter + i * 64, 64), 64)
                    t = r1[c, o, :].astype(F32)
                    for j in range(3):
                        t += rsx[j, c, d, :].astype(F32)
                    piece[c, d, :] = t.astype(BF16)
                    return 0

                lax.fori_loop(0, quarter // 64, one, 0)
            a_y(g).start()
        when(inner, go)

    def add_half(g, other, final):
        for cc in range(per):
            c = g * per + cc

            def one(i, _):
                d = pl.ds(pl.multiple_of(i * 32, 32), 32)
                o = pl.ds(pl.multiple_of(yh * half + i * 32, 32), 32)
                t = piece[c, o, :].astype(F32) + other[c, d, :].astype(F32)
                if final:
                    p = pl.ds(pl.multiple_of(x * quarter + yh * half + i * 32, 32), 32)
                    avg[c, p, :] = (t * (1.0 / NW)).astype(BF16)
                else:
                    piece[c, o, :] = t.astype(BF16)
                return 0

            lax.fori_loop(0, half // 32, one, 0)

    def e_z(g):
        def go():
            a_y(g).wait_recv()
            add_half(g, yrx, False)
            a_z(g).start()
        when(inner, go)

    def e_yg(g):
        def go():
            a_z(g).wait_recv()
            add_half(g, zrx, True)
            a_yg(g).start()
        when(inner, go)

    def e_zb(g):
        def go():
            a_yg(g).wait_recv()
            a_zb(g).start()
        when(inner, go)

    def e_zf(g):
        def go():
            a_zb(g).wait_recv()
            a_zf(g).start()
        when(outer, go)

    def e_x0(g):
        when(outer, lambda: (a_zf if around[g] else a_zb)(g).wait_recv())
        a_x(g, 0).start()
        a_x(g, 1).start()

    def e_x1(g):
        a_x(g, 0).wait_recv()
        a_x(g, 1).wait_recv()
        a_x(g, 2).start()
        a_x(g, 3).start()

    def e_x2(g):
        a_x(g, 2).wait_recv()
        a_x(g, 3).wait_recv()

    stages = (e_rs, e_y, e_z, e_yg, e_zb, e_zf, e_x0, e_x1, e_x2)
    plan = ((3, 5, 6, 10, 11, 14, 17, 19, 20),
            (7, 9, 10, 13, 14, 17, 20, 22, 23),
            (11, 13, 14, 17, 18, 21, 24, 26, 27),
            (15, 17, 18, 21, 22, None, 25, 27, 28))
    events = {}
    for g in range(groups):
        for f, slot in zip(stages, plan[g]):
            if slot is not None:
                events.setdefault(slot, []).append((f, g))

    ready = []
    for slot in range(2 * chunks):
        for cp in items(slot):
            cp.wait_recv()
        if slot < chunks:
            first(slot)
        else:
            second(slot)
        if EARLY <= slot + DEPTH < 2 * chunks:
            for cp in items(slot + DEPTH):
                cp.start()
        for f, g in events.get(slot, ()):
            f(g)
        if slot >= chunks:
            ready.append(slot)
            for i in [i for i in ready if plan[(i - chunks) // (2 * per)][-1] <= slot]:
                last(i)
                ready.remove(i)
    assert not ready

    for p in range(2):
        t_core(p).wait_send()
        t_mate(p).wait_send()
    for c in range(slabs):
        c_p(c).wait_send()
        c_q(c).wait_send()
        c_r(c).wait_send()
    for i in range(2 * chunks):
        for cp in items(i):
            cp.wait_send()
    for g in range(groups):
        def drain():
            for j in (1, 2, 3):
                a_rs(g, j).wait_send()
            for f in (a_y, a_z, a_yg, a_zb):
                f(g).wait_send()
        when(inner, drain)
        if around[g]:
            when(outer, lambda: a_zf(g).wait_send())
        for k in range(4):
            a_x(g, k).wait_send()
    for i in range(chunks, 2 * chunks):
        o_copy(i).wait()


def body(tokens, targets, up_weight, down_weight, mix_numer):
    rows, dim = down_weight.shape[1:]
    slabs = 8
    width = dim // slabs
    trow = tokens.shape[0]
    D = pltpu.SemaphoreType.DMA
    vm = lambda *shape: pltpu.VMEM(shape, BF16)
    any_ = pl.BlockSpec(memory_space=pl.ANY)
    return pl.pallas_call(
        kernel,
        out_shape=jax.ShapeDtypeStruct(down_weight.shape, BF16),
        in_specs=[pl.BlockSpec(memory_space=pltpu.SMEM)] + [any_] * 4,
        out_specs=any_,
        scratch_shapes=[vm(slabs, rows, width)] * 6 + [
            vm(3, slabs, rows // 4, width), vm(slabs, rows // 4, width),
            vm(slabs, rows // 8, width), vm(slabs, rows // 8, width),
            vm(4 * trow, dim), vm(4 * trow, rows),
            vm(slabs, 2 * trow, width), vm(slabs, 2 * trow, width),
            pltpu.VMEM((2 * trow, width), F32),
            D((5, slabs)), D((3, 2)), D((3, 2)),
            D((slabs,)), D((slabs,)), D((slabs,)), D((slabs,)), D((slabs,)), D((slabs,)),
            D((2, 4 * slabs)), D((2, 4 * slabs)), D((4, 3)), D((4, 3)), D((4, 4)), D((4, 4)),
            D((2, 4)), D((2, 4)), D((3, 4)), D((3, 4)), D((4 * slabs,)),
        ],
        compiler_params=pltpu.CompilerParams(
            collective_id=0, has_side_effects=True, vmem_limit_bytes=67_043_328),
        name="gossip",
    )(mix_numer.reshape(-1), tokens, targets, up_weight, down_weight)


def solution(mesh):
    in_specs = (P(("blk", "shard"), None), P(("blk", "shard"), None), P(None, "shard"), P("blk", "shard", None), P())
    return jax.shard_map(body, mesh=mesh, in_specs=in_specs, out_specs=P("blk", "shard", None), check_vma=False)
```

```python
import functools

import jax
import jax.numpy as jnp
from jax import lax
from jax.experimental import pallas as pl
from jax.experimental.pallas import tpu as pltpu
from jax.sharding import PartitionSpec as P

MESH = pl.DeviceIdType.MESH
LEARN_RATE = 2.0
NW = 32
WRAP_DEPTH = 2
F32 = jnp.float32
BF16 = jnp.bfloat16


def dot(a, b):
    return jnp.dot(a, b, preferred_element_type=F32)


def kernel(numer, tokens, targets, up, weight, out,
           s, l1, r1, l2, r2, avg, rsx, piece, yrx, zrx, tok, hid, qrx, rrx, pown,
           ls, ts, tr, ps, pr, qs, qr, rs, rr,
           gs, gr, xs, xr, as_, ar, ys, yr, zs, zr, os):
    b, sh = lax.axis_index("blk"), lax.axis_index("shard")
    x, yh, z = b // 8, (b // 4) % 2, b % 4
    yl, e = sh // 2, sh % 2
    slabs, rows, width = s.shape
    chunks, cr = 2 * slabs, rows // 2
    ff, dim = 4 * rows, slabs * width
    groups, per = 4, slabs // 4
    quarter, half = rows // 4, rows // 8
    trow = tokens.shape[0]
    tp = trow // 2

    def at(xx, yy, zz):
        return (xx * 8 + yy * 4 + zz, sh)

    left, right = ((b + 31) % 32, sh), ((b + 1) % 32, sh)
    core, mate = (b, 2 * yl + 1 - e), (b, 2 * (1 - yl) + e)
    ydev = at(x, 1 - yh, z)
    zdev = at(x, yh, 3 - z)
    xp, xm = at((x + 1) % 4, yh, z), at((x + 3) % 4, yh, z)
    inner = jnp.logical_or(z == 1, z == 2)
    outer = jnp.logical_or(z == 0, z == 3)
    loaded = jnp.logical_or(jnp.logical_and(z == 0, yh == 0), jnp.logical_and(z == 3, yh == 1))
    plain = jnp.logical_and(outer, jnp.logical_not(loaded))
    way = jnp.where(z == 0, 1, 3)

    def send(src, dst, ss, rsem, dev):
        return pltpu.make_async_remote_copy(src, dst, ss, rsem, device_id=dev, device_id_type=MESH)

    def up_a(j):
        return pltpu.make_async_copy(up.at[pl.ds(0, rows), pl.ds(j * width, width)], l2.at[j], ls.at[0, j])

    def up_b(j):
        return pltpu.make_async_copy(up.at[pl.ds(rows, dim - rows), pl.ds(j * width, width)],
                                     l2.at[slabs - 1, pl.ds(j * width, width)], ls.at[1, j])

    def w_in(c):
        return pltpu.make_async_copy(weight.at[0, :, pl.ds(c * width, width)], s.at[c], ls.at[2, c])

    def t_in(c):
        return pltpu.make_async_copy(targets.at[:, pl.ds(c * width, width)], piece.at[c, pl.ds(0, trow)], ls.at[3, c])

    def which(p, core_at):
        return p + core_at - 2 * p * core_at

    def spot(p, chip, core_from, core_at):
        at_row = (which(p, core_at) * 2 + chip) * trow + core_from * tp
        return pl.ds(pl.multiple_of(at_row, tp), tp)

    def own_in(p):
        return pltpu.make_async_copy(tokens.at[pl.ds(p * tp, tp)], tok.at[spot(p, yl, e, e)], ls.at[4, p])

    def t_core(p):
        return send(tokens.at[pl.ds(p * tp, tp)], tok.at[spot(p, yl, e, 1 - e)], ts.at[0, p], tr.at[0, p], core)

    def t_mate(p):
        return send(tokens.at[pl.ds(p * tp, tp)], tok.at[spot(p, yl, e, e)], ts.at[1, p], tr.at[1, p], mate)

    def t_fwd(p):
        return send(tok.at[spot(p, 1 - yl, e, e)], tok.at[spot(p, 1 - yl, e, 1 - e)], ts.at[2, p], tr.at[2, p], core)

    for p in range(2):
        own_in(p).start()
    for j in range(rows // width):
        up_a(j).start()
        up_b(j).start()

    barrier = pltpu.get_barrier_semaphore()
    for dev in (core, mate, left, right, xp, at((x + 2) % 4, yh, z), xm,
                ydev, at(x, yh, (z + 1) % 4), at(x, yh, (z + 3) % 4)):
        pl.semaphore_signal(barrier, inc=1, device_id=dev, device_id_type=MESH)
    pl.semaphore_wait(barrier, 10)

    for p in range(2):
        t_mate(p).start()
    for p in range(2):
        t_core(p).start()
    for c in range(slabs):
        w_in(c).start()
        t_in(c).start()

    def n(r, k, j):
        return numer[r * 96 + k * 3 + j].astype(F32)

    kl, kr, kll, krr = (b + 31) % 32, (b + 1) % 32, (b + 30) % 32, (b + 2) % 32

    def v(k0, k, k1):
        return n(1, k, 0) + n(1, k1, 1) + n(1, k0, 2)

    vb, vl, vr = v(kl, b, kr), v(kll, kl, b), v(b, kr, krr)
    vll, vrr = v((b + 29) % 32, kll, kl), v(kr, krr, (b + 3) % 32)
    wb = (n(0, b, 0) * vb + n(0, kr, 1) * vr + n(0, kl, 2) * vl) * (1.0 / 16)
    wl = (n(0, kl, 0) * vl + n(0, b, 1) * vb + n(0, kll, 2) * vll) * (1.0 / 16)
    wr = (n(0, kr, 0) * vr + n(0, krr, 1) * vrr + n(0, b, 2) * vb) * (1.0 / 16)
    wl = jnp.where(z == 1, wl, 0.0)
    wr = jnp.where(z == 2, wr, 0.0)
    m = [[n(r, b, j) * 0.25 for j in range(3)] for r in range(2)]

    def hidden(p, chip):
        t = which(p, e) * 2 + chip
        d = pl.ds(pl.multiple_of(t * trow, trow), trow)

        def one(j, _):
            lanes = pl.ds(pl.multiple_of(j * width, width), width)
            a = dot(tok[d, :rows], l2[j]) + dot(tok[d, rows:], l2[slabs - 1, lanes, :])
            h = a / (1.0 + jnp.exp(-a))
            hid[d, lanes] = h.astype(BF16)
            r2[t, lanes, :] = h.T.astype(BF16)
            return 0

        lax.fori_loop(0, rows // width, one, 0)

    scale = ff ** -0.5

    def lanes_of(c):
        return pl.ds(pl.multiple_of(c * width, width), width)

    def block(lo, i=0, size=None):
        return pl.ds(pl.multiple_of(lo * trow + i, 64), trow if size is None else size)

    def c_p(c, chip):
        return send(tok.at[block(2 + chip), lanes_of(c)], r2.at[4 + c // 3, block((c % 3) * 2 + chip)],
                    ps.at[c, chip], pr.at[c, chip], core)

    def c_q(c, chip):
        return send(tok.at[block(chip), lanes_of(c)], qrx.at[c, block(chip)], qs.at[c, chip], qr.at[c, chip], mate)

    def c_r(c):
        return send(qrx.at[c], rrx.at[c], rs.at[c], rr.at[c], core)

    def item(i):
        c, o = (i % chunks) // 2, i % 2
        d = pl.ds(o * cr, cr)
        return c, d

    def items(i):
        c, d = item(i)
        src, dl, dr = (s, l1, r1) if i < chunks else (l1, l2, r2)
        return (lambda: send(src.at[c, d], dl.at[c, d], gs.at[0, i], gr.at[0, i], right),
                lambda: send(src.at[c, d], dr.at[c, d], gs.at[1, i], gr.at[1, i], left))

    def right_item(c, o, i):
        d = pl.ds(o * cr if isinstance(o, int) else pl.multiple_of(o * cr, cr), cr)
        return send(s.at[c, d], l1.at[c, d], gs.at[0, i], gr.at[0, i], right)

    def left_item(c, o, i):
        d = pl.ds(o * cr if isinstance(o, int) else pl.multiple_of(o * cr, cr), cr)
        return send(s.at[c, d], r1.at[c, d], gs.at[1, i], gr.at[1, i], left)

    def early(c):
        @pl.when(z == 0)
        def _():
            for o in range(2):
                right_item(c, o, 2 * c + o).start()

        @pl.when(z == 3)
        def _():
            for o in range(2):
                left_item(c, o, 2 * c + o).start()

        @pl.when(inner)
        def _():
            right_item(c // 2, c % 2, c).start()
            left_item(c // 2, c % 2, c).start()

    row_core = lax.broadcasted_iota(jnp.int32, (trow, width), 0) // tp

    def stage_a(c, chip):
        lanes = lanes_of(c)

        def one(w, _):
            rows_at = block(w * 2 + chip)
            a = dot(hid[rows_at, :], s[c]) * scale
            p = w + e - 2 * w * e
            y = piece[c, pl.ds(pl.multiple_of(p * tp, tp), tp), :].astype(F32)
            y = jnp.concatenate([y, y], axis=0)
            a = a - jnp.where(jnp.logical_and(row_core == e, chip == yl), y, 0.0)

            @pl.when(w == 0)
            def _():
                pown[...] = a

            @pl.when(w == 1)
            def _():
                tok[rows_at, lanes] = a.astype(BF16)

            return 0

        lax.fori_loop(0, 2, one, 0)
        c_p(c, chip).start()

    def stage_b(c, chip):
        c_p(c, chip).wait_recv()
        lanes = lanes_of(c)

        def one(i, _):
            other = r2[4 + c // 3, block((c % 3) * 2 + chip, i * 64, 64), :]
            mine = pown[pl.ds(pl.multiple_of(i * 64, 64), 64), :]
            tok[block(chip, i * 64, 64), lanes] = (mine + other.astype(F32)).astype(BF16)
            return 0

        lax.fori_loop(0, trow // 64, one, 0)
        c_q(c, chip).start()

    def stage_c(c):
        for chip in range(2):
            c_q(c, chip).wait_recv()
        lanes = lanes_of(c)

        def one(i, _):
            o = pl.ds(pl.multiple_of(i * 64, 64), 64)
            qrx[c, o, :] = (qrx[c, o, :].astype(F32) + tok[o, lanes].astype(F32)).astype(BF16)
            return 0

        lax.fori_loop(0, 2 * trow // 64, one, 0)
        c_r(c).start()

    def stage_d(c):
        c_r(c).wait_recv()

        def one(i, _):
            d = pl.ds(pl.multiple_of(i * width, width), width)
            g = dot(r2[0, d, :], qrx[c, :trow, :])
            g += dot(r2[1, d, :], qrx[c, trow:, :])
            g += dot(r2[2, d, :], rrx[c, :trow, :])
            g += dot(r2[3, d, :], rrx[c, trow:, :])
            s[c, d, :] = (s[c, d, :].astype(F32) - (LEARN_RATE * scale) * g).astype(BF16)
            return 0

        lax.fori_loop(0, rows // width, one, 0)
        early(c)

    for p in range(2):
        own_in(p).wait()
    for j in range(rows // width):
        up_a(j).wait()
        up_b(j).wait()
    for p in range(2):
        t_core(p).wait_recv()
        hidden(p, yl)
    for c in range(slabs):
        w_in(c).wait()
        t_in(c).wait()

    def own_step(i, _):
        pl.when(i >= 1)(lambda: stage_b(i - 1, yl))
        pl.when(i < slabs)(lambda: stage_a(i, yl))
        return 0

    lax.fori_loop(0, slabs + 1, own_step, 0)
    for p in range(2):
        t_mate(p).wait_recv()
        t_fwd(p).start()
        t_fwd(p).wait_recv()
        hidden(p, 1 - yl)
    for p in range(2):
        t_fwd(p).wait_send()

    def other_step(i, _):
        pl.when(jnp.logical_and(i >= 1, i <= slabs))(lambda: stage_b(i - 1, 1 - yl))
        pl.when(i >= 2)(lambda: stage_c(i - 2))
        pl.when(i < slabs)(lambda: stage_a(i, 1 - yl))
        pl.when(i >= 2)(lambda: stage_d(i - 2))
        return 0

    lax.fori_loop(0, slabs + 2, other_step, 0)

    BR = 64

    def over(i, body):
        c, _ = item(i)
        lo = (i % 2) * cr

        def one(k, _):
            body(c, pl.ds(pl.multiple_of(lo + k * BR, BR), BR))
            return 0

        lax.fori_loop(0, cr // BR, one, 0)

    def first(i):
        def body(c, d):
            a = s[c, d, :].astype(F32)
            p = l1[c, d, :].astype(F32)
            q = r1[c, d, :].astype(F32)
            l1[c, d, :] = (m[0][0] * a + m[0][1] * p + m[0][2] * q).astype(BF16)
            r1[c, d, :] = (wb * a + wl * p + wr * q).astype(BF16)
        over(i, body)

    def second(i):
        def body(c, d):
            a = l1[c, d, :].astype(F32)
            p = l2[c, d, :].astype(F32)
            q = r2[c, d, :].astype(F32)
            l2[c, d, :] = (m[1][0] * a + m[1][1] * p + m[1][2] * q).astype(BF16)
        over(i, body)

    def o_copy(i):
        c, d = item(i)
        return pltpu.make_async_copy(l2.at[c, d], out.at[0, d, pl.ds(c * width, width)], os.at[i])

    def last(i):
        def body(c, d):
            l2[c, d, :] = (l2[c, d, :].astype(F32) - avg[c, d, :].astype(F32)).astype(BF16)
        over(i, body)
        o_copy(i).start()

    def own(g, xx, lo, size):
        return (pl.ds(g * per, per), pl.ds(pl.multiple_of(xx * quarter + lo, 32), size), slice(None))

    def a_rs(g, j):
        xx = (x + j) % 4
        return send(r1.at[own(g, xx, 0, quarter)], rsx.at[j - 1, pl.ds(g * per, per)],
                    xs.at[g, j - 1], xr.at[g, j - 1], at(xx, yh, z))

    def a_y(g):
        return send(piece.at[pl.ds(g * per, per), pl.ds(pl.multiple_of((1 - yh) * half, 32), half)],
                    yrx.at[pl.ds(g * per, per)], ys.at[0, g], yr.at[0, g], ydev)

    def a_z(g):
        return send(piece.at[pl.ds(g * per, per), pl.ds(pl.multiple_of(yh * half, 32), half)],
                    zrx.at[pl.ds(g * per, per)], zs.at[0, g], zr.at[0, g], zdev)

    def a_yg(g):
        ref = avg.at[own(g, x, yh * half, half)]
        return send(ref, ref, ys.at[1, g], yr.at[1, g], ydev)

    around = [g < groups - 1 for g in range(groups)]

    def a_zb(g):
        to = at(x, yh, jnp.where(z == 1, 0, jnp.where(z == 2, 3, 3 - z)))
        if around[g]:
            ref = avg.at[own(g, x, jnp.where(z <= 1, 0, half), half)]
        else:
            ref = avg.at[own(g, x, 0, quarter)]
        return send(ref, ref, zs.at[1, g], zr.at[1, g], to)

    def a_zf(g):
        ref = avg.at[own(g, x, jnp.where(z <= 1, 0, half), half)]
        return send(ref, ref, zs.at[2, g], zr.at[2, g], zdev)

    def a_x(g, k):
        if k == 0:
            ref, to = avg.at[own(g, x, 0, quarter)], xp
        elif k == 1:
            ref, to = avg.at[own(g, x, 0, quarter)], xm
        elif k == 2:
            ref, to = avg.at[own(g, (x + 3) % 4, 0, half)], xp
        else:
            ref, to = avg.at[own(g, (x + 1) % 4, half, half)], xm
        return send(ref, ref, as_.at[g, k], ar.at[g, k], to)

    def when(cond, *fs):
        @pl.when(cond)
        def _():
            for f in fs:
                f()

    def e_rs(g):
        for j in (1, 2, 3):
            a_rs(g, j).start()

    def e_y(g):
        for j in (1, 2, 3):
            a_rs(g, j).wait_recv()
        for cc in range(per):
            c = g * per + cc

            def one(i, _):
                d = pl.ds(pl.multiple_of(i * 64, 64), 64)
                o = pl.ds(pl.multiple_of(x * quarter + i * 64, 64), 64)
                t = r1[c, o, :].astype(F32)
                for j in range(3):
                    t += rsx[j, c, d, :].astype(F32)
                piece[c, d, :] = t.astype(BF16)
                return 0

            lax.fori_loop(0, quarter // 64, one, 0)
        a_y(g).start()

    def add_half(g, other, final):
        for cc in range(per):
            c = g * per + cc

            def one(i, _):
                d = pl.ds(pl.multiple_of(i * 32, 32), 32)
                o = pl.ds(pl.multiple_of(yh * half + i * 32, 32), 32)
                t = piece[c, o, :].astype(F32) + other[c, d, :].astype(F32)
                if final:
                    p = pl.ds(pl.multiple_of(x * quarter + yh * half + i * 32, 32), 32)
                    avg[c, p, :] = (t * (1.0 / NW)).astype(BF16)
                else:
                    piece[c, o, :] = t.astype(BF16)
                return 0

            lax.fori_loop(0, half // 32, one, 0)

    def e_z(g):
        a_y(g).wait_recv()
        add_half(g, yrx, False)
        a_z(g).start()

    def e_yg(g):
        a_z(g).wait_recv()
        add_half(g, zrx, True)
        a_yg(g).start()

    def e_zb(g):
        a_yg(g).wait_recv()
        a_zb(g).start()

    def e_zf(g):
        a_zb(g).wait_recv()
        a_zf(g).start()

    def e_x0(g):
        a_x(g, 0).start()
        a_x(g, 1).start()

    def e_x0_out(g):
        (a_zf if around[g] else a_zb)(g).wait_recv()
        e_x0(g)

    def e_x1(g):
        a_x(g, 0).wait_recv()
        a_x(g, 1).wait_recv()
        a_x(g, 2).start()
        a_x(g, 3).start()

    def e_x2(g):
        a_x(g, 2).wait_recv()
        a_x(g, 3).wait_recv()

    def a_way(g, k):
        ref = avg.at[own(g, (x + k * (4 - way)) % 4, 0, quarter)]
        return send(ref, ref, as_.at[g, k], ar.at[g, k], at((x + way) % 4, yh, z))

    def e_w0(g):
        (a_zf if around[g] else a_zb)(g).wait_recv()
        a_way(g, 0).start()

    def e_w(k, g):
        a_way(g, k).wait_recv()
        if k < 2:
            a_way(g, k + 1).start()

    stages = (e_rs, e_y, e_z, e_yg, e_zb, e_x0, e_x1, e_x2)
    plan_in = ((3, 5, 6, 10, 11, 12, 14, 16),
               (7, 9, 10, 14, 15, 16, 18, 20),
               (11, 13, 14, 18, 19, 20, 22, 24),
               (15, 17, 18, 22, 23, 24, 26, 28))
    plan_out = ((11, 13, 15, 17), (15, 17, 19, 21), (19, 21, 23, 25), (None, 24, 26, 28))
    plan_way = ((11, 13, 15, 17, 19), (15, 17, 19, 21, 23), (19, 21, 23, 25, 27), (None, 24, 26, 28, 30))
    ways = [functools.partial(e_w, k) for k in range(3)]
    inside, outside, special = {}, {}, {}
    for g in range(groups):
        for f, slot in zip(stages, plan_in[g]):
            inside.setdefault(slot, []).append((f, g))
        for f, slot in zip((e_zf, e_x0_out, e_x1, e_x2), plan_out[g]):
            if slot is not None:
                outside.setdefault(slot, []).append((f, g))
        for f, slot in zip((e_zf, e_w0, *ways), plan_way[g]):
            if slot is not None:
                special.setdefault(slot, []).append((f, g))
    jit, wrap, bulk = {}, {}, {}
    for i in range(slabs, 2 * chunks):
        jit.setdefault(i - 3 if i < chunks else max(i - 3, chunks - 2), []).append(i)
    for i in range(WRAP_DEPTH, 2 * chunks):
        wrap.setdefault(i - WRAP_DEPTH, []).append(i)
    for i in range(chunks, 2 * chunks):
        bulk.setdefault(max(i - chunks, slabs), []).append(i)

    def put(direction, those):
        for i in those:
            items(i)[direction]().start()

    def issue(slot):
        if slot in jit:
            when(inner, lambda: put(0, jit[slot]), lambda: put(1, jit[slot]))
        if slot in wrap or slot in bulk:
            when(z == 3, lambda: put(0, wrap.get(slot, ())), lambda: put(1, bulk.get(slot, ())))
            when(z == 0, lambda: put(1, wrap.get(slot, ())), lambda: put(0, bulk.get(slot, ())))

    when(z == 3, lambda: put(0, range(WRAP_DEPTH)))
    when(z == 0, lambda: put(1, range(WRAP_DEPTH)))
    ready = []
    for slot in range(2 * chunks):
        for cp in items(slot):
            cp().wait_recv()
        if slot < chunks:
            first(slot)
        else:
            second(slot)
        issue(slot)
        if slot in inside:
            when(inner, *[functools.partial(f, g) for f, g in inside[slot]])
        if slot in outside:
            when(plain, *[functools.partial(f, g) for f, g in outside[slot]])
        if slot in special:
            when(loaded, *[functools.partial(f, g) for f, g in special[slot]])
        if slot >= chunks:
            ready.append(slot)
            for i in [i for i in ready if max(p[(i - chunks) // (2 * per)][-1] for p in (plan_in, plan_out, plan_way)) <= slot]:
                last(i)
                ready.remove(i)
    assert not ready

    for p in range(2):
        t_core(p).wait_send()
        t_mate(p).wait_send()
    for c in range(slabs):
        for chip in range(2):
            c_p(c, chip).wait_send()
            c_q(c, chip).wait_send()
        c_r(c).wait_send()
    for i in range(2 * chunks):
        for cp in items(i):
            cp().wait_send()
    for g in range(groups):
        def drain():
            for j in (1, 2, 3):
                a_rs(g, j).wait_send()
            for f in (a_y, a_z, a_yg, a_zb):
                f(g).wait_send()
        when(inner, drain)
        if around[g]:
            when(outer, lambda: a_zf(g).wait_send())
        when(loaded, *[a_way(g, k).wait_send for k in range(3)])
        when(jnp.logical_not(loaded), *[a_x(g, k).wait_send for k in range(4)])
    for i in range(chunks, 2 * chunks):
        o_copy(i).wait()


def body(tokens, targets, up_weight, down_weight, mix_numer):
    rows, dim = down_weight.shape[1:]
    slabs = 8
    width = dim // slabs
    trow = tokens.shape[0]
    D = pltpu.SemaphoreType.DMA
    vm = lambda *shape: pltpu.VMEM(shape, BF16)
    any_ = pl.BlockSpec(memory_space=pl.ANY)
    return pl.pallas_call(
        kernel,
        out_shape=jax.ShapeDtypeStruct(down_weight.shape, BF16),
        in_specs=[pl.BlockSpec(memory_space=pltpu.SMEM)] + [any_] * 4,
        out_specs=any_,
        scratch_shapes=[vm(slabs, rows, width)] * 6 + [
            vm(3, slabs, rows // 4, width), vm(slabs, rows // 4, width),
            vm(slabs, rows // 8, width), vm(slabs, rows // 8, width),
            vm(4 * trow, dim), vm(4 * trow, rows),
            vm(slabs, 2 * trow, width), vm(slabs, 2 * trow, width),
            pltpu.VMEM((trow, width), F32),
            D((5, slabs)), D((3, 2)), D((3, 2)),
            D((slabs, 2)), D((slabs, 2)), D((slabs, 2)), D((slabs, 2)), D((slabs,)), D((slabs,)),
            D((2, 4 * slabs)), D((2, 4 * slabs)), D((4, 3)), D((4, 3)), D((4, 4)), D((4, 4)),
            D((2, 4)), D((2, 4)), D((3, 4)), D((3, 4)), D((4 * slabs,)),
        ],
        compiler_params=pltpu.CompilerParams(
            collective_id=0, has_side_effects=True, vmem_limit_bytes=67_043_328),
        name="gossip",
    )(mix_numer.reshape(-1), tokens, targets, up_weight, down_weight)


def solution(mesh):
    in_specs = (P(("blk", "shard"), None), P(("blk", "shard"), None), P(None, "shard"), P("blk", "shard", None), P())
    return jax.shard_map(body, mesh=mesh, in_specs=in_specs, out_specs=P("blk", "shard", None), check_vma=False)
```

```python
import functools

import jax
import jax.numpy as jnp
from jax import lax
from jax.experimental import pallas as pl
from jax.experimental.pallas import tpu as pltpu
from jax.sharding import PartitionSpec as P

MESH = pl.DeviceIdType.MESH
LEARN_RATE = 2.0
NW = 32
GRAD_ROWS = 896
HEAD = 4
WRAP_DEPTH = 3
F32 = jnp.float32
BF16 = jnp.bfloat16


def dot(a, b):
    return jnp.dot(a, b, preferred_element_type=F32)


def kernel(numer, tokens, targets, up, weight, out,
           s, l1, r1, l2, r2, avg, rsx, piece, yrx, zrx, tok, hid, qrx, rrx, pown,
           ls, ts, tr, ps, pr, qs, qr, rs, rr,
           gs, gr, xs, xr, as_, ar, ys, yr, zs, zr, os, free):
    b, sh = lax.axis_index("blk"), lax.axis_index("shard")
    x, yh, z = b // 8, (b // 4) % 2, b % 4
    yl, e = sh // 2, sh % 2
    slabs, rows, width = s.shape
    chunks, cr = 2 * slabs, rows // 2
    ff, dim = 4 * rows, slabs * width
    groups, per = 4, slabs // 4
    quarter, half = rows // 4, rows // 8
    trow = tokens.shape[0]
    tp = trow // 2

    def at(xx, yy, zz):
        return (xx * 8 + yy * 4 + zz, sh)

    left, right = ((b + 31) % 32, sh), ((b + 1) % 32, sh)
    core, mate = (b, 2 * yl + 1 - e), (b, 2 * (1 - yl) + e)
    ydev = at(x, 1 - yh, z)
    zdev = at(x, yh, 3 - z)
    xp, xm = at((x + 1) % 4, yh, z), at((x + 3) % 4, yh, z)
    inner = jnp.logical_or(z == 1, z == 2)
    outer = jnp.logical_or(z == 0, z == 3)
    loaded = jnp.logical_or(jnp.logical_and(z == 0, yh == 0), jnp.logical_and(z == 3, yh == 1))
    plain = jnp.logical_and(outer, jnp.logical_not(loaded))
    way = jnp.where(z == 0, 1, 3)

    def send(src, dst, ss, rsem, dev):
        return pltpu.make_async_remote_copy(src, dst, ss, rsem, device_id=dev, device_id_type=MESH)

    def when(cond, *fs):
        @pl.when(cond)
        def _():
            for f in fs:
                f()

    def up_a(j):
        return pltpu.make_async_copy(up.at[pl.ds(0, rows), pl.ds(j * width, width)], l2.at[j], ls.at[0, j])

    def up_b(j):
        return pltpu.make_async_copy(up.at[pl.ds(rows, dim - rows), pl.ds(j * width, width)],
                                     l2.at[slabs - 1, pl.ds(j * width, width)], ls.at[1, j])

    def w_in(c):
        return pltpu.make_async_copy(weight.at[0, :, pl.ds(c * width, width)], s.at[c], ls.at[2, c])

    def t_in(c):
        return pltpu.make_async_copy(targets.at[:, pl.ds(c * width, width)], piece.at[c, pl.ds(0, trow)], ls.at[3, c])

    def which(p, core_at):
        return p + core_at - 2 * p * core_at

    def spot(p, chip, core_from, core_at):
        at_row = (chip * 2 + which(p, core_at)) * trow + core_from * tp
        return pl.ds(pl.multiple_of(at_row, tp), tp)

    def own_in(p):
        return pltpu.make_async_copy(tokens.at[pl.ds(p * tp, tp)], tok.at[spot(p, yl, e, e)], ls.at[4, p])

    def t_core(p):
        return send(tokens.at[pl.ds(p * tp, tp)], tok.at[spot(p, yl, e, 1 - e)], ts.at[0, p], tr.at[0, p], core)

    def t_mate(p):
        return send(tokens.at[pl.ds(p * tp, tp)], tok.at[spot(p, yl, e, e)], ts.at[1, p], tr.at[1, p], mate)

    def t_fwd(p):
        return send(tok.at[spot(p, 1 - yl, e, e)], tok.at[spot(p, 1 - yl, e, 1 - e)], ts.at[2, p], tr.at[2, p], core)

    for p in range(2):
        own_in(p).start()
    for j in range(rows // width):
        up_a(j).start()
        up_b(j).start()

    barrier = pltpu.get_barrier_semaphore()
    for dev in (core, mate, left, right, xp, at((x + 2) % 4, yh, z), xm,
                ydev, at(x, yh, (z + 1) % 4), at(x, yh, (z + 3) % 4)):
        pl.semaphore_signal(barrier, inc=1, device_id=dev, device_id_type=MESH)
    pl.semaphore_wait(barrier, 10)

    for p in range(2):
        t_mate(p).start()
    for p in range(2):
        t_core(p).start()
    for c in range(slabs):
        w_in(c).start()
        t_in(c).start()

    def n(r, k, j):
        return numer[r * 96 + k * 3 + j].astype(F32)

    kl, kr, kll, krr = (b + 31) % 32, (b + 1) % 32, (b + 30) % 32, (b + 2) % 32

    def v(k0, k, k1):
        return n(1, k, 0) + n(1, k1, 1) + n(1, k0, 2)

    vb, vl, vr = v(kl, b, kr), v(kll, kl, b), v(b, kr, krr)
    vll, vrr = v((b + 29) % 32, kll, kl), v(kr, krr, (b + 3) % 32)
    wb = (n(0, b, 0) * vb + n(0, kr, 1) * vr + n(0, kl, 2) * vl) * (1.0 / 16)
    wl = (n(0, kl, 0) * vl + n(0, b, 1) * vb + n(0, kll, 2) * vll) * (1.0 / 16)
    wr = (n(0, kr, 0) * vr + n(0, krr, 1) * vrr + n(0, b, 2) * vb) * (1.0 / 16)
    wl = jnp.where(z == 1, wl, 0.0)
    wr = jnp.where(z == 2, wr, 0.0)
    m = [[n(r, b, j) * 0.25 for j in range(3)] for r in range(2)]

    def hidden(t, size):
        d = pl.ds(pl.multiple_of(t * trow, trow), size * trow)

        def one(j, _):
            lanes = pl.ds(pl.multiple_of(j * width, width), width)
            a = dot(tok[d, :rows], l2[j]) + dot(tok[d, rows:], l2[slabs - 1, lanes, :])
            h = (a / (1.0 + jnp.exp(-a))).astype(BF16)
            hid[d, lanes] = h
            for k in range(size):
                r2[t + k, lanes, :] = h[k * trow:(k + 1) * trow].T
            return 0

        lax.fori_loop(0, rows // width, one, 0)

    scale = ff ** -0.5

    def lanes_of(c):
        return pl.ds(pl.multiple_of(c * width, width), width)

    def block(lo, i=0, size=None):
        return pl.ds(pl.multiple_of(lo * trow + i, 64), trow if size is None else size)

    def c_p(c, chip):
        return send(tok.at[block(2 * chip + 1), lanes_of(c)], r2.at[4 + c // 3, block((c % 3) * 2 + chip)],
                    ps.at[c, chip], pr.at[c, chip], core)

    def c_q(c, chip):
        return send(tok.at[block(2 * chip), lanes_of(c)], qrx.at[c, block(chip)], qs.at[c, chip], qr.at[c, chip], mate)

    def c_r(c):
        return send(qrx.at[c], rrx.at[c], rs.at[c], rr.at[c], core)

    def item(i):
        c, o = (i % chunks) // 2, i % 2
        d = pl.ds(o * cr, cr)
        return c, d

    def items(i):
        c, d = item(i)
        src, dl, dr = (s, l1, r1) if i < chunks else (l1, l2, r2)
        return (lambda: send(src.at[c, d], dl.at[c, d], gs.at[0, i], gr.at[0, i], right),
                lambda: send(src.at[c, d], dr.at[c, d], gs.at[1, i], gr.at[1, i], left))

    def put(direction, those):
        for i in those:
            items(i)[direction]().start()

    def right_item(c, o, i):
        d = pl.ds(o * cr if isinstance(o, int) else pl.multiple_of(o * cr, cr), cr)
        return send(s.at[c, d], l1.at[c, d], gs.at[0, i], gr.at[0, i], right)

    def left_item(c, o, i):
        d = pl.ds(o * cr if isinstance(o, int) else pl.multiple_of(o * cr, cr), cr)
        return send(s.at[c, d], r1.at[c, d], gs.at[1, i], gr.at[1, i], left)

    def early(c):
        @pl.when(z == 0)
        def _():
            for o in range(2):
                right_item(c, o, 2 * c + o).start()

        @pl.when(z == 3)
        def _():
            for o in range(2):
                left_item(c, o, 2 * c + o).start()

        @pl.when(inner)
        def _():
            right_item(c // 2, c % 2, c).start()
            left_item(c // 2, c % 2, c).start()

    row_core = lax.broadcasted_iota(jnp.int32, (trow, width), 0) // tp

    def stage_a(c, chip):
        lanes = lanes_of(c)
        d = pl.ds(pl.multiple_of(chip * 2 * trow, 2 * trow), 2 * trow)
        a = dot(hid[d, :], s[c]) * scale
        for w in range(2):
            p = w + e - 2 * w * e
            y = piece[c, pl.ds(pl.multiple_of(p * tp, tp), tp), :].astype(F32)
            y = jnp.concatenate([y, y], axis=0)
            aw = a[w * trow:(w + 1) * trow] - jnp.where(jnp.logical_and(row_core == e, chip == yl), y, 0.0)
            if w == 0:
                pown[...] = aw
            else:
                tok[block(chip * 2 + 1), lanes] = aw.astype(BF16)
        c_p(c, chip).start()

    def stage_b(c, chip):
        c_p(c, chip).wait_recv()
        lanes = lanes_of(c)

        def one(i, _):
            other = r2[4 + c // 3, block((c % 3) * 2 + chip, i * 64, 64), :]
            mine = pown[pl.ds(pl.multiple_of(i * 64, 64), 64), :]
            tok[block(2 * chip, i * 64, 64), lanes] = (mine + other.astype(F32)).astype(BF16)
            return 0

        lax.fori_loop(0, trow // 64, one, 0)

    def stage_c(c):
        for chip in range(2):
            c_q(c, chip).wait_recv()
        lanes = lanes_of(c)

        def one(i, _):
            for chip in range(2):
                o = block(chip, i * 64, 64)
                mine = tok[block(2 * chip, i * 64, 64), lanes]
                qrx[c, o, :] = (qrx[c, o, :].astype(F32) + mine.astype(F32)).astype(BF16)
            return 0

        lax.fori_loop(0, trow // 64, one, 0)
        c_r(c).start()

    def stage_d(c):
        c_r(c).wait_recv()

        def one(i, _):
            d = pl.ds(pl.multiple_of(i * GRAD_ROWS, GRAD_ROWS), GRAD_ROWS)
            g = dot(r2[0, d, :], qrx[c, :trow, :])
            g += dot(r2[1, d, :], rrx[c, :trow, :])
            g += dot(r2[2, d, :], qrx[c, trow:, :])
            g += dot(r2[3, d, :], rrx[c, trow:, :])
            s[c, d, :] = (s[c, d, :].astype(F32) - (LEARN_RATE * scale) * g).astype(BF16)
            return 0

        lax.fori_loop(0, rows // GRAD_ROWS, one, 0)
        early(c)

    for p in range(2):
        own_in(p).wait()
    for j in range(rows // width):
        up_a(j).wait()
        up_b(j).wait()
    for p in range(2):
        t_core(p).wait_recv()
    hidden(2 * yl, 2)
    for c in range(slabs):
        w_in(c).wait()
        t_in(c).wait()

    def own_step(i, _):
        when(i >= 1, lambda: stage_b(i - 1, yl))
        when(jnp.logical_and(i >= 1, i <= HEAD), lambda: c_q(i - 1, yl).start())
        when(i < slabs, lambda: stage_a(i, yl))
        return 0

    lax.fori_loop(0, slabs + 1, own_step, 0)
    for p in range(2):
        t_mate(p).wait_recv()
        t_fwd(p).start()
        t_fwd(p).wait_recv()
        hidden(2 * (1 - yl) + which(p, e), 1)
    for p in range(2):
        t_fwd(p).wait_send()

    def other_step(i, _):
        when(jnp.logical_and(i >= 1, i <= slabs), lambda: stage_b(i - 1, 1 - yl),
             lambda: c_q(i - 1, 1 - yl).start())
        when(jnp.logical_and(i >= 1, i <= slabs - HEAD), lambda: c_q(i - 1 + HEAD, yl).start())
        when(jnp.logical_and(i == slabs, z == 3), lambda: put(0, range(WRAP_DEPTH)))
        when(jnp.logical_and(i == slabs, z == 0), lambda: put(1, range(WRAP_DEPTH)))
        when(i >= 2, lambda: stage_c(i - 2))
        when(i < slabs, lambda: stage_a(i, 1 - yl))
        when(i >= 2, lambda: stage_d(i - 2))
        return 0

    lax.fori_loop(0, slabs + 2, other_step, 0)

    BR = 64

    def over(i, body):
        c, _ = item(i)
        lo = (i % 2) * cr

        def one(k, _):
            body(c, pl.ds(pl.multiple_of(lo + k * BR, BR), BR))
            return 0

        lax.fori_loop(0, cr // BR, one, 0)

    def first(i):
        def body(c, d):
            a = s[c, d, :].astype(F32)
            p = l1[c, d, :].astype(F32)
            q = r1[c, d, :].astype(F32)
            l1[c, d, :] = (m[0][0] * a + m[0][1] * p + m[0][2] * q).astype(BF16)
            r1[c, d, :] = (wb * a + wl * p + wr * q).astype(BF16)
        over(i, body)

    def second(i):
        def body(c, d):
            a = l1[c, d, :].astype(F32)
            p = l2[c, d, :].astype(F32)
            q = r2[c, d, :].astype(F32)
            l2[c, d, :] = (m[1][0] * a + m[1][1] * p + m[1][2] * q).astype(BF16)
        over(i, body)

    def o_copy(i):
        c, d = item(i)
        return pltpu.make_async_copy(l2.at[c, d], out.at[0, d, pl.ds(c * width, width)], os.at[i])

    def last(i):
        def body(c, d):
            l2[c, d, :] = (l2[c, d, :].astype(F32) - avg[c, d, :].astype(F32)).astype(BF16)
        over(i, body)
        o_copy(i).start()

    def own(g, xx, lo, size):
        return (pl.ds(g * per, per), pl.ds(pl.multiple_of(xx * quarter + lo, 32), size), slice(None))

    def a_rs(g, j):
        xx = (x + j) % 4
        return send(r1.at[own(g, xx, 0, quarter)], rsx.at[j - 1, pl.ds(g % 2 * per, per)],
                    xs.at[g, j - 1], xr.at[g, j - 1], at(xx, yh, z))

    def a_y(g):
        return send(piece.at[pl.ds(g * per, per), pl.ds(pl.multiple_of((1 - yh) * half, 32), half)],
                    yrx.at[pl.ds(g * per, per)], ys.at[0, g], yr.at[0, g], ydev)

    def a_z(g):
        return send(piece.at[pl.ds(g * per, per), pl.ds(pl.multiple_of(yh * half, 32), half)],
                    zrx.at[pl.ds(g * per, per)], zs.at[0, g], zr.at[0, g], zdev)

    def a_yg(g):
        ref = avg.at[own(g, x, yh * half, half)]
        return send(ref, ref, ys.at[1, g], yr.at[1, g], ydev)

    around = [False] * groups

    def a_zb(g):
        to = at(x, yh, jnp.where(z == 1, 0, jnp.where(z == 2, 3, 3 - z)))
        if around[g]:
            ref = avg.at[own(g, x, jnp.where(z <= 1, 0, half), half)]
        else:
            ref = avg.at[own(g, x, 0, quarter)]
        return send(ref, ref, zs.at[1, g], zr.at[1, g], to)

    def a_zf(g):
        ref = avg.at[own(g, x, jnp.where(z <= 1, 0, half), half)]
        return send(ref, ref, zs.at[2, g], zr.at[2, g], zdev)

    def a_x(g, k):
        if k == 0:
            ref, to = avg.at[own(g, x, 0, quarter)], xp
        elif k == 1:
            ref, to = avg.at[own(g, x, 0, quarter)], xm
        elif k == 2:
            ref, to = avg.at[own(g, (x + 3) % 4, 0, half)], xp
        else:
            ref, to = avg.at[own(g, (x + 1) % 4, half, half)], xm
        return send(ref, ref, as_.at[g, k], ar.at[g, k], to)


    def e_rs(g):
        if g >= 2:
            pl.semaphore_wait(free.at[g - 2], 3)
        for j in (1, 2, 3):
            a_rs(g, j).start()

    def e_y(g):
        for j in (1, 2, 3):
            a_rs(g, j).wait_recv()
        for cc in range(per):
            c = g * per + cc

            def one(i, _):
                d = pl.ds(pl.multiple_of(i * 64, 64), 64)
                o = pl.ds(pl.multiple_of(x * quarter + i * 64, 64), 64)
                t = r1[c, o, :].astype(F32)
                for j in range(3):
                    t += rsx[j, g % 2 * per + cc, d, :].astype(F32)
                piece[c, d, :] = t.astype(BF16)
                return 0

            lax.fori_loop(0, quarter // 64, one, 0)
        if g < 2:
            for j in (1, 2, 3):
                pl.semaphore_signal(free.at[g], inc=1, device_id=at((x + j) % 4, yh, z), device_id_type=MESH)
        a_y(g).start()

    def add_half(g, other, final):
        for cc in range(per):
            c = g * per + cc

            def one(i, _):
                d = pl.ds(pl.multiple_of(i * 32, 32), 32)
                o = pl.ds(pl.multiple_of(yh * half + i * 32, 32), 32)
                t = piece[c, o, :].astype(F32) + other[c, d, :].astype(F32)
                if final:
                    p = pl.ds(pl.multiple_of(x * quarter + yh * half + i * 32, 32), 32)
                    avg[c, p, :] = (t * (1.0 / NW)).astype(BF16)
                else:
                    piece[c, o, :] = t.astype(BF16)
                return 0

            lax.fori_loop(0, half // 32, one, 0)

    def e_z(g):
        a_y(g).wait_recv()
        add_half(g, yrx, False)
        a_z(g).start()

    def e_yg(g):
        a_z(g).wait_recv()
        add_half(g, zrx, True)
        a_yg(g).start()

    def e_zb(g):
        a_yg(g).wait_recv()
        a_zb(g).start()

    def e_zf(g):
        a_zb(g).wait_recv()
        a_zf(g).start()

    def e_x0(g):
        a_x(g, 0).start()
        a_x(g, 1).start()

    def e_x0_out(g):
        (a_zf if around[g] else a_zb)(g).wait_recv()
        e_x0(g)

    def e_x1(g):
        a_x(g, 0).wait_recv()
        a_x(g, 1).wait_recv()
        a_x(g, 2).start()
        a_x(g, 3).start()

    def e_x2(g):
        a_x(g, 2).wait_recv()
        a_x(g, 3).wait_recv()

    def a_way(g, k):
        ref = avg.at[own(g, (x + k * (4 - way)) % 4, 0, quarter)]
        return send(ref, ref, as_.at[g, k], ar.at[g, k], at((x + way) % 4, yh, z))

    def e_w0(g):
        (a_zf if around[g] else a_zb)(g).wait_recv()
        a_way(g, 0).start()

    def e_w(k, g):
        a_way(g, k).wait_recv()
        if k < 2:
            a_way(g, k + 1).start()

    stages = (e_rs, e_y, e_z, e_yg, e_zb, e_x0, e_x1, e_x2)
    plan_in = ((3, 5, 6, 10, 11, 12, 14, 16),
               (7, 9, 10, 14, 15, 16, 18, 20),
               (11, 13, 14, 18, 19, 20, 22, 24),
               (15, 17, 18, 22, 23, 24, 26, 28))
    plan_out = ((None, 12, 14, 16), (None, 16, 18, 20), (None, 20, 22, 24), (None, 24, 26, 28))
    plan_way = ((None, 12, 14, 16, 18), (None, 16, 18, 20, 22), (None, 20, 22, 24, 26), (None, 24, 26, 28, 30))
    ways = [functools.partial(e_w, k) for k in range(3)]
    inside, outside, special = {}, {}, {}
    for g in range(groups):
        for f, slot in zip(stages, plan_in[g]):
            inside.setdefault(slot, []).append((f, g))
        for f, slot in zip((e_zf, e_x0_out, e_x1, e_x2), plan_out[g]):
            if slot is not None:
                outside.setdefault(slot, []).append((f, g))
        for f, slot in zip((e_zf, e_w0, *ways), plan_way[g]):
            if slot is not None:
                special.setdefault(slot, []).append((f, g))
    jit, wrap, bulk = {}, {}, {}
    for i in range(slabs, 2 * chunks):
        jit.setdefault(i - 3 if i < chunks else max(i - 3, chunks - 2), []).append(i)
    for i in range(WRAP_DEPTH, 2 * chunks):
        wrap.setdefault(i - WRAP_DEPTH, []).append(i)
    for i in range(chunks, 2 * chunks):
        bulk.setdefault(max(i - chunks, slabs), []).append(i)

    def issue(slot):
        if slot in jit:
            when(inner, lambda: put(0, jit[slot]), lambda: put(1, jit[slot]))
        if slot in wrap or slot in bulk:
            when(z == 3, lambda: put(0, wrap.get(slot, ())), lambda: put(1, bulk.get(slot, ())))
            when(z == 0, lambda: put(1, wrap.get(slot, ())), lambda: put(0, bulk.get(slot, ())))

    ready = []
    for slot in range(2 * chunks):
        for cp in items(slot):
            cp().wait_recv()
        if slot < chunks:
            first(slot)
        else:
            second(slot)
        issue(slot)
        if slot in inside:
            when(inner, *[functools.partial(f, g) for f, g in inside[slot]])
        if slot in outside:
            when(plain, *[functools.partial(f, g) for f, g in outside[slot]])
        if slot in special:
            when(loaded, *[functools.partial(f, g) for f, g in special[slot]])
        if slot >= chunks:
            ready.append(slot)
            for i in [i for i in ready if max(p[(i - chunks) // (2 * per)][-1] for p in (plan_in, plan_out, plan_way)) <= slot]:
                last(i)
                ready.remove(i)
    assert not ready

    for p in range(2):
        t_core(p).wait_send()
        t_mate(p).wait_send()
    for c in range(slabs):
        for chip in range(2):
            c_p(c, chip).wait_send()
            c_q(c, chip).wait_send()
        c_r(c).wait_send()
    for i in range(2 * chunks):
        for cp in items(i):
            cp().wait_send()
    for g in range(groups):
        def drain():
            for j in (1, 2, 3):
                a_rs(g, j).wait_send()
            for f in (a_y, a_z, a_yg, a_zb):
                f(g).wait_send()
        when(inner, drain)
        if around[g]:
            when(outer, lambda: a_zf(g).wait_send())
        when(loaded, *[a_way(g, k).wait_send for k in range(3)])
        when(jnp.logical_not(loaded), *[a_x(g, k).wait_send for k in range(4)])
    for i in range(chunks, 2 * chunks):
        o_copy(i).wait()


def copy_kernel(src, dst, held, isem, osem):
    parts = held.shape[0]
    size = src.shape[1] // parts

    def move(i, back):
        there = pl.ds(i * size, size)
        if back:
            return pltpu.make_async_copy(held.at[i], dst.at[0, there], osem.at[i])
        return pltpu.make_async_copy(src.at[0, there], held.at[i], isem.at[i])

    for i in range(parts):
        move(i, False).start()
    for i in range(parts):
        move(i, False).wait()
        move(i, True).start()
    for i in range(parts):
        move(i, True).wait()


def copy_call(a):
    parts = 14
    any_ = pl.BlockSpec(memory_space=pl.ANY)
    return pl.pallas_call(
        copy_kernel,
        out_shape=jax.ShapeDtypeStruct(a.shape, a.dtype),
        in_specs=[any_],
        out_specs=any_,
        scratch_shapes=[pltpu.VMEM((parts, a.shape[1] // parts, a.shape[2]), a.dtype),
                        pltpu.SemaphoreType.DMA((parts,)), pltpu.SemaphoreType.DMA((parts,))],
        compiler_params=pltpu.CompilerParams(vmem_limit_bytes=67_043_328),
        name="place",
    )(a)


def body(tokens, targets, up_weight, down_weight, mix_numer):
    rows, dim = down_weight.shape[1:]
    slabs = 8
    width = dim // slabs
    trow = tokens.shape[0]
    D = pltpu.SemaphoreType.DMA
    vm = lambda *shape: pltpu.VMEM(shape, BF16)
    any_ = pl.BlockSpec(memory_space=pl.ANY)
    return copy_call(pl.pallas_call(
        kernel,
        out_shape=jax.ShapeDtypeStruct(down_weight.shape, BF16),
        in_specs=[pl.BlockSpec(memory_space=pltpu.SMEM)] + [any_] * 4,
        out_specs=any_,
        scratch_shapes=[vm(slabs, rows, width)] * 6 + [
            vm(3, slabs // 2, rows // 4, width), vm(slabs, rows // 4, width),
            vm(slabs, rows // 8, width), vm(slabs, rows // 8, width),
            vm(4 * trow, dim), vm(4 * trow, rows),
            vm(slabs, 2 * trow, width), vm(slabs, 2 * trow, width),
            pltpu.VMEM((trow, width), F32),
            D((5, slabs)), D((3, 2)), D((3, 2)),
            D((slabs, 2)), D((slabs, 2)), D((slabs, 2)), D((slabs, 2)), D((slabs,)), D((slabs,)),
            D((2, 4 * slabs)), D((2, 4 * slabs)), D((4, 3)), D((4, 3)), D((4, 4)), D((4, 4)),
            D((2, 4)), D((2, 4)), D((3, 4)), D((3, 4)), D((4 * slabs,)), pltpu.SemaphoreType.REGULAR((2,)),
        ],
        compiler_params=pltpu.CompilerParams(
            collective_id=0, has_side_effects=True, vmem_limit_bytes=67_043_328),
        name="gossip",
    )(mix_numer.reshape(-1), tokens, targets, up_weight, down_weight))


def solution(mesh):
    in_specs = (P(("blk", "shard"), None), P(("blk", "shard"), None), P(None, "shard"), P("blk", "shard", None), P())
    return jax.shard_map(body, mesh=mesh, in_specs=in_specs, out_specs=P("blk", "shard", None), check_vma=False)
```

```python
import functools

import jax
import jax.numpy as jnp
from jax import lax
from jax.experimental import pallas as pl
from jax.experimental.pallas import tpu as pltpu
from jax.sharding import PartitionSpec as P

MESH = pl.DeviceIdType.MESH
LEARN_RATE = 2.0
NW = 32
GRAD_ROWS = 896
HEAD = 4
RELAY_AT = 3
RING = 4
LAGS = (0, 2, 3, 6, 7, 8, 9)
WRAP_DEPTH = 3
F32 = jnp.float32
BF16 = jnp.bfloat16


def dot(a, b):
    return jnp.dot(a, b, preferred_element_type=F32)


def kernel(numer, tokens, targets, up, weight, out,
           s, l1, r1, l2, r2, avg, rsx, piece, yrx, zrx, tok, hid, qrx, rrx, pown, rel, rels, relr,
           ls, ts, tr, ps, pr, qs, qr, rs, rr,
           gs, gr, xs, xr, as_, ar, ys, yr, zs, zr, os, free):
    b, sh = lax.axis_index("blk"), lax.axis_index("shard")
    x, yh, z = b // 8, (b // 4) % 2, b % 4
    yl, e = sh // 2, sh % 2
    slabs, rows, width = s.shape
    chunks, cr = 2 * slabs, rows // 2
    ff, dim = 4 * rows, slabs * width
    groups = slabs
    quarter, half = rows // 4, rows // 8
    trow = tokens.shape[0]
    tp = trow // 2

    def at(xx, yy, zz):
        return (xx * 8 + yy * 4 + zz, sh)

    left, right = ((b + 31) % 32, sh), ((b + 1) % 32, sh)
    core, mate = (b, 2 * yl + 1 - e), (b, 2 * (1 - yl) + e)
    ydev = at(x, 1 - yh, z)
    zdev = at(x, yh, 3 - z)
    xp, xm = at((x + 1) % 4, yh, z), at((x + 3) % 4, yh, z)
    inner = jnp.logical_or(z == 1, z == 2)
    outer = jnp.logical_not(inner)
    beside = (b + jnp.where(z % 2 == 0, 1, 31)) % 32

    def send(src, dst, ss, rsem, dev):
        return pltpu.make_async_remote_copy(src, dst, ss, rsem, device_id=dev, device_id_type=MESH)

    def when(cond, *fs):
        @pl.when(cond)
        def _():
            for f in fs:
                f()

    def up_a(j):
        return pltpu.make_async_copy(up.at[pl.ds(0, rows), pl.ds(j * width, width)], l2.at[j], ls.at[0, j])

    def up_b(j):
        return pltpu.make_async_copy(up.at[pl.ds(rows, dim - rows), pl.ds(j * width, width)],
                                     l2.at[slabs - 1, pl.ds(j * width, width)], ls.at[1, j])

    def w_in(c):
        return pltpu.make_async_copy(weight.at[0, :, pl.ds(c * width, width)], s.at[c], ls.at[2, c])

    def t_in(c):
        return pltpu.make_async_copy(targets.at[:, pl.ds(c * width, width)], piece.at[c, pl.ds(0, trow)], ls.at[3, c])

    def which(p, core_at):
        return p + core_at - 2 * p * core_at

    def spot(p, chip, core_from, core_at):
        at_row = (chip * 2 + which(p, core_at)) * trow + core_from * tp
        return pl.ds(pl.multiple_of(at_row, tp), tp)

    def own_in(p):
        return pltpu.make_async_copy(tokens.at[pl.ds(p * tp, tp)], tok.at[spot(p, yl, e, e)], ls.at[4, p])

    def t_core(p):
        return send(tokens.at[pl.ds(p * tp, tp)], tok.at[spot(p, yl, e, 1 - e)], ts.at[0, p], tr.at[0, p], core)

    def t_mate(p):
        return send(tokens.at[pl.ds(p * tp, tp)], tok.at[spot(p, yl, e, e)], ts.at[1, p], tr.at[1, p], mate)

    def t_fwd(p):
        return send(tok.at[spot(p, 1 - yl, e, e)], tok.at[spot(p, 1 - yl, e, 1 - e)], ts.at[2, p], tr.at[2, p], core)

    for p in range(2):
        own_in(p).start()
    for j in range(rows // width):
        up_a(j).start()
        up_b(j).start()

    barrier = pltpu.get_barrier_semaphore()
    for dev in (core, mate, left, right, (beside, mate[1])):
        pl.semaphore_signal(barrier, inc=1, device_id=dev, device_id_type=MESH)

    @pl.when(inner)
    def _():
        for dev in (xp, at((x + 2) % 4, yh, z), xm, ydev):
            pl.semaphore_signal(barrier, inc=1, device_id=dev, device_id_type=MESH)

    pl.semaphore_wait(barrier, jnp.where(inner, 9, 5))

    for p in range(2):
        t_mate(p).start()
    for p in range(2):
        t_core(p).start()
    for c in range(slabs):
        w_in(c).start()
        t_in(c).start()

    def n(r, k, j):
        return numer[r * 96 + k * 3 + j].astype(F32)

    kl, kr, kll, krr = (b + 31) % 32, (b + 1) % 32, (b + 30) % 32, (b + 2) % 32

    def v(k0, k, k1):
        return n(1, k, 0) + n(1, k1, 1) + n(1, k0, 2)

    vb, vl, vr = v(kl, b, kr), v(kll, kl, b), v(b, kr, krr)
    vll, vrr = v((b + 29) % 32, kll, kl), v(kr, krr, (b + 3) % 32)
    wb = (n(0, b, 0) * vb + n(0, kr, 1) * vr + n(0, kl, 2) * vl) * (1.0 / 16)
    wl = (n(0, kl, 0) * vl + n(0, b, 1) * vb + n(0, kll, 2) * vll) * (1.0 / 16)
    wr = (n(0, kr, 0) * vr + n(0, krr, 1) * vrr + n(0, b, 2) * vb) * (1.0 / 16)
    wl = jnp.where(z == 1, wl, 0.0)
    wr = jnp.where(z == 2, wr, 0.0)
    m = [[n(r, b, j) * 0.25 for j in range(3)] for r in range(2)]

    def hidden(t, size):
        d = pl.ds(pl.multiple_of(t * trow, trow), size * trow)

        def one(j, _):
            lanes = pl.ds(pl.multiple_of(j * width, width), width)
            a = dot(tok[d, :rows], l2[j]) + dot(tok[d, rows:], l2[slabs - 1, lanes, :])
            h = (a / (1.0 + jnp.exp(-a))).astype(BF16)
            hid[d, lanes] = h
            for k in range(size):
                r2[t + k, lanes, :] = h[k * trow:(k + 1) * trow].T
            return 0

        lax.fori_loop(0, rows // width, one, 0)

    scale = ff ** -0.5

    def lanes_of(c):
        return pl.ds(pl.multiple_of(c * width, width), width)

    def block(lo, i=0, size=None):
        return pl.ds(pl.multiple_of(lo * trow + i, 64), trow if size is None else size)

    def c_p(c, chip):
        return send(tok.at[block(2 * chip + 1), lanes_of(c)], r2.at[4 + c // 3, block((c % 3) * 2 + chip)],
                    ps.at[c, chip], pr.at[c, chip], core)

    def c_q(c, chip):
        return send(tok.at[block(2 * chip), lanes_of(c)], qrx.at[c, block(chip)], qs.at[c, chip], qr.at[c, chip], mate)

    def relay_out(c):
        return send(tok.at[block(2 * yl), lanes_of(c)], rel.at[c - HEAD], qs.at[c, yl], relr.at[c - HEAD],
                    (beside, sh))

    def relay_on(k):
        return send(rel.at[k], qrx.at[HEAD + k, block(yl)], rels.at[k], qr.at[HEAD + k, yl], (beside, mate[1]))

    def c_r(c):
        return send(qrx.at[c], rrx.at[c], rs.at[c], rr.at[c], core)

    def item(i):
        c, o = (i % chunks) // 2, i % 2
        d = pl.ds(o * cr, cr)
        return c, d

    def items(i, later=None):
        c, d = item(i)
        src, dl, dr = (s, l1, r1) if i < chunks else (l1 if later is None else later, l2, r2)
        return (lambda: send(src.at[c, d], dl.at[c, d], gs.at[0, i], gr.at[0, i], right),
                lambda: send(src.at[c, d], dr.at[c, d], gs.at[1, i], gr.at[1, i], left))

    def put(direction, those, later=None):
        for i in those:
            items(i, later)[direction]().start()

    def right_item(c, o, i):
        d = pl.ds(o * cr if isinstance(o, int) else pl.multiple_of(o * cr, cr), cr)
        return send(s.at[c, d], l1.at[c, d], gs.at[0, i], gr.at[0, i], right)

    def left_item(c, o, i):
        d = pl.ds(o * cr if isinstance(o, int) else pl.multiple_of(o * cr, cr), cr)
        return send(s.at[c, d], r1.at[c, d], gs.at[1, i], gr.at[1, i], left)

    def early(c):
        @pl.when(z == 0)
        def _():
            for o in range(2):
                right_item(c, o, 2 * c + o).start()

        @pl.when(z == 3)
        def _():
            for o in range(2):
                left_item(c, o, 2 * c + o).start()

        @pl.when(inner)
        def _():
            right_item(c // 2, c % 2, c).start()
            left_item(c // 2, c % 2, c).start()

    row_core = lax.broadcasted_iota(jnp.int32, (trow, width), 0) // tp

    def stage_a(c, chip):
        lanes = lanes_of(c)
        d = pl.ds(pl.multiple_of(chip * 2 * trow, 2 * trow), 2 * trow)
        a = dot(hid[d, :], s[c]) * scale
        for w in range(2):
            p = w + e - 2 * w * e
            y = piece[c, pl.ds(pl.multiple_of(p * tp, tp), tp), :].astype(F32)
            y = jnp.concatenate([y, y], axis=0)
            aw = a[w * trow:(w + 1) * trow] - jnp.where(jnp.logical_and(row_core == e, chip == yl), y, 0.0)
            if w == 0:
                pown[...] = aw
            else:
                tok[block(chip * 2 + 1), lanes] = aw.astype(BF16)
        c_p(c, chip).start()

    def stage_b(c, chip):
        c_p(c, chip).wait_recv()
        lanes = lanes_of(c)

        def one(i, _):
            other = r2[4 + c // 3, block((c % 3) * 2 + chip, i * 64, 64), :]
            mine = pown[pl.ds(pl.multiple_of(i * 64, 64), 64), :]
            tok[block(2 * chip, i * 64, 64), lanes] = (mine + other.astype(F32)).astype(BF16)
            return 0

        lax.fori_loop(0, trow // 64, one, 0)

    def stage_c(c):
        for chip in range(2):
            c_q(c, chip).wait_recv()
        lanes = lanes_of(c)

        def one(i, _):
            for chip in range(2):
                o = block(chip, i * 64, 64)
                mine = tok[block(2 * chip, i * 64, 64), lanes]
                qrx[c, o, :] = (qrx[c, o, :].astype(F32) + mine.astype(F32)).astype(BF16)
            return 0

        lax.fori_loop(0, trow // 64, one, 0)
        c_r(c).start()

    def stage_d(c):
        c_r(c).wait_recv()

        def one(i, _):
            d = pl.ds(pl.multiple_of(i * GRAD_ROWS, GRAD_ROWS), GRAD_ROWS)
            g = dot(r2[0, d, :], qrx[c, :trow, :])
            g += dot(r2[1, d, :], rrx[c, :trow, :])
            g += dot(r2[2, d, :], qrx[c, trow:, :])
            g += dot(r2[3, d, :], rrx[c, trow:, :])
            s[c, d, :] = (s[c, d, :].astype(F32) - (LEARN_RATE * scale) * g).astype(BF16)
            return 0

        lax.fori_loop(0, rows // GRAD_ROWS, one, 0)
        early(c)

    for p in range(2):
        own_in(p).wait()
    for j in range(rows // width):
        up_a(j).wait()
        up_b(j).wait()
    for p in range(2):
        t_core(p).wait_recv()
    hidden(2 * yl, 2)
    for c in range(slabs):
        w_in(c).wait()
        t_in(c).wait()

    def own_step(i, _):
        when(i >= 1, lambda: stage_b(i - 1, yl))
        when(jnp.logical_and(i >= 1, i <= HEAD), lambda: c_q(i - 1, yl).start())
        when(jnp.logical_and(i > HEAD, outer), lambda: relay_out(i - 1).start())
        when(i < slabs, lambda: stage_a(i, yl))
        return 0

    lax.fori_loop(0, slabs + 1, own_step, 0)
    for p in range(2):
        t_mate(p).wait_recv()
        t_fwd(p).start()
        t_fwd(p).wait_recv()
        hidden(2 * (1 - yl) + which(p, e), 1)
    for p in range(2):
        t_fwd(p).wait_send()

    def other_step(i, _):
        when(jnp.logical_and(i >= 1, i <= slabs), lambda: stage_b(i - 1, 1 - yl),
             lambda: c_q(i - 1, 1 - yl).start())

        @pl.when(jnp.logical_and(i == RELAY_AT, inner))
        def _():
            for k in range(slabs - HEAD):
                relay_out(HEAD + k).wait_recv()
                relay_on(k).start()

        when(jnp.logical_and(jnp.logical_and(i >= 1, i <= slabs - HEAD), inner),
             lambda: c_q(i - 1 + HEAD, yl).start())
        when(jnp.logical_and(i == slabs, z == 3), lambda: put(0, range(WRAP_DEPTH)))
        when(jnp.logical_and(i == slabs, z == 0), lambda: put(1, range(WRAP_DEPTH)))
        when(i >= 2, lambda: stage_c(i - 2))
        when(i < slabs, lambda: stage_a(i, 1 - yl))
        when(i >= 2, lambda: stage_d(i - 2))
        return 0

    lax.fori_loop(0, slabs + 2, other_step, 0)

    BR = 64

    def over(i, body):
        c, _ = item(i)
        lo = (i % 2) * cr

        def one(k, _):
            body(c, pl.ds(pl.multiple_of(lo + k * BR, BR), BR))
            return 0

        lax.fori_loop(0, cr // BR, one, 0)

    def first(i):
        def body(c, d):
            a = s[c, d, :].astype(F32)
            p = l1[c, d, :].astype(F32)
            q = r1[c, d, :].astype(F32)
            l1[c, d, :] = (m[0][0] * a + m[0][1] * p + m[0][2] * q).astype(BF16)
            r1[c, d, :] = (wb * a + wl * p + wr * q).astype(BF16)
        over(i, body)

    def mixed(c, d):
        a = l1[c, d, :].astype(F32)
        p = l2[c, d, :].astype(F32)
        q = r2[c, d, :].astype(F32)
        return m[1][0] * a + m[1][1] * p + m[1][2] * q

    def o_copy(i):
        c, d = item(i)
        return pltpu.make_async_copy(l2.at[c, d], out.at[0, d, pl.ds(c * width, width)], os.at[i])

    def second(i):
        def inside(c, d):
            l2[c, d, :] = (mixed(c, d) - avg[c, d, :].astype(F32)).astype(BF16)

        def outside(c, d):
            l2[c, d, :] = mixed(c, d).astype(BF16)

        when(inner, lambda: over(i, inside))
        when(jnp.logical_not(inner), lambda: over(i, outside))
        o_copy(i).start()

    unmix = 4.0 / jnp.where(z == 1, n(1, kl, 2), n(1, kr, 1))

    def outward(i):
        g = (i % chunks) // 2
        if i % 2 == 0:
            for j in (1, 2, 3):
                a_rs(g, j).wait_send()

        def body(c, d):
            r1[c, d, :] = (l1[c, d, :].astype(F32) - unmix * avg[c, d, :].astype(F32)).astype(BF16)

        over(i, body)

    def own(g, xx, lo, size):
        return (g, pl.ds(pl.multiple_of(xx * quarter + lo, 32), size))

    def a_rs(g, j):
        xx = (x + j) % 4
        return send(r1.at[own(g, xx, 0, quarter)], rsx.at[j - 1, g % RING],
                    xs.at[g, j - 1], xr.at[g, j - 1], at(xx, yh, z))

    def a_y(g):
        return send(piece.at[g, pl.ds(pl.multiple_of((1 - yh) * half, 32), half)],
                    yrx.at[g], ys.at[0, g], yr.at[0, g], ydev)

    def a_z(g):
        return send(piece.at[g, pl.ds(pl.multiple_of(yh * half, 32), half)],
                    zrx.at[g], zs.at[g], zr.at[g], zdev)

    def a_yg(g):
        ref = avg.at[own(g, x, yh * half, half)]
        return send(ref, ref, ys.at[1, g], yr.at[1, g], ydev)

    def a_x(g, k):
        if k == 0:
            ref, to = avg.at[own(g, x, 0, quarter)], xp
        elif k == 1:
            ref, to = avg.at[own(g, x, 0, quarter)], xm
        elif k == 2:
            ref, to = avg.at[own(g, (x + 3) % 4, 0, half)], xp
        else:
            ref, to = avg.at[own(g, (x + 1) % 4, half, half)], xm
        return send(ref, ref, as_.at[g, k], ar.at[g, k], to)


    def e_rs(g):
        if g >= RING:
            pl.semaphore_wait(free.at[g - RING], 3)
        for j in (1, 2, 3):
            a_rs(g, j).start()

    def e_y(g):
        for j in (1, 2, 3):
            a_rs(g, j).wait_recv()
        def one(i, _):
            d = pl.ds(pl.multiple_of(i * 64, 64), 64)
            o = pl.ds(pl.multiple_of(x * quarter + i * 64, 64), 64)
            t = r1[g, o, :].astype(F32)
            for j in range(3):
                t += rsx[j, g % RING, d, :].astype(F32)
            piece[g, d, :] = t.astype(BF16)
            return 0

        lax.fori_loop(0, quarter // 64, one, 0)
        if g < groups - RING:
            for j in (1, 2, 3):
                pl.semaphore_signal(free.at[g], inc=1, device_id=at((x + j) % 4, yh, z), device_id_type=MESH)
        a_y(g).start()

    def add_half(g, other, final):
        def one(i, _):
            d = pl.ds(pl.multiple_of(i * 32, 32), 32)
            o = pl.ds(pl.multiple_of(yh * half + i * 32, 32), 32)
            t = piece[g, o, :].astype(F32) + other[g, d, :].astype(F32)
            if final:
                p = pl.ds(pl.multiple_of(x * quarter + yh * half + i * 32, 32), 32)
                avg[g, p, :] = (t * (1.0 / NW)).astype(BF16)
            else:
                piece[g, o, :] = t.astype(BF16)
            return 0

        lax.fori_loop(0, half // 32, one, 0)

    def e_z(g):
        a_y(g).wait_recv()
        add_half(g, yrx, False)
        a_z(g).start()

    def e_yg(g):
        a_z(g).wait_recv()
        add_half(g, zrx, True)
        a_yg(g).start()

    def e_x0(g):
        a_yg(g).wait_recv()
        a_x(g, 0).start()
        a_x(g, 1).start()

    def e_x1(g):
        a_x(g, 0).wait_recv()
        a_x(g, 1).wait_recv()
        a_x(g, 2).start()
        a_x(g, 3).start()

    def e_x2(g):
        a_x(g, 2).wait_recv()
        a_x(g, 3).wait_recv()

    inside = {}
    for g in range(groups):
        for f, lag in zip((e_rs, e_y, e_z, e_yg, e_x0, e_x1, e_x2), LAGS):
            inside.setdefault(2 * g + 1 + lag, []).append(functools.partial(f, g))
    jit, wrap, bulk = {}, {}, {}
    for i in range(slabs, 2 * chunks):
        jit.setdefault(i - 3 if i < chunks else max(i - 3, chunks - 2), []).append(i)
    for i in range(WRAP_DEPTH, 2 * chunks):
        wrap.setdefault(i - WRAP_DEPTH, []).append(i)
    for i in range(chunks, 2 * chunks):
        bulk.setdefault(max(i - chunks, slabs), []).append(i)

    def issue(slot):
        if slot in jit:
            @pl.when(inner)
            def _():
                for i in jit[slot]:
                    if i >= chunks:
                        outward(i)
            when(z == 1, lambda: put(0, jit[slot]), lambda: put(1, jit[slot], r1))
            when(z == 2, lambda: put(1, jit[slot]), lambda: put(0, jit[slot], r1))
        when(z == 3, lambda: put(0, wrap.get(slot, ())), lambda: put(1, bulk.get(slot, ())))
        when(z == 0, lambda: put(1, wrap.get(slot, ())), lambda: put(0, bulk.get(slot, ())))

    for slot in range(2 * chunks):
        for cp in items(slot):
            cp().wait_recv()
        if slot < chunks:
            first(slot)
        else:
            second(slot)
        if slot in inside:
            when(inner, *inside[slot])
        issue(slot)

    for p in range(2):
        t_core(p).wait_send()
        t_mate(p).wait_send()
    for c in range(slabs):
        for chip in range(2):
            c_p(c, chip).wait_send()
            c_q(c, chip).wait_send()
        c_r(c).wait_send()
    for i in range(2 * chunks):
        for cp in items(i):
            cp().wait_send()

    @pl.when(inner)
    def _():
        for g in range(groups):
            for f in (a_y, a_z, a_yg):
                f(g).wait_send()
            if g < slabs - HEAD:
                relay_on(g).wait_send()
            for k in range(4):
                a_x(g, k).wait_send()

    for i in range(chunks, 2 * chunks):
        o_copy(i).wait()


def copy_kernel(src, dst, held, isem, osem):
    parts = held.shape[0]
    size = src.shape[1] // parts

    def move(i, back):
        there = pl.ds(i * size, size)
        if back:
            return pltpu.make_async_copy(held.at[i], dst.at[0, there], osem.at[i])
        return pltpu.make_async_copy(src.at[0, there], held.at[i], isem.at[i])

    for i in range(parts):
        move(i, False).start()
    for i in range(parts):
        move(i, False).wait()
        move(i, True).start()
    for i in range(parts):
        move(i, True).wait()


def copy_call(a):
    parts = 14
    any_ = pl.BlockSpec(memory_space=pl.ANY)
    return pl.pallas_call(
        copy_kernel,
        out_shape=jax.ShapeDtypeStruct(a.shape, a.dtype),
        in_specs=[any_],
        out_specs=any_,
        scratch_shapes=[pltpu.VMEM((parts, a.shape[1] // parts, a.shape[2]), a.dtype),
                        pltpu.SemaphoreType.DMA((parts,)), pltpu.SemaphoreType.DMA((parts,))],
        compiler_params=pltpu.CompilerParams(vmem_limit_bytes=67_043_328),
        name="place",
    )(a)


def body(tokens, targets, up_weight, down_weight, mix_numer):
    rows, dim = down_weight.shape[1:]
    slabs = 8
    width = dim // slabs
    trow = tokens.shape[0]
    D = pltpu.SemaphoreType.DMA
    vm = lambda *shape: pltpu.VMEM(shape, BF16)
    any_ = pl.BlockSpec(memory_space=pl.ANY)
    return copy_call(pl.pallas_call(
        kernel,
        out_shape=jax.ShapeDtypeStruct(down_weight.shape, BF16),
        in_specs=[pl.BlockSpec(memory_space=pltpu.SMEM)] + [any_] * 4,
        out_specs=any_,
        scratch_shapes=[vm(slabs, rows, width)] * 6 + [
            vm(3, RING, rows // 4, width), vm(slabs, rows // 4, width),
            vm(slabs, rows // 8, width), vm(slabs, rows // 8, width),
            vm(4 * trow, dim), vm(4 * trow, rows),
            vm(slabs, 2 * trow, width), vm(slabs, 2 * trow, width),
            pltpu.VMEM((trow, width), F32), vm(slabs - HEAD, trow, width), D((slabs - HEAD,)), D((slabs - HEAD,)),
            D((5, slabs)), D((3, 2)), D((3, 2)),
            D((slabs, 2)), D((slabs, 2)), D((slabs, 2)), D((slabs, 2)), D((slabs,)), D((slabs,)),
            D((2, 4 * slabs)), D((2, 4 * slabs)), D((slabs, 3)), D((slabs, 3)), D((slabs, 4)), D((slabs, 4)),
            D((2, slabs)), D((2, slabs)), D((slabs,)), D((slabs,)), D((4 * slabs,)),
            pltpu.SemaphoreType.REGULAR((slabs - RING,)),
        ],
        compiler_params=pltpu.CompilerParams(
            collective_id=0, has_side_effects=True, vmem_limit_bytes=67_043_328),
        name="gossip",
    )(mix_numer.reshape(-1), tokens, targets, up_weight, down_weight))


def solution(mesh):
    in_specs = (P(("blk", "shard"), None), P(("blk", "shard"), None), P(None, "shard"), P("blk", "shard", None), P())
    return jax.shard_map(body, mesh=mesh, in_specs=in_specs, out_specs=P("blk", "shard", None), check_vma=False)
```

```python
import functools

import jax
import jax.numpy as jnp
from jax import lax
from jax.experimental import pallas as pl
from jax.experimental.pallas import tpu as pltpu
from jax.sharding import PartitionSpec as P

MESH = pl.DeviceIdType.MESH
LEARN_RATE = 2.0
NW = 32
GRAD_ROWS = 896
HEAD = 4
RELAY_AT = 3
LAG = (2, 4)
HEAD_IN = 4
PAIR = 2
RING = 4
LAGS = (0, 2, 3, 6, 7, 8, 9)
WRAP_DEPTH = 3
F32 = jnp.float32
BF16 = jnp.bfloat16


def dot(a, b):
    return jnp.dot(a, b, preferred_element_type=F32)


def kernel(numer, tokens, targets, up, weight, out,
           s, l1, r1, l2, r2, avg, rsx, piece, yrx, zrx, tok, hid, qrx, rrx, pown, rel, rels, relr,
           ls, ts, tr, ps, pr, qs, qr, rs, rr,
           gs, gr, xs, xr, as_, ar, ys, yr, zs, zr, os, free):
    b, sh = lax.axis_index("blk"), lax.axis_index("shard")
    x, yh, z = b // 8, (b // 4) % 2, b % 4
    yl, e = sh // 2, sh % 2
    slabs, rows, width = s.shape
    chunks, cr = 2 * slabs, rows // 2
    ff, dim = 4 * rows, slabs * width
    groups = slabs
    quarter, half = rows // 4, rows // 8
    trow = tokens.shape[0]
    tp = trow // 2

    def at(xx, yy, zz):
        return (xx * 8 + yy * 4 + zz, sh)

    left, right = ((b + 31) % 32, sh), ((b + 1) % 32, sh)
    core, mate = (b, 2 * yl + 1 - e), (b, 2 * (1 - yl) + e)
    ydev = at(x, 1 - yh, z)
    zdev = at(x, yh, 3 - z)
    xp, xm = at((x + 1) % 4, yh, z), at((x + 3) % 4, yh, z)
    inner = jnp.logical_or(z == 1, z == 2)
    outer = jnp.logical_not(inner)
    beside = (b + jnp.where(z % 2 == 0, 1, 31)) % 32

    def send(src, dst, ss, rsem, dev):
        return pltpu.make_async_remote_copy(src, dst, ss, rsem, device_id=dev, device_id_type=MESH)

    def when(cond, *fs):
        @pl.when(cond)
        def _():
            for f in fs:
                f()

    def up_a(j):
        return pltpu.make_async_copy(up.at[pl.ds(0, rows), pl.ds(j * width, width)], l2.at[j], ls.at[0, j])

    def up_b(j):
        return pltpu.make_async_copy(up.at[pl.ds(rows, dim - rows), pl.ds(j * width, width)],
                                     l2.at[slabs - 1, pl.ds(j * width, width)], ls.at[1, j])

    def w_in(c):
        return pltpu.make_async_copy(weight.at[0, :, pl.ds(c * width, width)], s.at[c], ls.at[2, c])

    def t_in(c):
        return pltpu.make_async_copy(targets.at[:, pl.ds(c * width, width)], piece.at[c, pl.ds(0, trow)], ls.at[3, c])

    def which(p, core_at):
        return p + core_at - 2 * p * core_at

    def spot(p, chip, core_from, core_at):
        at_row = (chip * 2 + which(p, core_at)) * trow + core_from * tp
        return pl.ds(pl.multiple_of(at_row, tp), tp)

    def own_in(p):
        return pltpu.make_async_copy(tokens.at[pl.ds(p * tp, tp)], tok.at[spot(p, yl, e, e)], ls.at[4, p])

    def t_core(p):
        return send(tokens.at[pl.ds(p * tp, tp)], tok.at[spot(p, yl, e, 1 - e)], ts.at[0, p], tr.at[0, p], core)

    def t_mate(p):
        return send(tokens.at[pl.ds(p * tp, tp)], tok.at[spot(p, yl, e, e)], ts.at[1, p], tr.at[1, p], mate)

    def t_fwd(p):
        return send(tok.at[spot(p, 1 - yl, e, e)], tok.at[spot(p, 1 - yl, e, 1 - e)], ts.at[2, p], tr.at[2, p], core)

    barrier = pltpu.get_barrier_semaphore()
    for dev in (core, mate, left, right, (beside, mate[1])):
        pl.semaphore_signal(barrier, inc=1, device_id=dev, device_id_type=MESH)

    @pl.when(inner)
    def _():
        for dev in (xp, at((x + 2) % 4, yh, z), xm, ydev):
            pl.semaphore_signal(barrier, inc=1, device_id=dev, device_id_type=MESH)

    for p in range(2):
        own_in(p).start()
    for j in range(rows // width):
        up_a(j).start()
        up_b(j).start()

    pl.semaphore_wait(barrier, jnp.where(inner, 9, 5))

    for p in range(2):
        t_mate(p).start()
    for p in range(2):
        t_core(p).start()
    for c in range(slabs):
        w_in(c).start()
        t_in(c).start()

    def n(r, k, j):
        return numer[r, k, j].astype(F32)

    kl, kr, kll, krr = (b + 31) % 32, (b + 1) % 32, (b + 30) % 32, (b + 2) % 32

    def v(k0, k, k1):
        return n(1, k, 0) + n(1, k1, 1) + n(1, k0, 2)

    vb, vl, vr = v(kl, b, kr), v(kll, kl, b), v(b, kr, krr)
    vll, vrr = v((b + 29) % 32, kll, kl), v(kr, krr, (b + 3) % 32)
    wb = (n(0, b, 0) * vb + n(0, kr, 1) * vr + n(0, kl, 2) * vl) * (1.0 / 16)
    wl = (n(0, kl, 0) * vl + n(0, b, 1) * vb + n(0, kll, 2) * vll) * (1.0 / 16)
    wr = (n(0, kr, 0) * vr + n(0, krr, 1) * vrr + n(0, b, 2) * vb) * (1.0 / 16)
    wl = jnp.where(z == 1, wl, 0.0)
    wr = jnp.where(z == 2, wr, 0.0)
    m = [[n(r, b, j) * 0.25 for j in range(3)] for r in range(2)]

    def hidden(t, size):
        d = pl.ds(pl.multiple_of(t * trow, trow), size * trow)

        def tiles(j, many):
            at_j = [j + k for k in range(many)]
            lanes = [pl.ds(pl.multiple_of(jj * width, width), width) for jj in at_j]
            above = jnp.concatenate([l2[jj] for jj in at_j], axis=1)
            below = jnp.concatenate([l2[slabs - 1, n, :] for n in lanes], axis=1)
            a = dot(tok[d, :rows], above) + dot(tok[d, rows:], below)
            h = (a / (1.0 + jnp.exp(-a))).astype(BF16)
            for i, n in enumerate(lanes):
                hh = h[:, i * width:(i + 1) * width]
                hid[d, n] = hh
                for k in range(size):
                    r2[t + k, n, :] = hh[k * trow:(k + 1) * trow].T

        many = PAIR if size == 1 else 1
        whole = rows // width // many

        def one(j, _):
            tiles(j * many, many)
            return 0

        lax.fori_loop(0, whole, one, 0)
        for j in range(whole * many, rows // width):
            tiles(j, 1)

    scale = ff ** -0.5

    def lanes_of(c):
        return pl.ds(pl.multiple_of(c * width, width), width)

    def block(lo, i=0, size=None):
        return pl.ds(pl.multiple_of(lo * trow + i, 64), trow if size is None else size)

    def c_p(c, chip):
        return send(tok.at[block(2 * chip + 1), lanes_of(c)], r2.at[4 + c // 3, block((c % 3) * 2 + chip)],
                    ps.at[c, chip], pr.at[c, chip], core)

    def c_q(c, chip):
        return send(tok.at[block(2 * chip), lanes_of(c)], qrx.at[c, block(chip)], qs.at[c, chip], qr.at[c, chip], mate)

    def relay_out(c):
        return send(tok.at[block(2 * yl), lanes_of(c)], rel.at[c - HEAD], qs.at[c, yl], relr.at[c - HEAD],
                    (beside, sh))

    def relay_on(k):
        return send(rel.at[k], qrx.at[HEAD + k, block(yl)], rels.at[k], qr.at[HEAD + k, yl], (beside, mate[1]))

    def c_r(c):
        return send(qrx.at[c], rrx.at[c], rs.at[c], rr.at[c], core)

    def item(i):
        c, o = (i % chunks) // 2, i % 2
        d = pl.ds(o * cr, cr)
        return c, d

    def items(i, later=None):
        c, d = item(i)
        src, dl, dr = (s, l1, r1) if i < chunks else (l1 if later is None else later, l2, r2)
        return (lambda: send(src.at[c, d], dl.at[c, d], gs.at[0, i], gr.at[0, i], right),
                lambda: send(src.at[c, d], dr.at[c, d], gs.at[1, i], gr.at[1, i], left))

    def put(direction, those, later=None):
        for i in those:
            items(i, later)[direction]().start()

    def right_item(c, o, i):
        d = pl.ds(o * cr if isinstance(o, int) else pl.multiple_of(o * cr, cr), cr)
        return send(s.at[c, d], l1.at[c, d], gs.at[0, i], gr.at[0, i], right)

    def left_item(c, o, i):
        d = pl.ds(o * cr if isinstance(o, int) else pl.multiple_of(o * cr, cr), cr)
        return send(s.at[c, d], r1.at[c, d], gs.at[1, i], gr.at[1, i], left)

    def early(c):
        @pl.when(z == 0)
        def _():
            for o in range(2):
                right_item(c, o, 2 * c + o).start()

        @pl.when(z == 3)
        def _():
            for o in range(2):
                left_item(c, o, 2 * c + o).start()

        @pl.when(inner)
        def _():
            right_item(c // 2, c % 2, c).start()
            left_item(c // 2, c % 2, c).start()

    row_core = lax.broadcasted_iota(jnp.int32, (trow, width), 0) // tp

    def stage_a(c, chip):
        lanes = lanes_of(c)
        d = pl.ds(pl.multiple_of(chip * 2 * trow, 2 * trow), 2 * trow)
        a = dot(hid[d, :], s[c]) * scale
        for w in range(2):
            p = w + e - 2 * w * e
            y = piece[c, pl.ds(pl.multiple_of(p * tp, tp), tp), :].astype(F32)
            y = jnp.concatenate([y, y], axis=0)
            aw = a[w * trow:(w + 1) * trow] - jnp.where(jnp.logical_and(row_core == e, chip == yl), y, 0.0)
            if w == 0:
                pown[...] = aw
            else:
                tok[block(chip * 2 + 1), lanes] = aw.astype(BF16)
        c_p(c, chip).start()

    def stage_b(c, chip):
        c_p(c, chip).wait_recv()
        lanes = lanes_of(c)

        def one(i, _):
            other = r2[4 + c // 3, block((c % 3) * 2 + chip, i * 64, 64), :]
            mine = pown[pl.ds(pl.multiple_of(i * 64, 64), 64), :]
            tok[block(2 * chip, i * 64, 64), lanes] = (mine + other.astype(F32)).astype(BF16)
            return 0

        lax.fori_loop(0, trow // 64, one, 0)

    def stage_c(c):
        for chip in range(2):
            c_q(c, chip).wait_recv()
        lanes = lanes_of(c)

        def one(i, _):
            for chip in range(2):
                o = block(chip, i * 64, 64)
                mine = tok[block(2 * chip, i * 64, 64), lanes]
                qrx[c, o, :] = (qrx[c, o, :].astype(F32) + mine.astype(F32)).astype(BF16)
            return 0

        lax.fori_loop(0, trow // 64, one, 0)
        c_r(c).start()

    def stage_d(c):
        c_r(c).wait_recv()

        def one(i, _):
            d = pl.ds(pl.multiple_of(i * GRAD_ROWS, GRAD_ROWS), GRAD_ROWS)
            g = dot(r2[0, d, :], qrx[c, :trow, :])
            g += dot(r2[1, d, :], rrx[c, :trow, :])
            g += dot(r2[2, d, :], qrx[c, trow:, :])
            g += dot(r2[3, d, :], rrx[c, trow:, :])
            s[c, d, :] = (s[c, d, :].astype(F32) - (LEARN_RATE * scale) * g).astype(BF16)
            return 0

        lax.fori_loop(0, rows // GRAD_ROWS, one, 0)
        early(c)

    for p in range(2):
        own_in(p).wait()
    for j in range(rows // width):
        up_a(j).wait()
        up_b(j).wait()
    for p in range(2):
        t_core(p).wait_recv()
    hidden(2 * yl, 2)
    for c in range(slabs):
        w_in(c).wait()
        t_in(c).wait()

    def own_step(i, _):
        when(i >= 1, lambda: stage_b(i - 1, yl))
        when(jnp.logical_and(i >= 1, i <= jnp.where(inner, HEAD_IN, HEAD)), lambda: c_q(i - 1, yl).start())
        when(jnp.logical_and(i > HEAD, outer), lambda: relay_out(i - 1).start())
        when(i < slabs, lambda: stage_a(i, yl))
        return 0

    lax.fori_loop(0, slabs + 1, own_step, 0)
    for p in range(2):
        t_mate(p).wait_recv()
        t_fwd(p).start()
        t_fwd(p).wait_recv()
        hidden(2 * (1 - yl) + which(p, e), 1)
    for p in range(2):
        t_fwd(p).wait_send()

    def other_step(i, _):
        when(jnp.logical_and(i >= 1, i <= slabs), lambda: stage_b(i - 1, 1 - yl),
             lambda: c_q(i - 1, 1 - yl).start())

        @pl.when(jnp.logical_and(i == RELAY_AT, inner))
        def _():
            for k in range(slabs - HEAD):
                relay_out(HEAD + k).wait_recv()
                relay_on(k).start()

        when(jnp.logical_and(jnp.logical_and(i >= 1, i <= slabs - HEAD_IN), inner),
             lambda: c_q(i - 1 + HEAD_IN, yl).start())
        when(jnp.logical_and(i == slabs, z == 3), lambda: put(0, range(WRAP_DEPTH)))
        when(jnp.logical_and(i == slabs, z == 0), lambda: put(1, range(WRAP_DEPTH)))
        behind = i - jnp.where(inner, LAG[0], LAG[1])
        due = jnp.logical_and(behind >= 0, behind < slabs)
        when(due, lambda: stage_c(behind))
        when(i < slabs, lambda: stage_a(i, 1 - yl))
        when(due, lambda: stage_d(behind))
        return 0

    lax.fori_loop(0, slabs + LAG[1], other_step, 0)

    BR = 64

    def over(i, body):
        c, _ = item(i)
        lo = (i % 2) * cr

        def one(k, _):
            body(c, pl.ds(pl.multiple_of(lo + k * BR, BR), BR))
            return 0

        lax.fori_loop(0, cr // BR, one, 0)

    def first(i):
        def body(c, d):
            a = s[c, d, :].astype(F32)
            p = l1[c, d, :].astype(F32)
            q = r1[c, d, :].astype(F32)
            l1[c, d, :] = (m[0][0] * a + m[0][1] * p + m[0][2] * q).astype(BF16)
            r1[c, d, :] = (wb * a + wl * p + wr * q).astype(BF16)
        over(i, body)

    def mixed(c, d):
        a = l1[c, d, :].astype(F32)
        p = l2[c, d, :].astype(F32)
        q = r2[c, d, :].astype(F32)
        return m[1][0] * a + m[1][1] * p + m[1][2] * q

    def o_copy(i):
        c, d = item(i)
        return pltpu.make_async_copy(l2.at[c, d], out.at[0, d, pl.ds(c * width, width)], os.at[i])

    def second(i):
        def inside(c, d):
            l2[c, d, :] = (mixed(c, d) - avg[c, d, :].astype(F32)).astype(BF16)

        def outside(c, d):
            l2[c, d, :] = mixed(c, d).astype(BF16)

        when(inner, lambda: over(i, inside))
        when(jnp.logical_not(inner), lambda: over(i, outside))
        o_copy(i).start()

    unmix = 4.0 / jnp.where(z == 1, n(1, kl, 2), n(1, kr, 1))

    def outward(i):
        g = (i % chunks) // 2
        if i % 2 == 0:
            for j in (1, 2, 3):
                a_rs(g, j).wait_send()

        def body(c, d):
            r1[c, d, :] = (l1[c, d, :].astype(F32) - unmix * avg[c, d, :].astype(F32)).astype(BF16)

        over(i, body)

    def own(g, xx, lo, size):
        return (g, pl.ds(pl.multiple_of(xx * quarter + lo, 32), size))

    def a_rs(g, j):
        xx = (x + j) % 4
        return send(r1.at[own(g, xx, 0, quarter)], rsx.at[j - 1, g % RING],
                    xs.at[g, j - 1], xr.at[g, j - 1], at(xx, yh, z))

    def a_y(g):
        return send(piece.at[g, pl.ds(pl.multiple_of((1 - yh) * half, 32), half)],
                    yrx.at[g], ys.at[0, g], yr.at[0, g], ydev)

    def a_z(g):
        return send(piece.at[g, pl.ds(pl.multiple_of(yh * half, 32), half)],
                    zrx.at[g], zs.at[g], zr.at[g], zdev)

    def a_yg(g):
        ref = avg.at[own(g, x, yh * half, half)]
        return send(ref, ref, ys.at[1, g], yr.at[1, g], ydev)

    def a_x(g, k):
        if k == 0:
            ref, to = avg.at[own(g, x, 0, quarter)], xp
        elif k == 1:
            ref, to = avg.at[own(g, x, 0, quarter)], xm
        elif k == 2:
            ref, to = avg.at[own(g, (x + 3) % 4, 0, half)], xp
        else:
            ref, to = avg.at[own(g, (x + 1) % 4, half, half)], xm
        return send(ref, ref, as_.at[g, k], ar.at[g, k], to)


    def e_rs(g):
        if g >= RING:
            pl.semaphore_wait(free.at[g - RING], 3)
        for j in (1, 2, 3):
            a_rs(g, j).start()

    def e_y(g):
        for j in (1, 2, 3):
            a_rs(g, j).wait_recv()
        def one(i, _):
            d = pl.ds(pl.multiple_of(i * 64, 64), 64)
            o = pl.ds(pl.multiple_of(x * quarter + i * 64, 64), 64)
            t = r1[g, o, :].astype(F32)
            for j in range(3):
                t += rsx[j, g % RING, d, :].astype(F32)
            piece[g, d, :] = t.astype(BF16)
            return 0

        lax.fori_loop(0, quarter // 64, one, 0)
        if g < groups - RING:
            for j in (1, 2, 3):
                pl.semaphore_signal(free.at[g], inc=1, device_id=at((x + j) % 4, yh, z), device_id_type=MESH)
        a_y(g).start()

    def add_half(g, other, final):
        def one(i, _):
            d = pl.ds(pl.multiple_of(i * 32, 32), 32)
            o = pl.ds(pl.multiple_of(yh * half + i * 32, 32), 32)
            t = piece[g, o, :].astype(F32) + other[g, d, :].astype(F32)
            if final:
                p = pl.ds(pl.multiple_of(x * quarter + yh * half + i * 32, 32), 32)
                avg[g, p, :] = (t * (1.0 / NW)).astype(BF16)
            else:
                piece[g, o, :] = t.astype(BF16)
            return 0

        lax.fori_loop(0, half // 32, one, 0)

    def e_z(g):
        a_y(g).wait_recv()
        add_half(g, yrx, False)
        a_z(g).start()

    def e_yg(g):
        a_z(g).wait_recv()
        add_half(g, zrx, True)
        a_yg(g).start()

    def e_x0(g):
        a_yg(g).wait_recv()
        a_x(g, 0).start()
        a_x(g, 1).start()

    def e_x1(g):
        a_x(g, 0).wait_recv()
        a_x(g, 1).wait_recv()
        a_x(g, 2).start()
        a_x(g, 3).start()

    def e_x2(g):
        a_x(g, 2).wait_recv()
        a_x(g, 3).wait_recv()

    inside = {}
    for g in range(groups):
        for f, lag in zip((e_rs, e_y, e_z, e_yg, e_x0, e_x1, e_x2), LAGS):
            inside.setdefault(2 * g + 1 + lag, []).append(functools.partial(f, g))
    jit, wrap, bulk = {}, {}, {}
    for i in range(slabs, 2 * chunks):
        jit.setdefault(i - 3 if i < chunks else max(i - 3, chunks - 2), []).append(i)
    for i in range(WRAP_DEPTH, 2 * chunks):
        wrap.setdefault(i - WRAP_DEPTH, []).append(i)
    for i in range(chunks, 2 * chunks):
        bulk.setdefault(max(i - chunks, slabs), []).append(i)

    def issue(slot):
        if slot in jit:
            @pl.when(inner)
            def _():
                for i in jit[slot]:
                    if i >= chunks:
                        outward(i)
            when(z == 1, lambda: put(0, jit[slot]), lambda: put(1, jit[slot], r1))
            when(z == 2, lambda: put(1, jit[slot]), lambda: put(0, jit[slot], r1))
        when(z == 3, lambda: put(0, wrap.get(slot, ())), lambda: put(1, bulk.get(slot, ())))
        when(z == 0, lambda: put(1, wrap.get(slot, ())), lambda: put(0, bulk.get(slot, ())))

    for slot in range(2 * chunks):
        for cp in items(slot):
            cp().wait_recv()
        if slot < chunks:
            first(slot)
        else:
            second(slot)
        if slot in inside:
            when(inner, *inside[slot])
        issue(slot)

    for p in range(2):
        t_core(p).wait_send()
        t_mate(p).wait_send()
    for c in range(slabs):
        for chip in range(2):
            c_p(c, chip).wait_send()
            c_q(c, chip).wait_send()
        c_r(c).wait_send()
    for i in range(2 * chunks):
        for cp in items(i):
            cp().wait_send()

    @pl.when(inner)
    def _():
        for g in range(groups):
            for f in (a_y, a_z, a_yg):
                f(g).wait_send()
            if g < slabs - HEAD:
                relay_on(g).wait_send()
            for k in range(4):
                a_x(g, k).wait_send()

    for i in range(chunks, 2 * chunks):
        o_copy(i).wait()


def copy_kernel(src, dst, held, isem, osem):
    parts = held.shape[0]
    size = src.shape[1] // parts

    def move(i, back):
        there = pl.ds(i * size, size)
        if back:
            return pltpu.make_async_copy(held.at[i], dst.at[0, there], osem.at[i])
        return pltpu.make_async_copy(src.at[0, there], held.at[i], isem.at[i])

    for i in range(parts):
        move(i, False).start()
    for i in range(parts):
        move(i, False).wait()
        move(i, True).start()
    for i in range(parts):
        move(i, True).wait()


def copy_call(a):
    parts = 14
    any_ = pl.BlockSpec(memory_space=pl.ANY)
    return pl.pallas_call(
        copy_kernel,
        out_shape=jax.ShapeDtypeStruct(a.shape, a.dtype),
        in_specs=[any_],
        out_specs=any_,
        scratch_shapes=[pltpu.VMEM((parts, a.shape[1] // parts, a.shape[2]), a.dtype),
                        pltpu.SemaphoreType.DMA((parts,)), pltpu.SemaphoreType.DMA((parts,))],
        compiler_params=pltpu.CompilerParams(vmem_limit_bytes=67_043_328),
        name="place",
    )(a)


def body(tokens, targets, up_weight, down_weight, mix_numer):
    rows, dim = down_weight.shape[1:]
    slabs = 8
    width = dim // slabs
    trow = tokens.shape[0]
    D = pltpu.SemaphoreType.DMA
    vm = lambda *shape: pltpu.VMEM(shape, BF16)
    any_ = pl.BlockSpec(memory_space=pl.ANY)
    return copy_call(pl.pallas_call(
        kernel,
        out_shape=jax.ShapeDtypeStruct(down_weight.shape, BF16),
        in_specs=[pl.BlockSpec(memory_space=pltpu.SMEM)] + [any_] * 4,
        out_specs=any_,
        scratch_shapes=[vm(slabs, rows, width)] * 6 + [
            vm(3, RING, rows // 4, width), vm(slabs, rows // 4, width),
            vm(slabs, rows // 8, width), vm(slabs, rows // 8, width),
            vm(4 * trow, dim), vm(4 * trow, rows),
            vm(slabs, 2 * trow, width), vm(slabs, 2 * trow, width),
            pltpu.VMEM((trow, width), F32), vm(slabs - HEAD, trow, width), D((slabs - HEAD,)), D((slabs - HEAD,)),
            D((5, slabs)), D((3, 2)), D((3, 2)),
            D((slabs, 2)), D((slabs, 2)), D((slabs, 2)), D((slabs, 2)), D((slabs,)), D((slabs,)),
            D((2, 4 * slabs)), D((2, 4 * slabs)), D((slabs, 3)), D((slabs, 3)), D((slabs, 4)), D((slabs, 4)),
            D((2, slabs)), D((2, slabs)), D((slabs,)), D((slabs,)), D((4 * slabs,)),
            pltpu.SemaphoreType.REGULAR((slabs - RING,)),
        ],
        compiler_params=pltpu.CompilerParams(
            collective_id=0, has_side_effects=True, vmem_limit_bytes=67_043_328),
        name="gossip",
    )(mix_numer, tokens, targets, up_weight, down_weight))


def solution(mesh):
    in_specs = (P(("blk", "shard"), None), P(("blk", "shard"), None), P(None, "shard"), P("blk", "shard", None), P())
    return jax.shard_map(body, mesh=mesh, in_specs=in_specs, out_specs=P("blk", "shard", None), check_vma=False)
```

```python
import functools

import jax
import jax.numpy as jnp
from jax import lax
from jax.experimental import pallas as pl
from jax.experimental.pallas import tpu as pltpu
from jax.sharding import PartitionSpec as P

MESH = pl.DeviceIdType.MESH
LEARN_RATE = 2.0
NW = 32
GRAD_ROWS = 896
HEAD = 4
RELAY_AT = 3
LAG = (2, 4)
HEAD_IN = 4
PAIR = 2
LIM = 67_043_328 - 7_800_000
RING = 4
LAGS = (0, 2, 3, 6, 7, 8, 9)
WRAP_DEPTH = 3
F32 = jnp.float32
BF16 = jnp.bfloat16


def dot(a, b):
    return jnp.dot(a, b, preferred_element_type=F32)


def kernel(numer, tokens, targets, up, weight, l2,
           s, l1, r1, r2, avg, rsx, piece, yrx, zrx, tok, hid, qrx, rrx, pown, rel, rels, relr,
           ls, ts, tr, ps, pr, qs, qr, rs, rr,
           gs, gr, xs, xr, as_, ar, ys, yr, zs, zr, free):
    b, sh = lax.axis_index("blk"), lax.axis_index("shard")
    x, yh, z = b // 8, (b // 4) % 2, b % 4
    yl, e = sh // 2, sh % 2
    slabs, rows, width = s.shape
    chunks, cr = 2 * slabs, rows // 2
    ff, dim = 4 * rows, slabs * width
    groups = slabs
    quarter, half = rows // 4, rows // 8
    trow = tokens.shape[0]
    tp = trow // 2

    def at(xx, yy, zz):
        return (xx * 8 + yy * 4 + zz, sh)

    left, right = ((b + 31) % 32, sh), ((b + 1) % 32, sh)
    core, mate = (b, 2 * yl + 1 - e), (b, 2 * (1 - yl) + e)
    ydev = at(x, 1 - yh, z)
    zdev = at(x, yh, 3 - z)
    xp, xm = at((x + 1) % 4, yh, z), at((x + 3) % 4, yh, z)
    inner = jnp.logical_or(z == 1, z == 2)
    outer = jnp.logical_not(inner)
    beside = (b + jnp.where(z % 2 == 0, 1, 31)) % 32

    def send(src, dst, ss, rsem, dev):
        return pltpu.make_async_remote_copy(src, dst, ss, rsem, device_id=dev, device_id_type=MESH)

    def when(cond, *fs):
        @pl.when(cond)
        def _():
            for f in fs:
                f()

    def up_a(j):
        return pltpu.make_async_copy(up.at[pl.ds(0, rows), pl.ds(j * width, width)], l2.at[j], ls.at[0, j])

    def up_b(j):
        return pltpu.make_async_copy(up.at[pl.ds(rows, dim - rows), pl.ds(j * width, width)],
                                     l2.at[slabs - 1, pl.ds(j * width, width)], ls.at[1, j])

    def w_in(c):
        return pltpu.make_async_copy(weight.at[0, :, pl.ds(c * width, width)], s.at[c], ls.at[2, c])

    def t_in(c):
        return pltpu.make_async_copy(targets.at[:, pl.ds(c * width, width)], piece.at[c, pl.ds(0, trow)], ls.at[3, c])

    def which(p, core_at):
        return p + core_at - 2 * p * core_at

    def spot(p, chip, core_from, core_at):
        at_row = (chip * 2 + which(p, core_at)) * trow + core_from * tp
        return pl.ds(pl.multiple_of(at_row, tp), tp)

    def own_in(p):
        return pltpu.make_async_copy(tokens.at[pl.ds(p * tp, tp)], tok.at[spot(p, yl, e, e)], ls.at[4, p])

    def t_core(p):
        return send(tokens.at[pl.ds(p * tp, tp)], tok.at[spot(p, yl, e, 1 - e)], ts.at[0, p], tr.at[0, p], core)

    def t_mate(p):
        return send(tokens.at[pl.ds(p * tp, tp)], tok.at[spot(p, yl, e, e)], ts.at[1, p], tr.at[1, p], mate)

    def t_fwd(p):
        return send(tok.at[spot(p, 1 - yl, e, e)], tok.at[spot(p, 1 - yl, e, 1 - e)], ts.at[2, p], tr.at[2, p], core)

    barrier = pltpu.get_barrier_semaphore()
    for dev in (core, mate, left, right, (beside, mate[1])):
        pl.semaphore_signal(barrier, inc=1, device_id=dev, device_id_type=MESH)

    @pl.when(inner)
    def _():
        for dev in (xp, at((x + 2) % 4, yh, z), xm, ydev):
            pl.semaphore_signal(barrier, inc=1, device_id=dev, device_id_type=MESH)

    for p in range(2):
        own_in(p).start()
    for j in range(rows // width):
        up_a(j).start()
        up_b(j).start()

    pl.semaphore_wait(barrier, jnp.where(inner, 9, 5))

    for p in range(2):
        t_mate(p).start()
    for p in range(2):
        t_core(p).start()
    for c in range(slabs):
        w_in(c).start()
        t_in(c).start()

    def n(r, k, j):
        return numer[r, k, j].astype(F32)

    kl, kr, kll, krr = (b + 31) % 32, (b + 1) % 32, (b + 30) % 32, (b + 2) % 32

    def v(k0, k, k1):
        return n(1, k, 0) + n(1, k1, 1) + n(1, k0, 2)

    vb, vl, vr = v(kl, b, kr), v(kll, kl, b), v(b, kr, krr)
    vll, vrr = v((b + 29) % 32, kll, kl), v(kr, krr, (b + 3) % 32)
    wb = (n(0, b, 0) * vb + n(0, kr, 1) * vr + n(0, kl, 2) * vl) * (1.0 / 16)
    wl = (n(0, kl, 0) * vl + n(0, b, 1) * vb + n(0, kll, 2) * vll) * (1.0 / 16)
    wr = (n(0, kr, 0) * vr + n(0, krr, 1) * vrr + n(0, b, 2) * vb) * (1.0 / 16)
    wl = jnp.where(z == 1, wl, 0.0)
    wr = jnp.where(z == 2, wr, 0.0)
    m = [[n(r, b, j) * 0.25 for j in range(3)] for r in range(2)]

    def hidden(t, size):
        d = pl.ds(pl.multiple_of(t * trow, trow), size * trow)

        def tiles(j, many):
            at_j = [j + k for k in range(many)]
            lanes = [pl.ds(pl.multiple_of(jj * width, width), width) for jj in at_j]
            above = jnp.concatenate([l2[jj] for jj in at_j], axis=1)
            below = jnp.concatenate([l2[slabs - 1, n, :] for n in lanes], axis=1)
            a = dot(tok[d, :rows], above) + dot(tok[d, rows:], below)
            h = (a / (1.0 + jnp.exp(-a))).astype(BF16)
            for i, n in enumerate(lanes):
                hh = h[:, i * width:(i + 1) * width]
                hid[d, n] = hh
                for k in range(size):
                    r2[t + k, n, :] = hh[k * trow:(k + 1) * trow].T

        many = PAIR if size == 1 else 1
        whole = rows // width // many

        def one(j, _):
            tiles(j * many, many)
            return 0

        lax.fori_loop(0, whole, one, 0)
        for j in range(whole * many, rows // width):
            tiles(j, 1)

    scale = ff ** -0.5

    def lanes_of(c):
        return pl.ds(pl.multiple_of(c * width, width), width)

    def block(lo, i=0, size=None):
        return pl.ds(pl.multiple_of(lo * trow + i, 64), trow if size is None else size)

    def c_p(c, chip):
        return send(tok.at[block(2 * chip + 1), lanes_of(c)], r2.at[4 + c // 3, block((c % 3) * 2 + chip)],
                    ps.at[c, chip], pr.at[c, chip], core)

    def c_q(c, chip):
        return send(tok.at[block(2 * chip), lanes_of(c)], qrx.at[c, block(chip)], qs.at[c, chip], qr.at[c, chip], mate)

    def relay_out(c):
        return send(tok.at[block(2 * yl), lanes_of(c)], rel.at[c - HEAD], qs.at[c, yl], relr.at[c - HEAD],
                    (beside, sh))

    def relay_on(k):
        return send(rel.at[k], qrx.at[HEAD + k, block(yl)], rels.at[k], qr.at[HEAD + k, yl], (beside, mate[1]))

    def c_r(c):
        return send(qrx.at[c], rrx.at[c], rs.at[c], rr.at[c], core)

    def item(i):
        c, o = (i % chunks) // 2, i % 2
        d = pl.ds(o * cr, cr)
        return c, d

    def items(i, later=None):
        c, d = item(i)
        src, dl, dr = (s, l1, r1) if i < chunks else (l1 if later is None else later, l2, r2)
        return (lambda: send(src.at[c, d], dl.at[c, d], gs.at[0, i], gr.at[0, i], right),
                lambda: send(src.at[c, d], dr.at[c, d], gs.at[1, i], gr.at[1, i], left))

    def put(direction, those, later=None):
        for i in those:
            items(i, later)[direction]().start()

    def right_item(c, o, i):
        d = pl.ds(o * cr if isinstance(o, int) else pl.multiple_of(o * cr, cr), cr)
        return send(s.at[c, d], l1.at[c, d], gs.at[0, i], gr.at[0, i], right)

    def left_item(c, o, i):
        d = pl.ds(o * cr if isinstance(o, int) else pl.multiple_of(o * cr, cr), cr)
        return send(s.at[c, d], r1.at[c, d], gs.at[1, i], gr.at[1, i], left)

    def early(c):
        @pl.when(z == 0)
        def _():
            for o in range(2):
                right_item(c, o, 2 * c + o).start()

        @pl.when(z == 3)
        def _():
            for o in range(2):
                left_item(c, o, 2 * c + o).start()

        @pl.when(inner)
        def _():
            right_item(c // 2, c % 2, c).start()
            left_item(c // 2, c % 2, c).start()

    row_core = lax.broadcasted_iota(jnp.int32, (trow, width), 0) // tp

    def stage_a(c, chip):
        lanes = lanes_of(c)
        d = pl.ds(pl.multiple_of(chip * 2 * trow, 2 * trow), 2 * trow)
        a = dot(hid[d, :], s[c]) * scale
        for w in range(2):
            p = w + e - 2 * w * e
            y = piece[c, pl.ds(pl.multiple_of(p * tp, tp), tp), :].astype(F32)
            y = jnp.concatenate([y, y], axis=0)
            aw = a[w * trow:(w + 1) * trow] - jnp.where(jnp.logical_and(row_core == e, chip == yl), y, 0.0)
            if w == 0:
                pown[...] = aw
            else:
                tok[block(chip * 2 + 1), lanes] = aw.astype(BF16)
        c_p(c, chip).start()

    def stage_b(c, chip):
        c_p(c, chip).wait_recv()
        lanes = lanes_of(c)

        def one(i, _):
            other = r2[4 + c // 3, block((c % 3) * 2 + chip, i * 64, 64), :]
            mine = pown[pl.ds(pl.multiple_of(i * 64, 64), 64), :]
            tok[block(2 * chip, i * 64, 64), lanes] = (mine + other.astype(F32)).astype(BF16)
            return 0

        lax.fori_loop(0, trow // 64, one, 0)

    def stage_c(c):
        for chip in range(2):
            c_q(c, chip).wait_recv()
        lanes = lanes_of(c)

        def one(i, _):
            for chip in range(2):
                o = block(chip, i * 64, 64)
                mine = tok[block(2 * chip, i * 64, 64), lanes]
                qrx[c, o, :] = (qrx[c, o, :].astype(F32) + mine.astype(F32)).astype(BF16)
            return 0

        lax.fori_loop(0, trow // 64, one, 0)
        c_r(c).start()

    def stage_d(c):
        c_r(c).wait_recv()

        def one(i, _):
            d = pl.ds(pl.multiple_of(i * GRAD_ROWS, GRAD_ROWS), GRAD_ROWS)
            g = dot(r2[0, d, :], qrx[c, :trow, :])
            g += dot(r2[1, d, :], rrx[c, :trow, :])
            g += dot(r2[2, d, :], qrx[c, trow:, :])
            g += dot(r2[3, d, :], rrx[c, trow:, :])
            s[c, d, :] = (s[c, d, :].astype(F32) - (LEARN_RATE * scale) * g).astype(BF16)
            return 0

        lax.fori_loop(0, rows // GRAD_ROWS, one, 0)
        early(c)

    for p in range(2):
        own_in(p).wait()
    for j in range(rows // width):
        up_a(j).wait()
        up_b(j).wait()
    for p in range(2):
        t_core(p).wait_recv()
    hidden(2 * yl, 2)
    for c in range(slabs):
        w_in(c).wait()
        t_in(c).wait()

    def own_step(i, _):
        when(i >= 1, lambda: stage_b(i - 1, yl))
        when(jnp.logical_and(i >= 1, i <= jnp.where(inner, HEAD_IN, HEAD)), lambda: c_q(i - 1, yl).start())
        when(jnp.logical_and(i > HEAD, outer), lambda: relay_out(i - 1).start())
        when(i < slabs, lambda: stage_a(i, yl))
        return 0

    lax.fori_loop(0, slabs + 1, own_step, 0)
    for p in range(2):
        t_mate(p).wait_recv()
        t_fwd(p).start()
        t_fwd(p).wait_recv()
        hidden(2 * (1 - yl) + which(p, e), 1)
    for p in range(2):
        t_fwd(p).wait_send()

    def other_step(i, _):
        when(jnp.logical_and(i >= 1, i <= slabs), lambda: stage_b(i - 1, 1 - yl),
             lambda: c_q(i - 1, 1 - yl).start())

        @pl.when(jnp.logical_and(i == RELAY_AT, inner))
        def _():
            for k in range(slabs - HEAD):
                relay_out(HEAD + k).wait_recv()
                relay_on(k).start()

        when(jnp.logical_and(jnp.logical_and(i >= 1, i <= slabs - HEAD_IN), inner),
             lambda: c_q(i - 1 + HEAD_IN, yl).start())
        when(jnp.logical_and(i == slabs, z == 3), lambda: put(0, range(WRAP_DEPTH)))
        when(jnp.logical_and(i == slabs, z == 0), lambda: put(1, range(WRAP_DEPTH)))
        behind = i - jnp.where(inner, LAG[0], LAG[1])
        due = jnp.logical_and(behind >= 0, behind < slabs)
        when(due, lambda: stage_c(behind))
        when(i < slabs, lambda: stage_a(i, 1 - yl))
        when(due, lambda: stage_d(behind))
        return 0

    lax.fori_loop(0, slabs + LAG[1], other_step, 0)

    BR = 64

    def over(i, body):
        c, _ = item(i)
        lo = (i % 2) * cr

        def one(k, _):
            body(c, pl.ds(pl.multiple_of(lo + k * BR, BR), BR))
            return 0

        lax.fori_loop(0, cr // BR, one, 0)

    def first(i):
        def body(c, d):
            a = s[c, d, :].astype(F32)
            p = l1[c, d, :].astype(F32)
            q = r1[c, d, :].astype(F32)
            l1[c, d, :] = (m[0][0] * a + m[0][1] * p + m[0][2] * q).astype(BF16)
            r1[c, d, :] = (wb * a + wl * p + wr * q).astype(BF16)
        over(i, body)

    def mixed(c, d):
        a = l1[c, d, :].astype(F32)
        p = l2[c, d, :].astype(F32)
        q = r2[c, d, :].astype(F32)
        return m[1][0] * a + m[1][1] * p + m[1][2] * q

    def second(i):
        def inside(c, d):
            l2[c, d, :] = (mixed(c, d) - avg[c, d, :].astype(F32)).astype(BF16)

        def outside(c, d):
            l2[c, d, :] = mixed(c, d).astype(BF16)

        when(inner, lambda: over(i, inside))
        when(jnp.logical_not(inner), lambda: over(i, outside))

    unmix = 4.0 / jnp.where(z == 1, n(1, kl, 2), n(1, kr, 1))

    def outward(i):
        g = (i % chunks) // 2
        if i % 2 == 0:
            for j in (1, 2, 3):
                a_rs(g, j).wait_send()

        def body(c, d):
            r1[c, d, :] = (l1[c, d, :].astype(F32) - unmix * avg[c, d, :].astype(F32)).astype(BF16)

        over(i, body)

    def own(g, xx, lo, size):
        return (g, pl.ds(pl.multiple_of(xx * quarter + lo, 32), size))

    def a_rs(g, j):
        xx = (x + j) % 4
        return send(r1.at[own(g, xx, 0, quarter)], rsx.at[j - 1, g % RING],
                    xs.at[g, j - 1], xr.at[g, j - 1], at(xx, yh, z))

    def a_y(g):
        return send(piece.at[g, pl.ds(pl.multiple_of((1 - yh) * half, 32), half)],
                    yrx.at[g], ys.at[0, g], yr.at[0, g], ydev)

    def a_z(g):
        return send(piece.at[g, pl.ds(pl.multiple_of(yh * half, 32), half)],
                    zrx.at[g], zs.at[g], zr.at[g], zdev)

    def a_yg(g):
        ref = avg.at[own(g, x, yh * half, half)]
        return send(ref, ref, ys.at[1, g], yr.at[1, g], ydev)

    def a_x(g, k):
        if k == 0:
            ref, to = avg.at[own(g, x, 0, quarter)], xp
        elif k == 1:
            ref, to = avg.at[own(g, x, 0, quarter)], xm
        elif k == 2:
            ref, to = avg.at[own(g, (x + 3) % 4, 0, half)], xp
        else:
            ref, to = avg.at[own(g, (x + 1) % 4, half, half)], xm
        return send(ref, ref, as_.at[g, k], ar.at[g, k], to)


    def e_rs(g):
        if g >= RING:
            pl.semaphore_wait(free.at[g - RING], 3)
        for j in (1, 2, 3):
            a_rs(g, j).start()

    def e_y(g):
        for j in (1, 2, 3):
            a_rs(g, j).wait_recv()
        def one(i, _):
            d = pl.ds(pl.multiple_of(i * 64, 64), 64)
            o = pl.ds(pl.multiple_of(x * quarter + i * 64, 64), 64)
            t = r1[g, o, :].astype(F32)
            for j in range(3):
                t += rsx[j, g % RING, d, :].astype(F32)
            piece[g, d, :] = t.astype(BF16)
            return 0

        lax.fori_loop(0, quarter // 64, one, 0)
        if g < groups - RING:
            for j in (1, 2, 3):
                pl.semaphore_signal(free.at[g], inc=1, device_id=at((x + j) % 4, yh, z), device_id_type=MESH)
        a_y(g).start()

    def add_half(g, other, final):
        def one(i, _):
            d = pl.ds(pl.multiple_of(i * 32, 32), 32)
            o = pl.ds(pl.multiple_of(yh * half + i * 32, 32), 32)
            t = piece[g, o, :].astype(F32) + other[g, d, :].astype(F32)
            if final:
                p = pl.ds(pl.multiple_of(x * quarter + yh * half + i * 32, 32), 32)
                avg[g, p, :] = (t * (1.0 / NW)).astype(BF16)
            else:
                piece[g, o, :] = t.astype(BF16)
            return 0

        lax.fori_loop(0, half // 32, one, 0)

    def e_z(g):
        a_y(g).wait_recv()
        add_half(g, yrx, False)
        a_z(g).start()

    def e_yg(g):
        a_z(g).wait_recv()
        add_half(g, zrx, True)
        a_yg(g).start()

    def e_x0(g):
        a_yg(g).wait_recv()
        a_x(g, 0).start()
        a_x(g, 1).start()

    def e_x1(g):
        a_x(g, 0).wait_recv()
        a_x(g, 1).wait_recv()
        a_x(g, 2).start()
        a_x(g, 3).start()

    def e_x2(g):
        a_x(g, 2).wait_recv()
        a_x(g, 3).wait_recv()

    inside = {}
    for g in range(groups):
        for f, lag in zip((e_rs, e_y, e_z, e_yg, e_x0, e_x1, e_x2), LAGS):
            inside.setdefault(2 * g + 1 + lag, []).append(functools.partial(f, g))
    jit, wrap, bulk = {}, {}, {}
    for i in range(slabs, 2 * chunks):
        jit.setdefault(i - 3 if i < chunks else max(i - 3, chunks - 2), []).append(i)
    for i in range(WRAP_DEPTH, 2 * chunks):
        wrap.setdefault(i - WRAP_DEPTH, []).append(i)
    for i in range(chunks, 2 * chunks):
        bulk.setdefault(max(i - chunks, slabs), []).append(i)

    def issue(slot):
        if slot in jit:
            @pl.when(inner)
            def _():
                for i in jit[slot]:
                    if i >= chunks:
                        outward(i)
            when(z == 1, lambda: put(0, jit[slot]), lambda: put(1, jit[slot], r1))
            when(z == 2, lambda: put(1, jit[slot]), lambda: put(0, jit[slot], r1))
        when(z == 3, lambda: put(0, wrap.get(slot, ())), lambda: put(1, bulk.get(slot, ())))
        when(z == 0, lambda: put(1, wrap.get(slot, ())), lambda: put(0, bulk.get(slot, ())))

    for slot in range(2 * chunks):
        for cp in items(slot):
            cp().wait_recv()
        if slot < chunks:
            first(slot)
        else:
            second(slot)
        if slot in inside:
            when(inner, *inside[slot])
        issue(slot)

    for p in range(2):
        t_core(p).wait_send()
        t_mate(p).wait_send()
    for c in range(slabs):
        for chip in range(2):
            c_p(c, chip).wait_send()
            c_q(c, chip).wait_send()
        c_r(c).wait_send()
    for i in range(2 * chunks):
        for cp in items(i):
            cp().wait_send()

    @pl.when(inner)
    def _():
        for g in range(groups):
            for f in (a_y, a_z, a_yg):
                f(g).wait_send()
            if g < slabs - HEAD:
                relay_on(g).wait_send()
            for k in range(4):
                a_x(g, k).wait_send()


def copy_kernel(src, dst, sem):
    slabs, _, width = src.shape

    def move(i):
        return pltpu.make_async_copy(src.at[i], dst.at[0, :, pl.ds(i * width, width)], sem.at[i])

    for i in range(slabs):
        move(i).start()
    for i in range(slabs):
        move(i).wait()


def copy_call(a):
    slabs, rows, width = a.shape
    return pl.pallas_call(
        copy_kernel,
        out_shape=jax.ShapeDtypeStruct((1, rows, slabs * width), a.dtype),
        in_specs=[pl.BlockSpec(memory_space=pltpu.VMEM)],
        out_specs=pl.BlockSpec(memory_space=pl.ANY),
        scratch_shapes=[pltpu.SemaphoreType.DMA((slabs,))],
        compiler_params=pltpu.CompilerParams(vmem_limit_bytes=8 * 2**20),
        name="place",
    )(a)


def body(tokens, targets, up_weight, down_weight, mix_numer):
    rows, dim = down_weight.shape[1:]
    slabs = 8
    width = dim // slabs
    trow = tokens.shape[0]
    D = pltpu.SemaphoreType.DMA
    vm = lambda *shape: pltpu.VMEM(shape, BF16)
    any_ = pl.BlockSpec(memory_space=pl.ANY)
    return copy_call(pl.pallas_call(
        kernel,
        out_shape=pltpu.VMEM((slabs, rows, width), BF16),
        in_specs=[pl.BlockSpec(memory_space=pltpu.SMEM)] + [any_] * 4,
        out_specs=pl.BlockSpec(memory_space=pltpu.VMEM),
        scratch_shapes=[vm(slabs, rows, width)] * 5 + [
            vm(3, RING, rows // 4, width), vm(slabs, rows // 4, width),
            vm(slabs, rows // 8, width), vm(slabs, rows // 8, width),
            vm(4 * trow, dim), vm(4 * trow, rows),
            vm(slabs, 2 * trow, width), vm(slabs, 2 * trow, width),
            pltpu.VMEM((trow, width), F32), vm(slabs - HEAD, trow, width), D((slabs - HEAD,)), D((slabs - HEAD,)),
            D((5, slabs)), D((3, 2)), D((3, 2)),
            D((slabs, 2)), D((slabs, 2)), D((slabs, 2)), D((slabs, 2)), D((slabs,)), D((slabs,)),
            D((2, 4 * slabs)), D((2, 4 * slabs)), D((slabs, 3)), D((slabs, 3)), D((slabs, 4)), D((slabs, 4)),
            D((2, slabs)), D((2, slabs)), D((slabs,)), D((slabs,)),
            pltpu.SemaphoreType.REGULAR((slabs - RING,)),
        ],
        compiler_params=pltpu.CompilerParams(
            collective_id=0, has_side_effects=True, vmem_limit_bytes=LIM),
        name="gossip",
    )(mix_numer, tokens, targets, up_weight, down_weight))


def solution(mesh):
    in_specs = (P(("blk", "shard"), None), P(("blk", "shard"), None), P(None, "shard"), P("blk", "shard", None), P())
    return jax.shard_map(body, mesh=mesh, in_specs=in_specs, out_specs=P("blk", "shard", None), check_vma=False)
```

```python
import functools

import jax
import jax.numpy as jnp
from jax import lax
from jax.experimental import pallas as pl
from jax.experimental.pallas import tpu as pltpu
from jax.sharding import PartitionSpec as P

MESH = pl.DeviceIdType.MESH
LEARN_RATE = 2.0
NW = 32
GRAD_ROWS = 896
HEAD = 4
RELAY_AT = 3
LAG = (2, 4)
HEAD_IN = 4
PAIR = 2
LIM = 67_043_328 - 7_800_000
RING = 4
LAGS = (0, 2, 3, 6, 7, 8, 9)
WRAP_DEPTH = 3
F32 = jnp.float32
BF16 = jnp.bfloat16


def dot(a, b):
    return jnp.dot(a, b, preferred_element_type=F32)


def kernel(numer, tokens, targets, up, weight, l2,
           s, l1, r1, r2, avg, rsx, piece, yrx, zrx, tok, hid, qrx, rrx, pown, rel, rels, relr,
           ls, ts, tr, ps, pr, qs, qr, rs, rr,
           gs, gr, xs, xr, as_, ar, ys, yr, zs, zr, free):
    b, sh = lax.axis_index("blk"), lax.axis_index("shard")
    x, yh, z = b // 8, (b // 4) % 2, b % 4
    yl, e = sh // 2, sh % 2
    slabs, rows, width = s.shape
    chunks, cr = 2 * slabs, rows // 2
    ff, dim = 4 * rows, slabs * width
    groups = slabs
    quarter, half = rows // 4, rows // 8
    trow = tokens.shape[0]
    tp = trow // 2

    def at(xx, yy, zz):
        return (xx * 8 + yy * 4 + zz, sh)

    left, right = ((b + 31) % 32, sh), ((b + 1) % 32, sh)
    core, mate = (b, 2 * yl + 1 - e), (b, 2 * (1 - yl) + e)
    ydev = at(x, 1 - yh, z)
    zdev = at(x, yh, 3 - z)
    xp, xm = at((x + 1) % 4, yh, z), at((x + 3) % 4, yh, z)
    inner = jnp.logical_or(z == 1, z == 2)
    outer = jnp.logical_not(inner)
    beside = (b + jnp.where(z % 2 == 0, 1, 31)) % 32

    def send(src, dst, ss, rsem, dev):
        return pltpu.make_async_remote_copy(src, dst, ss, rsem, device_id=dev, device_id_type=MESH)

    def when(cond, *fs):
        @pl.when(cond)
        def _():
            for f in fs:
                f()

    def up_a(j):
        return pltpu.make_async_copy(up.at[pl.ds(0, rows), pl.ds(j * width, width)], l2.at[j], ls.at[0, j])

    def up_b(j):
        return pltpu.make_async_copy(up.at[pl.ds(rows, dim - rows), pl.ds(j * width, width)],
                                     l2.at[slabs - 1, pl.ds(j * width, width)], ls.at[1, j])

    def w_in(c):
        return pltpu.make_async_copy(weight.at[0, :, pl.ds(c * width, width)], s.at[c], ls.at[2, c])

    def t_in(c):
        return pltpu.make_async_copy(targets.at[:, pl.ds(c * width, width)], piece.at[c, pl.ds(0, trow)], ls.at[3, c])

    def which(p, core_at):
        return p + core_at - 2 * p * core_at

    def spot(p, chip, core_from, core_at):
        at_row = (chip * 2 + which(p, core_at)) * trow + core_from * tp
        return pl.ds(pl.multiple_of(at_row, tp), tp)

    def own_in(p):
        return pltpu.make_async_copy(tokens.at[pl.ds(p * tp, tp)], tok.at[spot(p, yl, e, e)], ls.at[4, p])

    def t_core(p):
        return send(tokens.at[pl.ds(p * tp, tp)], tok.at[spot(p, yl, e, 1 - e)], ts.at[0, p], tr.at[0, p], core)

    def t_mate(p):
        return send(tokens.at[pl.ds(p * tp, tp)], tok.at[spot(p, yl, e, e)], ts.at[1, p], tr.at[1, p], mate)

    def t_fwd(p):
        return send(tok.at[spot(p, 1 - yl, e, e)], tok.at[spot(p, 1 - yl, e, 1 - e)], ts.at[2, p], tr.at[2, p], core)

    barrier = pltpu.get_barrier_semaphore()
    for dev in (core, mate, left, right, (beside, mate[1])):
        pl.semaphore_signal(barrier, inc=1, device_id=dev, device_id_type=MESH)

    @pl.when(inner)
    def _():
        for dev in (xp, at((x + 2) % 4, yh, z), xm, ydev):
            pl.semaphore_signal(barrier, inc=1, device_id=dev, device_id_type=MESH)

    for p in range(2):
        own_in(p).start()
    for j in range(rows // width):
        up_a(j).start()
        up_b(j).start()

    pl.semaphore_wait(barrier, jnp.where(inner, 9, 5))

    for p in range(2):
        t_mate(p).start()
    for p in range(2):
        t_core(p).start()
    for c in range(slabs):
        w_in(c).start()
        t_in(c).start()

    def n(r, k, j):
        return numer[j, r, k].astype(F32)

    kl, kr, kll, krr = (b + 31) % 32, (b + 1) % 32, (b + 30) % 32, (b + 2) % 32

    def v(k0, k, k1):
        return n(1, k, 0) + n(1, k1, 1) + n(1, k0, 2)

    vb, vl, vr = v(kl, b, kr), v(kll, kl, b), v(b, kr, krr)
    vll, vrr = v((b + 29) % 32, kll, kl), v(kr, krr, (b + 3) % 32)
    wb = (n(0, b, 0) * vb + n(0, kr, 1) * vr + n(0, kl, 2) * vl) * (1.0 / 16)
    wl = (n(0, kl, 0) * vl + n(0, b, 1) * vb + n(0, kll, 2) * vll) * (1.0 / 16)
    wr = (n(0, kr, 0) * vr + n(0, krr, 1) * vrr + n(0, b, 2) * vb) * (1.0 / 16)
    wl = jnp.where(z == 1, wl, 0.0)
    wr = jnp.where(z == 2, wr, 0.0)
    m = [[n(r, b, j) * 0.25 for j in range(3)] for r in range(2)]

    def hidden(t, size):
        d = pl.ds(pl.multiple_of(t * trow, trow), size * trow)

        def tiles(j, many):
            at_j = [j + k for k in range(many)]
            lanes = [pl.ds(pl.multiple_of(jj * width, width), width) for jj in at_j]
            above = jnp.concatenate([l2[jj] for jj in at_j], axis=1)
            below = jnp.concatenate([l2[slabs - 1, n, :] for n in lanes], axis=1)
            a = dot(tok[d, :rows], above) + dot(tok[d, rows:], below)
            h = (a / (1.0 + jnp.exp(-a))).astype(BF16)
            for i, n in enumerate(lanes):
                hh = h[:, i * width:(i + 1) * width]
                hid[d, n] = hh
                for k in range(size):
                    r2[t + k, n, :] = hh[k * trow:(k + 1) * trow].T

        many = PAIR if size == 1 else 1
        whole = rows // width // many

        def one(j, _):
            tiles(j * many, many)
            return 0

        lax.fori_loop(0, whole, one, 0)
        for j in range(whole * many, rows // width):
            tiles(j, 1)

    scale = ff ** -0.5

    def lanes_of(c):
        return pl.ds(pl.multiple_of(c * width, width), width)

    def block(lo, i=0, size=None):
        return pl.ds(pl.multiple_of(lo * trow + i, 64), trow if size is None else size)

    def c_p(c, chip):
        return send(tok.at[block(2 * chip + 1), lanes_of(c)], r2.at[4 + c // 3, block((c % 3) * 2 + chip)],
                    ps.at[c, chip], pr.at[c, chip], core)

    def c_q(c, chip):
        return send(tok.at[block(2 * chip), lanes_of(c)], qrx.at[c, block(chip)], qs.at[c, chip], qr.at[c, chip], mate)

    def relay_out(c):
        return send(tok.at[block(2 * yl), lanes_of(c)], rel.at[c - HEAD], qs.at[c, yl], relr.at[c - HEAD],
                    (beside, sh))

    def relay_on(k):
        return send(rel.at[k], qrx.at[HEAD + k, block(yl)], rels.at[k], qr.at[HEAD + k, yl], (beside, mate[1]))

    def c_r(c):
        return send(qrx.at[c], rrx.at[c], rs.at[c], rr.at[c], core)

    def item(i):
        c, o = (i % chunks) // 2, i % 2
        d = pl.ds(o * cr, cr)
        return c, d

    def items(i, later=None):
        c, d = item(i)
        src, dl, dr = (s, l1, r1) if i < chunks else (l1 if later is None else later, l2, r2)
        return (lambda: send(src.at[c, d], dl.at[c, d], gs.at[0, i], gr.at[0, i], right),
                lambda: send(src.at[c, d], dr.at[c, d], gs.at[1, i], gr.at[1, i], left))

    def put(direction, those, later=None):
        for i in those:
            items(i, later)[direction]().start()

    def right_item(c, o, i):
        d = pl.ds(o * cr if isinstance(o, int) else pl.multiple_of(o * cr, cr), cr)
        return send(s.at[c, d], l1.at[c, d], gs.at[0, i], gr.at[0, i], right)

    def left_item(c, o, i):
        d = pl.ds(o * cr if isinstance(o, int) else pl.multiple_of(o * cr, cr), cr)
        return send(s.at[c, d], r1.at[c, d], gs.at[1, i], gr.at[1, i], left)

    def early(c):
        @pl.when(z == 0)
        def _():
            for o in range(2):
                right_item(c, o, 2 * c + o).start()

        @pl.when(z == 3)
        def _():
            for o in range(2):
                left_item(c, o, 2 * c + o).start()

        @pl.when(inner)
        def _():
            right_item(c // 2, c % 2, c).start()
            left_item(c // 2, c % 2, c).start()

    row_core = lax.broadcasted_iota(jnp.int32, (trow, width), 0) // tp

    def stage_a(c, chip):
        lanes = lanes_of(c)
        d = pl.ds(pl.multiple_of(chip * 2 * trow, 2 * trow), 2 * trow)
        a = dot(hid[d, :], s[c]) * scale
        for w in range(2):
            p = w + e - 2 * w * e
            y = piece[c, pl.ds(pl.multiple_of(p * tp, tp), tp), :].astype(F32)
            y = jnp.concatenate([y, y], axis=0)
            aw = a[w * trow:(w + 1) * trow] - jnp.where(jnp.logical_and(row_core == e, chip == yl), y, 0.0)
            if w == 0:
                pown[...] = aw
            else:
                tok[block(chip * 2 + 1), lanes] = aw.astype(BF16)
        c_p(c, chip).start()

    def stage_b(c, chip):
        c_p(c, chip).wait_recv()
        lanes = lanes_of(c)

        def one(i, _):
            other = r2[4 + c // 3, block((c % 3) * 2 + chip, i * 64, 64), :]
            mine = pown[pl.ds(pl.multiple_of(i * 64, 64), 64), :]
            tok[block(2 * chip, i * 64, 64), lanes] = (mine + other.astype(F32)).astype(BF16)
            return 0

        lax.fori_loop(0, trow // 64, one, 0)

    def stage_c(c):
        for chip in range(2):
            c_q(c, chip).wait_recv()
        lanes = lanes_of(c)

        def one(i, _):
            for chip in range(2):
                o = block(chip, i * 64, 64)
                mine = tok[block(2 * chip, i * 64, 64), lanes]
                qrx[c, o, :] = (qrx[c, o, :].astype(F32) + mine.astype(F32)).astype(BF16)
            return 0

        lax.fori_loop(0, trow // 64, one, 0)
        c_r(c).start()

    def stage_d(c):
        c_r(c).wait_recv()

        def one(i, _):
            d = pl.ds(pl.multiple_of(i * GRAD_ROWS, GRAD_ROWS), GRAD_ROWS)
            g = dot(r2[0, d, :], qrx[c, :trow, :])
            g += dot(r2[1, d, :], rrx[c, :trow, :])
            g += dot(r2[2, d, :], qrx[c, trow:, :])
            g += dot(r2[3, d, :], rrx[c, trow:, :])
            s[c, d, :] = (s[c, d, :].astype(F32) - (LEARN_RATE * scale) * g).astype(BF16)
            return 0

        lax.fori_loop(0, rows // GRAD_ROWS, one, 0)
        early(c)

    for p in range(2):
        own_in(p).wait()
    for j in range(rows // width):
        up_a(j).wait()
        up_b(j).wait()
    for p in range(2):
        t_core(p).wait_recv()
    hidden(2 * yl, 2)
    for c in range(slabs):
        w_in(c).wait()
        t_in(c).wait()

    def own_step(i, _):
        when(i >= 1, lambda: stage_b(i - 1, yl))
        when(jnp.logical_and(i >= 1, i <= jnp.where(inner, HEAD_IN, HEAD)), lambda: c_q(i - 1, yl).start())
        when(jnp.logical_and(i > HEAD, outer), lambda: relay_out(i - 1).start())
        when(i < slabs, lambda: stage_a(i, yl))
        return 0

    lax.fori_loop(0, slabs + 1, own_step, 0)
    for p in range(2):
        t_mate(p).wait_recv()
        t_fwd(p).start()
        t_fwd(p).wait_recv()
        hidden(2 * (1 - yl) + which(p, e), 1)
    for p in range(2):
        t_fwd(p).wait_send()

    def other_step(i, _):
        when(jnp.logical_and(i >= 1, i <= slabs), lambda: stage_b(i - 1, 1 - yl),
             lambda: c_q(i - 1, 1 - yl).start())

        @pl.when(jnp.logical_and(i == RELAY_AT, inner))
        def _():
            for k in range(slabs - HEAD):
                relay_out(HEAD + k).wait_recv()
                relay_on(k).start()

        when(jnp.logical_and(jnp.logical_and(i >= 1, i <= slabs - HEAD_IN), inner),
             lambda: c_q(i - 1 + HEAD_IN, yl).start())
        when(jnp.logical_and(i == slabs, z == 3), lambda: put(0, range(WRAP_DEPTH)))
        when(jnp.logical_and(i == slabs, z == 0), lambda: put(1, range(WRAP_DEPTH)))
        behind = i - jnp.where(inner, LAG[0], LAG[1])
        due = jnp.logical_and(behind >= 0, behind < slabs)
        when(due, lambda: stage_c(behind))
        when(i < slabs, lambda: stage_a(i, 1 - yl))
        when(due, lambda: stage_d(behind))
        return 0

    lax.fori_loop(0, slabs + LAG[1], other_step, 0)

    BR = 64

    def over(i, body):
        c, _ = item(i)
        lo = (i % 2) * cr

        def one(k, _):
            body(c, pl.ds(pl.multiple_of(lo + k * BR, BR), BR))
            return 0

        lax.fori_loop(0, cr // BR, one, 0)

    def first(i):
        def body(c, d):
            a = s[c, d, :].astype(F32)
            p = l1[c, d, :].astype(F32)
            q = r1[c, d, :].astype(F32)
            l1[c, d, :] = (m[0][0] * a + m[0][1] * p + m[0][2] * q).astype(BF16)
            r1[c, d, :] = (wb * a + wl * p + wr * q).astype(BF16)
        over(i, body)

    def mixed(c, d):
        a = l1[c, d, :].astype(F32)
        p = l2[c, d, :].astype(F32)
        q = r2[c, d, :].astype(F32)
        return m[1][0] * a + m[1][1] * p + m[1][2] * q

    def second(i):
        def inside(c, d):
            l2[c, d, :] = (mixed(c, d) - avg[c, d, :].astype(F32)).astype(BF16)

        def outside(c, d):
            l2[c, d, :] = mixed(c, d).astype(BF16)

        when(inner, lambda: over(i, inside))
        when(jnp.logical_not(inner), lambda: over(i, outside))

    unmix = 4.0 / jnp.where(z == 1, n(1, kl, 2), n(1, kr, 1))

    def outward(i):
        g = (i % chunks) // 2
        if i % 2 == 0:
            for j in (1, 2, 3):
                a_rs(g, j).wait_send()

        def body(c, d):
            r1[c, d, :] = (l1[c, d, :].astype(F32) - unmix * avg[c, d, :].astype(F32)).astype(BF16)

        over(i, body)

    def own(g, xx, lo, size):
        return (g, pl.ds(pl.multiple_of(xx * quarter + lo, 32), size))

    def a_rs(g, j):
        xx = (x + j) % 4
        return send(r1.at[own(g, xx, 0, quarter)], rsx.at[j - 1, g % RING],
                    xs.at[g, j - 1], xr.at[g, j - 1], at(xx, yh, z))

    def a_y(g):
        return send(piece.at[g, pl.ds(pl.multiple_of((1 - yh) * half, 32), half)],
                    yrx.at[g], ys.at[0, g], yr.at[0, g], ydev)

    def a_z(g):
        return send(piece.at[g, pl.ds(pl.multiple_of(yh * half, 32), half)],
                    zrx.at[g], zs.at[g], zr.at[g], zdev)

    def a_yg(g):
        ref = avg.at[own(g, x, yh * half, half)]
        return send(ref, ref, ys.at[1, g], yr.at[1, g], ydev)

    def a_x(g, k):
        if k == 0:
            ref, to = avg.at[own(g, x, 0, quarter)], xp
        elif k == 1:
            ref, to = avg.at[own(g, x, 0, quarter)], xm
        elif k == 2:
            ref, to = avg.at[own(g, (x + 3) % 4, 0, half)], xp
        else:
            ref, to = avg.at[own(g, (x + 1) % 4, half, half)], xm
        return send(ref, ref, as_.at[g, k], ar.at[g, k], to)


    def e_rs(g):
        if g >= RING:
            pl.semaphore_wait(free.at[g - RING], 3)
        for j in (1, 2, 3):
            a_rs(g, j).start()

    def e_y(g):
        for j in (1, 2, 3):
            a_rs(g, j).wait_recv()
        def one(i, _):
            d = pl.ds(pl.multiple_of(i * 64, 64), 64)
            o = pl.ds(pl.multiple_of(x * quarter + i * 64, 64), 64)
            t = r1[g, o, :].astype(F32)
            for j in range(3):
                t += rsx[j, g % RING, d, :].astype(F32)
            piece[g, d, :] = t.astype(BF16)
            return 0

        lax.fori_loop(0, quarter // 64, one, 0)
        if g < groups - RING:
            for j in (1, 2, 3):
                pl.semaphore_signal(free.at[g], inc=1, device_id=at((x + j) % 4, yh, z), device_id_type=MESH)
        a_y(g).start()

    def add_half(g, other, final):
        def one(i, _):
            d = pl.ds(pl.multiple_of(i * 32, 32), 32)
            o = pl.ds(pl.multiple_of(yh * half + i * 32, 32), 32)
            t = piece[g, o, :].astype(F32) + other[g, d, :].astype(F32)
            if final:
                p = pl.ds(pl.multiple_of(x * quarter + yh * half + i * 32, 32), 32)
                avg[g, p, :] = (t * (1.0 / NW)).astype(BF16)
            else:
                piece[g, o, :] = t.astype(BF16)
            return 0

        lax.fori_loop(0, half // 32, one, 0)

    def e_z(g):
        a_y(g).wait_recv()
        add_half(g, yrx, False)
        a_z(g).start()

    def e_yg(g):
        a_z(g).wait_recv()
        add_half(g, zrx, True)
        a_yg(g).start()

    def e_x0(g):
        a_yg(g).wait_recv()
        a_x(g, 0).start()
        a_x(g, 1).start()

    def e_x1(g):
        a_x(g, 0).wait_recv()
        a_x(g, 1).wait_recv()
        a_x(g, 2).start()
        a_x(g, 3).start()

    def e_x2(g):
        a_x(g, 2).wait_recv()
        a_x(g, 3).wait_recv()

    inside = {}
    for g in range(groups):
        for f, lag in zip((e_rs, e_y, e_z, e_yg, e_x0, e_x1, e_x2), LAGS):
            inside.setdefault(2 * g + 1 + lag, []).append(functools.partial(f, g))
    jit, wrap, bulk = {}, {}, {}
    for i in range(slabs, 2 * chunks):
        jit.setdefault(i - 3 if i < chunks else max(i - 3, chunks - 2), []).append(i)
    for i in range(WRAP_DEPTH, 2 * chunks):
        wrap.setdefault(i - WRAP_DEPTH, []).append(i)
    for i in range(chunks, 2 * chunks):
        bulk.setdefault(max(i - chunks, slabs), []).append(i)

    def issue(slot):
        if slot in jit:
            @pl.when(inner)
            def _():
                for i in jit[slot]:
                    if i >= chunks:
                        outward(i)
            when(z == 1, lambda: put(0, jit[slot]), lambda: put(1, jit[slot], r1))
            when(z == 2, lambda: put(1, jit[slot]), lambda: put(0, jit[slot], r1))
        when(z == 3, lambda: put(0, wrap.get(slot, ())), lambda: put(1, bulk.get(slot, ())))
        when(z == 0, lambda: put(1, wrap.get(slot, ())), lambda: put(0, bulk.get(slot, ())))

    for slot in range(2 * chunks):
        for cp in items(slot):
            cp().wait_recv()
        if slot < chunks:
            first(slot)
        else:
            second(slot)
        if slot in inside:
            when(inner, *inside[slot])
        issue(slot)

    for p in range(2):
        t_core(p).wait_send()
        t_mate(p).wait_send()
    for c in range(slabs):
        for chip in range(2):
            c_p(c, chip).wait_send()
            c_q(c, chip).wait_send()
        c_r(c).wait_send()
    for i in range(2 * chunks):
        for cp in items(i):
            cp().wait_send()

    @pl.when(inner)
    def _():
        for g in range(groups):
            for f in (a_y, a_z, a_yg):
                f(g).wait_send()
            if g < slabs - HEAD:
                relay_on(g).wait_send()
            for k in range(4):
                a_x(g, k).wait_send()


def copy_kernel(src, dst, sem):
    slabs, _, width = src.shape

    def move(i):
        return pltpu.make_async_copy(src.at[i], dst.at[0, :, pl.ds(i * width, width)], sem.at[i])

    for i in range(slabs):
        move(i).start()
    for i in range(slabs):
        move(i).wait()


def copy_call(a):
    slabs, rows, width = a.shape
    return pl.pallas_call(
        copy_kernel,
        out_shape=jax.ShapeDtypeStruct((1, rows, slabs * width), a.dtype),
        in_specs=[pl.BlockSpec(memory_space=pltpu.VMEM)],
        out_specs=pl.BlockSpec(memory_space=pl.ANY),
        scratch_shapes=[pltpu.SemaphoreType.DMA((slabs,))],
        compiler_params=pltpu.CompilerParams(vmem_limit_bytes=8 * 2**20),
        name="place",
    )(a)


def body(tokens, targets, up_weight, down_weight, mix_numer):
    rows, dim = down_weight.shape[1:]
    slabs = 8
    width = dim // slabs
    trow = tokens.shape[0]
    D = pltpu.SemaphoreType.DMA
    vm = lambda *shape: pltpu.VMEM(shape, BF16)
    any_ = pl.BlockSpec(memory_space=pl.ANY)
    return copy_call(pl.pallas_call(
        kernel,
        out_shape=pltpu.VMEM((slabs, rows, width), BF16),
        in_specs=[pl.BlockSpec(memory_space=pltpu.SMEM)] + [any_] * 4,
        out_specs=pl.BlockSpec(memory_space=pltpu.VMEM),
        scratch_shapes=[vm(slabs, rows, width)] * 5 + [
            vm(3, RING, rows // 4, width), vm(slabs, rows // 4, width),
            vm(slabs, rows // 8, width), vm(slabs, rows // 8, width),
            vm(4 * trow, dim), vm(4 * trow, rows),
            vm(slabs, 2 * trow, width), vm(slabs, 2 * trow, width),
            pltpu.VMEM((trow, width), F32), vm(slabs - HEAD, trow, width), D((slabs - HEAD,)), D((slabs - HEAD,)),
            D((5, slabs)), D((3, 2)), D((3, 2)),
            D((slabs, 2)), D((slabs, 2)), D((slabs, 2)), D((slabs, 2)), D((slabs,)), D((slabs,)),
            D((2, 4 * slabs)), D((2, 4 * slabs)), D((slabs, 3)), D((slabs, 3)), D((slabs, 4)), D((slabs, 4)),
            D((2, slabs)), D((2, slabs)), D((slabs,)), D((slabs,)),
            pltpu.SemaphoreType.REGULAR((slabs - RING,)),
        ],
        compiler_params=pltpu.CompilerParams(
            collective_id=0, has_side_effects=True, vmem_limit_bytes=LIM),
        name="gossip",
    )(mix_numer.transpose(2, 0, 1), tokens, targets, up_weight, down_weight))


def solution(mesh):
    in_specs = (P(("blk", "shard"), None), P(("blk", "shard"), None), P(None, "shard"), P("blk", "shard", None), P())
    return jax.shard_map(body, mesh=mesh, in_specs=in_specs, out_specs=P("blk", "shard", None), check_vma=False)
```

```python
import functools

import jax
import jax.numpy as jnp
from jax import lax
from jax.experimental import pallas as pl
from jax.experimental.pallas import tpu as pltpu
from jax.sharding import PartitionSpec as P

MESH = pl.DeviceIdType.MESH
LEARN_RATE = 2.0
NW = 32
GRAD_ROWS = 896
HEAD = 4
RELAY_AT = 1
LAG = (2, 4)
HEAD_IN = 4
PAIR = 2
LIM = 67_043_328 - 7_800_000
RING = 4
LAGS = (0, 2, 3, 6, 7, 8, 9)
WRAP_DEPTH = 3
F32 = jnp.float32
BF16 = jnp.bfloat16


def dot(a, b):
    return jnp.dot(a, b, preferred_element_type=F32)


def kernel(numer, tokens, targets, up, weight, l2,
           s, l1, r1, r2, avg, rsx, piece, yrx, zrx, tok, hid, qrx, rrx, pown, rel, rels, relr,
           ls, ts, tr, ps, pr, qs, qr, rs, rr,
           gs, gr, xs, xr, as_, ar, ys, yr, zs, zr, free):
    b, sh = lax.axis_index("blk"), lax.axis_index("shard")
    x, yh, z = b // 8, (b // 4) % 2, b % 4
    yl, e = sh // 2, sh % 2
    slabs, rows, width = s.shape
    chunks, cr = 2 * slabs, rows // 2
    ff, dim = 4 * rows, slabs * width
    groups = slabs
    quarter, half = rows // 4, rows // 8
    trow = tokens.shape[0]
    tp = trow // 2

    def at(xx, yy, zz):
        return (xx * 8 + yy * 4 + zz, sh)

    left, right = ((b + 31) % 32, sh), ((b + 1) % 32, sh)
    core, mate = (b, 2 * yl + 1 - e), (b, 2 * (1 - yl) + e)
    ydev = at(x, 1 - yh, z)
    zdev = at(x, yh, 3 - z)
    xp, xm = at((x + 1) % 4, yh, z), at((x + 3) % 4, yh, z)
    inner = jnp.logical_or(z == 1, z == 2)
    outer = jnp.logical_not(inner)
    beside = (b + jnp.where(z % 2 == 0, 1, 31)) % 32

    def send(src, dst, ss, rsem, dev):
        return pltpu.make_async_remote_copy(src, dst, ss, rsem, device_id=dev, device_id_type=MESH)

    def when(cond, *fs):
        @pl.when(cond)
        def _():
            for f in fs:
                f()

    def up_a(j):
        return pltpu.make_async_copy(up.at[pl.ds(0, rows), pl.ds(j * width, width)], l2.at[j], ls.at[0, j])

    def up_b(j):
        return pltpu.make_async_copy(up.at[pl.ds(rows, dim - rows), pl.ds(j * width, width)],
                                     l2.at[slabs - 1, pl.ds(j * width, width)], ls.at[1, j])

    def w_in(c):
        return pltpu.make_async_copy(weight.at[0, :, pl.ds(c * width, width)], s.at[c], ls.at[2, c])

    def t_in(c):
        return pltpu.make_async_copy(targets.at[:, pl.ds(c * width, width)], piece.at[c, pl.ds(0, trow)], ls.at[3, c])

    def which(p, core_at):
        return p + core_at - 2 * p * core_at

    def spot(p, chip, core_from, core_at):
        at_row = (chip * 2 + which(p, core_at)) * trow + core_from * tp
        return pl.ds(pl.multiple_of(at_row, tp), tp)

    def own_in(p):
        return pltpu.make_async_copy(tokens.at[pl.ds(p * tp, tp)], tok.at[spot(p, yl, e, e)], ls.at[4, p])

    def t_core(p):
        return send(tokens.at[pl.ds(p * tp, tp)], tok.at[spot(p, yl, e, 1 - e)], ts.at[0, p], tr.at[0, p], core)

    def t_mate(p):
        return send(tokens.at[pl.ds(p * tp, tp)], tok.at[spot(p, yl, e, e)], ts.at[1, p], tr.at[1, p], mate)

    def t_fwd(p):
        return send(tok.at[spot(p, 1 - yl, e, e)], tok.at[spot(p, 1 - yl, e, 1 - e)], ts.at[2, p], tr.at[2, p], core)

    barrier = pltpu.get_barrier_semaphore()
    for dev in (core, mate, left, right, (beside, mate[1])):
        pl.semaphore_signal(barrier, inc=1, device_id=dev, device_id_type=MESH)

    @pl.when(inner)
    def _():
        for dev in (xp, at((x + 2) % 4, yh, z), xm, ydev):
            pl.semaphore_signal(barrier, inc=1, device_id=dev, device_id_type=MESH)

    for p in range(2):
        own_in(p).start()
    for j in range(rows // width):
        up_a(j).start()
        up_b(j).start()

    pl.semaphore_wait(barrier, jnp.where(inner, 9, 5))

    for p in range(2):
        t_mate(p).start()
    for p in range(2):
        t_core(p).start()
    for c in range(slabs):
        w_in(c).start()
        t_in(c).start()

    def n(r, k, j):
        return numer[j, r, k].astype(F32)

    kl, kr, kll, krr = (b + 31) % 32, (b + 1) % 32, (b + 30) % 32, (b + 2) % 32

    def v(k0, k, k1):
        return n(1, k, 0) + n(1, k1, 1) + n(1, k0, 2)

    vb, vl, vr = v(kl, b, kr), v(kll, kl, b), v(b, kr, krr)
    vll, vrr = v((b + 29) % 32, kll, kl), v(kr, krr, (b + 3) % 32)
    wb = (n(0, b, 0) * vb + n(0, kr, 1) * vr + n(0, kl, 2) * vl) * (1.0 / 16)
    wl = (n(0, kl, 0) * vl + n(0, b, 1) * vb + n(0, kll, 2) * vll) * (1.0 / 16)
    wr = (n(0, kr, 0) * vr + n(0, krr, 1) * vrr + n(0, b, 2) * vb) * (1.0 / 16)
    wl = jnp.where(z == 1, wl, 0.0)
    wr = jnp.where(z == 2, wr, 0.0)
    m = [[n(r, b, j) * 0.25 for j in range(3)] for r in range(2)]

    def hidden(t, size):
        d = pl.ds(pl.multiple_of(t * trow, trow), size * trow)

        def tiles(j, many):
            at_j = [j + k for k in range(many)]
            lanes = [pl.ds(pl.multiple_of(jj * width, width), width) for jj in at_j]
            above = jnp.concatenate([l2[jj] for jj in at_j], axis=1)
            below = jnp.concatenate([l2[slabs - 1, n, :] for n in lanes], axis=1)
            a = dot(tok[d, :rows], above) + dot(tok[d, rows:], below)
            h = (a / (1.0 + jnp.exp(-a))).astype(BF16)
            for i, n in enumerate(lanes):
                hh = h[:, i * width:(i + 1) * width]
                hid[d, n] = hh
                for k in range(size):
                    r2[t + k, n, :] = hh[k * trow:(k + 1) * trow].T

        many = PAIR if size == 1 else 1
        whole = rows // width // many

        def one(j, _):
            tiles(j * many, many)
            return 0

        lax.fori_loop(0, whole, one, 0)
        for j in range(whole * many, rows // width):
            tiles(j, 1)

    scale = ff ** -0.5

    def lanes_of(c):
        return pl.ds(pl.multiple_of(c * width, width), width)

    def block(lo, i=0, size=None):
        return pl.ds(pl.multiple_of(lo * trow + i, 64), trow if size is None else size)

    def c_p(c, chip):
        return send(tok.at[block(2 * chip + 1), lanes_of(c)], r2.at[4 + c // 3, block((c % 3) * 2 + chip)],
                    ps.at[c, chip], pr.at[c, chip], core)

    def c_q(c, chip):
        return send(tok.at[block(2 * chip), lanes_of(c)], qrx.at[c, block(chip)], qs.at[c, chip], qr.at[c, chip], mate)

    def relay_out(c):
        return send(tok.at[block(2 * yl), lanes_of(c)], rel.at[c - HEAD], qs.at[c, yl], relr.at[c - HEAD],
                    (beside, sh))

    def relay_on(k):
        return send(rel.at[k], qrx.at[HEAD + k, block(yl)], rels.at[k], qr.at[HEAD + k, yl], (beside, mate[1]))

    def c_r(c):
        return send(qrx.at[c], rrx.at[c], rs.at[c], rr.at[c], core)

    def item(i):
        c, o = (i % chunks) // 2, i % 2
        d = pl.ds(o * cr, cr)
        return c, d

    def items(i, later=None):
        c, d = item(i)
        src, dl, dr = (s, l1, r1) if i < chunks else (l1 if later is None else later, l2, r2)
        return (lambda: send(src.at[c, d], dl.at[c, d], gs.at[0, i], gr.at[0, i], right),
                lambda: send(src.at[c, d], dr.at[c, d], gs.at[1, i], gr.at[1, i], left))

    def put(direction, those, later=None):
        for i in those:
            items(i, later)[direction]().start()

    def right_item(c, o, i):
        d = pl.ds(o * cr if isinstance(o, int) else pl.multiple_of(o * cr, cr), cr)
        return send(s.at[c, d], l1.at[c, d], gs.at[0, i], gr.at[0, i], right)

    def left_item(c, o, i):
        d = pl.ds(o * cr if isinstance(o, int) else pl.multiple_of(o * cr, cr), cr)
        return send(s.at[c, d], r1.at[c, d], gs.at[1, i], gr.at[1, i], left)

    def early(c):
        @pl.when(z == 0)
        def _():
            for o in range(2):
                right_item(c, o, 2 * c + o).start()

        @pl.when(z == 3)
        def _():
            for o in range(2):
                left_item(c, o, 2 * c + o).start()

        @pl.when(inner)
        def _():
            right_item(c // 2, c % 2, c).start()
            left_item(c // 2, c % 2, c).start()

    row_core = lax.broadcasted_iota(jnp.int32, (trow, width), 0) // tp

    def stage_a(c, chip):
        lanes = lanes_of(c)
        d = pl.ds(pl.multiple_of(chip * 2 * trow, 2 * trow), 2 * trow)
        a = dot(hid[d, :], s[c]) * scale
        for w in range(2):
            p = w + e - 2 * w * e
            y = piece[c, pl.ds(pl.multiple_of(p * tp, tp), tp), :].astype(F32)
            y = jnp.concatenate([y, y], axis=0)
            aw = a[w * trow:(w + 1) * trow] - jnp.where(jnp.logical_and(row_core == e, chip == yl), y, 0.0)
            if w == 0:
                pown[...] = aw
            else:
                tok[block(chip * 2 + 1), lanes] = aw.astype(BF16)
        c_p(c, chip).start()

    def stage_b(c, chip):
        c_p(c, chip).wait_recv()
        lanes = lanes_of(c)

        def one(i, _):
            other = r2[4 + c // 3, block((c % 3) * 2 + chip, i * 64, 64), :]
            mine = pown[pl.ds(pl.multiple_of(i * 64, 64), 64), :]
            tok[block(2 * chip, i * 64, 64), lanes] = (mine + other.astype(F32)).astype(BF16)
            return 0

        lax.fori_loop(0, trow // 64, one, 0)

    def stage_c(c):
        for chip in range(2):
            c_q(c, chip).wait_recv()
        lanes = lanes_of(c)

        def one(i, _):
            for chip in range(2):
                o = block(chip, i * 64, 64)
                mine = tok[block(2 * chip, i * 64, 64), lanes]
                qrx[c, o, :] = (qrx[c, o, :].astype(F32) + mine.astype(F32)).astype(BF16)
            return 0

        lax.fori_loop(0, trow // 64, one, 0)
        c_r(c).start()

    def stage_d(c):
        c_r(c).wait_recv()

        def one(i, _):
            d = pl.ds(pl.multiple_of(i * GRAD_ROWS, GRAD_ROWS), GRAD_ROWS)
            g = dot(r2[0, d, :], qrx[c, :trow, :])
            g += dot(r2[1, d, :], rrx[c, :trow, :])
            g += dot(r2[2, d, :], qrx[c, trow:, :])
            g += dot(r2[3, d, :], rrx[c, trow:, :])
            s[c, d, :] = (s[c, d, :].astype(F32) - (LEARN_RATE * scale) * g).astype(BF16)
            return 0

        lax.fori_loop(0, rows // GRAD_ROWS, one, 0)
        early(c)

    for p in range(2):
        own_in(p).wait()
    for j in range(rows // width):
        up_a(j).wait()
        up_b(j).wait()
    for p in range(2):
        t_core(p).wait_recv()
    hidden(2 * yl, 2)
    for c in range(slabs):
        w_in(c).wait()
        t_in(c).wait()

    def own_step(i, _):
        when(i >= 1, lambda: stage_b(i - 1, yl))
        when(jnp.logical_and(i >= 1, i <= jnp.where(inner, HEAD_IN, HEAD)), lambda: c_q(i - 1, yl).start())
        when(jnp.logical_and(i > HEAD, outer), lambda: relay_out(i - 1).start())
        when(i < slabs, lambda: stage_a(i, yl))
        return 0

    lax.fori_loop(0, slabs + 1, own_step, 0)
    for p in range(2):
        t_mate(p).wait_recv()
        t_fwd(p).start()
        t_fwd(p).wait_recv()
        hidden(2 * (1 - yl) + which(p, e), 1)
    for p in range(2):
        t_fwd(p).wait_send()

    def other_step(i, _):
        when(jnp.logical_and(i >= 1, i <= slabs), lambda: stage_b(i - 1, 1 - yl),
             lambda: c_q(i - 1, 1 - yl).start())

        for k in range(slabs - HEAD):
            when(jnp.logical_and(i == RELAY_AT + k, inner),
                 lambda: relay_out(HEAD + k).wait_recv(), lambda: relay_on(k).start())

        when(jnp.logical_and(jnp.logical_and(i >= 1, i <= slabs - HEAD_IN), inner),
             lambda: c_q(i - 1 + HEAD_IN, yl).start())
        when(jnp.logical_and(i == slabs, z == 3), lambda: put(0, range(WRAP_DEPTH)))
        when(jnp.logical_and(i == slabs, z == 0), lambda: put(1, range(WRAP_DEPTH)))
        behind = i - jnp.where(inner, LAG[0], LAG[1])
        due = jnp.logical_and(behind >= 0, behind < slabs)
        when(due, lambda: stage_c(behind))
        when(i < slabs, lambda: stage_a(i, 1 - yl))
        when(due, lambda: stage_d(behind))
        return 0

    lax.fori_loop(0, slabs + LAG[1], other_step, 0)

    BR = 64

    def over(i, body):
        c, _ = item(i)
        lo = (i % 2) * cr

        def one(k, _):
            body(c, pl.ds(pl.multiple_of(lo + k * BR, BR), BR))
            return 0

        lax.fori_loop(0, cr // BR, one, 0)

    def first(i):
        def body(c, d):
            a = s[c, d, :].astype(F32)
            p = l1[c, d, :].astype(F32)
            q = r1[c, d, :].astype(F32)
            l1[c, d, :] = (m[0][0] * a + m[0][1] * p + m[0][2] * q).astype(BF16)
            r1[c, d, :] = (wb * a + wl * p + wr * q).astype(BF16)
        over(i, body)

    def mixed(c, d):
        a = l1[c, d, :].astype(F32)
        p = l2[c, d, :].astype(F32)
        q = r2[c, d, :].astype(F32)
        return m[1][0] * a + m[1][1] * p + m[1][2] * q

    def second(i):
        def inside(c, d):
            l2[c, d, :] = (mixed(c, d) - avg[c, d, :].astype(F32)).astype(BF16)

        def outside(c, d):
            l2[c, d, :] = mixed(c, d).astype(BF16)

        when(inner, lambda: over(i, inside))
        when(jnp.logical_not(inner), lambda: over(i, outside))

    unmix = 4.0 / jnp.where(z == 1, n(1, kl, 2), n(1, kr, 1))

    def outward(i):
        g = (i % chunks) // 2
        if i % 2 == 0:
            for j in (1, 2, 3):
                a_rs(g, j).wait_send()

        def body(c, d):
            r1[c, d, :] = (l1[c, d, :].astype(F32) - unmix * avg[c, d, :].astype(F32)).astype(BF16)

        over(i, body)

    def own(g, xx, lo, size):
        return (g, pl.ds(pl.multiple_of(xx * quarter + lo, 32), size))

    def a_rs(g, j):
        xx = (x + j) % 4
        return send(r1.at[own(g, xx, 0, quarter)], rsx.at[j - 1, g % RING],
                    xs.at[g, j - 1], xr.at[g, j - 1], at(xx, yh, z))

    def a_y(g):
        return send(piece.at[g, pl.ds(pl.multiple_of((1 - yh) * half, 32), half)],
                    yrx.at[g], ys.at[0, g], yr.at[0, g], ydev)

    def a_z(g):
        return send(piece.at[g, pl.ds(pl.multiple_of(yh * half, 32), half)],
                    zrx.at[g], zs.at[g], zr.at[g], zdev)

    def a_yg(g):
        ref = avg.at[own(g, x, yh * half, half)]
        return send(ref, ref, ys.at[1, g], yr.at[1, g], ydev)

    def a_x(g, k):
        if k == 0:
            ref, to = avg.at[own(g, x, 0, quarter)], xp
        elif k == 1:
            ref, to = avg.at[own(g, x, 0, quarter)], xm
        elif k == 2:
            ref, to = avg.at[own(g, (x + 3) % 4, 0, half)], xp
        else:
            ref, to = avg.at[own(g, (x + 1) % 4, half, half)], xm
        return send(ref, ref, as_.at[g, k], ar.at[g, k], to)


    def e_rs(g):
        if g >= RING:
            pl.semaphore_wait(free.at[g - RING], 3)
        for j in (1, 2, 3):
            a_rs(g, j).start()

    def e_y(g):
        for j in (1, 2, 3):
            a_rs(g, j).wait_recv()
        def one(i, _):
            d = pl.ds(pl.multiple_of(i * 64, 64), 64)
            o = pl.ds(pl.multiple_of(x * quarter + i * 64, 64), 64)
            t = r1[g, o, :].astype(F32)
            for j in range(3):
                t += rsx[j, g % RING, d, :].astype(F32)
            piece[g, d, :] = t.astype(BF16)
            return 0

        lax.fori_loop(0, quarter // 64, one, 0)
        if g < groups - RING:
            for j in (1, 2, 3):
                pl.semaphore_signal(free.at[g], inc=1, device_id=at((x + j) % 4, yh, z), device_id_type=MESH)
        a_y(g).start()

    def add_half(g, other, final):
        def one(i, _):
            d = pl.ds(pl.multiple_of(i * 32, 32), 32)
            o = pl.ds(pl.multiple_of(yh * half + i * 32, 32), 32)
            t = piece[g, o, :].astype(F32) + other[g, d, :].astype(F32)
            if final:
                p = pl.ds(pl.multiple_of(x * quarter + yh * half + i * 32, 32), 32)
                avg[g, p, :] = (t * (1.0 / NW)).astype(BF16)
            else:
                piece[g, o, :] = t.astype(BF16)
            return 0

        lax.fori_loop(0, half // 32, one, 0)

    def e_z(g):
        a_y(g).wait_recv()
        add_half(g, yrx, False)
        a_z(g).start()

    def e_yg(g):
        a_z(g).wait_recv()
        add_half(g, zrx, True)
        a_yg(g).start()

    def e_x0(g):
        a_yg(g).wait_recv()
        a_x(g, 0).start()
        a_x(g, 1).start()

    def e_x1(g):
        a_x(g, 0).wait_recv()
        a_x(g, 1).wait_recv()
        a_x(g, 2).start()
        a_x(g, 3).start()

    def e_x2(g):
        a_x(g, 2).wait_recv()
        a_x(g, 3).wait_recv()

    inside = {}
    for g in range(groups):
        for f, lag in zip((e_rs, e_y, e_z, e_yg, e_x0, e_x1, e_x2), LAGS):
            inside.setdefault(2 * g + 1 + lag, []).append(functools.partial(f, g))
    jit, wrap, bulk = {}, {}, {}
    for i in range(slabs, 2 * chunks):
        jit.setdefault(i - 3 if i < chunks else max(i - 3, chunks - 2), []).append(i)
    for i in range(WRAP_DEPTH, 2 * chunks):
        wrap.setdefault(i - WRAP_DEPTH, []).append(i)
    for i in range(chunks, 2 * chunks):
        bulk.setdefault(max(i - chunks, slabs), []).append(i)

    def issue(slot):
        if slot in jit:
            @pl.when(inner)
            def _():
                for i in jit[slot]:
                    if i >= chunks:
                        outward(i)
            when(z == 1, lambda: put(0, jit[slot]), lambda: put(1, jit[slot], r1))
            when(z == 2, lambda: put(1, jit[slot]), lambda: put(0, jit[slot], r1))
        when(z == 3, lambda: put(0, wrap.get(slot, ())), lambda: put(1, bulk.get(slot, ())))
        when(z == 0, lambda: put(1, wrap.get(slot, ())), lambda: put(0, bulk.get(slot, ())))

    for slot in range(2 * chunks):
        for cp in items(slot):
            cp().wait_recv()
        if slot < chunks:
            first(slot)
        else:
            second(slot)
        if slot in inside:
            when(inner, *inside[slot])
        issue(slot)

    for p in range(2):
        t_core(p).wait_send()
        t_mate(p).wait_send()
    for c in range(slabs):
        for chip in range(2):
            c_p(c, chip).wait_send()
            c_q(c, chip).wait_send()
        c_r(c).wait_send()
    for i in range(2 * chunks):
        for cp in items(i):
            cp().wait_send()

    @pl.when(inner)
    def _():
        for g in range(groups):
            for f in (a_y, a_z, a_yg):
                f(g).wait_send()
            if g < slabs - HEAD:
                relay_on(g).wait_send()
            for k in range(4):
                a_x(g, k).wait_send()


def copy_kernel(src, dst, sem):
    slabs, _, width = src.shape

    def move(i):
        return pltpu.make_async_copy(src.at[i], dst.at[0, :, pl.ds(i * width, width)], sem.at[i])

    for i in range(slabs):
        move(i).start()
    for i in range(slabs):
        move(i).wait()


def copy_call(a):
    slabs, rows, width = a.shape
    return pl.pallas_call(
        copy_kernel,
        out_shape=jax.ShapeDtypeStruct((1, rows, slabs * width), a.dtype),
        in_specs=[pl.BlockSpec(memory_space=pltpu.VMEM)],
        out_specs=pl.BlockSpec(memory_space=pl.ANY),
        scratch_shapes=[pltpu.SemaphoreType.DMA((slabs,))],
        compiler_params=pltpu.CompilerParams(vmem_limit_bytes=8 * 2**20),
        name="place",
    )(a)


def body(tokens, targets, up_weight, down_weight, mix_numer):
    rows, dim = down_weight.shape[1:]
    slabs = 8
    width = dim // slabs
    trow = tokens.shape[0]
    D = pltpu.SemaphoreType.DMA
    vm = lambda *shape: pltpu.VMEM(shape, BF16)
    any_ = pl.BlockSpec(memory_space=pl.ANY)
    return copy_call(pl.pallas_call(
        kernel,
        out_shape=pltpu.VMEM((slabs, rows, width), BF16),
        in_specs=[pl.BlockSpec(memory_space=pltpu.SMEM)] + [any_] * 4,
        out_specs=pl.BlockSpec(memory_space=pltpu.VMEM),
        scratch_shapes=[vm(slabs, rows, width)] * 5 + [
            vm(3, RING, rows // 4, width), vm(slabs, rows // 4, width),
            vm(slabs, rows // 8, width), vm(slabs, rows // 8, width),
            vm(4 * trow, dim), vm(4 * trow, rows),
            vm(slabs, 2 * trow, width), vm(slabs, 2 * trow, width),
            pltpu.VMEM((trow, width), F32), vm(slabs - HEAD, trow, width), D((slabs - HEAD,)), D((slabs - HEAD,)),
            D((5, slabs)), D((3, 2)), D((3, 2)),
            D((slabs, 2)), D((slabs, 2)), D((slabs, 2)), D((slabs, 2)), D((slabs,)), D((slabs,)),
            D((2, 4 * slabs)), D((2, 4 * slabs)), D((slabs, 3)), D((slabs, 3)), D((slabs, 4)), D((slabs, 4)),
            D((2, slabs)), D((2, slabs)), D((slabs,)), D((slabs,)),
            pltpu.SemaphoreType.REGULAR((slabs - RING,)),
        ],
        compiler_params=pltpu.CompilerParams(
            collective_id=0, has_side_effects=True, vmem_limit_bytes=LIM),
        name="gossip",
    )(mix_numer.transpose(2, 0, 1), tokens, targets, up_weight, down_weight))


def solution(mesh):
    in_specs = (P(("blk", "shard"), None), P(("blk", "shard"), None), P(None, "shard"), P("blk", "shard", None), P())
    return jax.shard_map(body, mesh=mesh, in_specs=in_specs, out_specs=P("blk", "shard", None), check_vma=False)
```
